256 devices in a mesh: gx: 8 (over x_hi, y), gy: 32 (over z, x_lo, core).
Axes of the slice: x: 4 (x_hi: 2, x_lo: 2; x = x_hi * 2 + x_lo), y: 4, z: 8, core: 2. Of those that a mesh axis runs over, the one named last changes fastest.
Arguments:
- charges: float32 [8, 32, 16384], P('gx', 'gy'), may hold values from -1.2 to 1.2
- fractions: float32 [8, 32, 3, 16384], P('gx', 'gy'), may hold values from 0 to 1
- cells: int32 [8, 32, 2, 16384], P('gx', 'gy'), may hold values from 0 to 511, as said below
Outputs:
- potential_grid: float32 [256, 512, 128], P('gx', 'gy')
- atom_potential: float32 [8, 32, 16384], P('gx', 'gy')
The draws below stay inside these ranges and needn't reach their ends.
Inputs may be any that keep to these rules, and one draw needn't show every extreme that they name: cells[i, j, 0, a] lies in i-independent range j * 16 + 1 to j * 16 + 16, taken modulo 512; cells[i, j, 1, a] is a cell along the third dimension.
All inputs are finite; a program needn't handle non-finite values.
Results may differ from the reference program's by a relative error of at most 0.0003.
Values sent between devices are 32-bit elements; how exact they have to be, the bound alone decides.
A program may use at most 128 MiB of HBM per device.

```python
import jax
import jax.numpy as jnp
import numpy as np
from jax import lax

CX = 32
CY = 16
NZ = 128
ATOMS_DEV = 16384
N_GX = 8
N_GY = 32


def draw_cells(key, part):
    first_key, second_key = jax.random.split(jax.random.fold_in(key, 11))
    offsets_y = jax.random.randint(first_key, (N_GX, N_GY, ATOMS_DEV), 0, CY)
    column = jnp.arange(N_GY, dtype=jnp.int32)[None, :, None] * CY
    cell_y = (column + 1 + offsets_y) % (CY * N_GY)
    cell_z = jax.random.randint(second_key, (N_GX, N_GY, ATOMS_DEV), 0, NZ)
    return jnp.stack([cell_y, cell_z], axis=2).astype(jnp.int32)


def level_of(stream_key, dims, shards, least, largest):
    level = 1.0
    for dim, shards_of in shards:
        heights = jax.random.uniform(jax.random.fold_in(jax.random.fold_in(stream_key, 6), dim), (shards_of,), jnp.float32, least / len(shards), largest / len(shards))
        level = level * jnp.repeat(jnp.exp(heights), dims[dim] // shards_of).reshape((-1,) + (1,) * (len(dims) - 1 - dim))
    return level


def noise(own_key, shape, deviation, bound, cuts=(), kind=jnp.bfloat16):
    result = jax.random.normal(own_key, shape, jnp.float32) * deviation
    if len(cuts) > 0:
        result = level_of(own_key, shape, cuts, -0.22, 0.18) * result
    return jnp.clip(result, min=-bound, max=bound).astype(kind)


def setup_inputs(seed: int = 0) -> dict:
    streams_of = jax.random.split(jax.random.key(seed), 4)
    return {
        "charges": noise(streams_of[0], (N_GX, N_GY, ATOMS_DEV), 0.2, 1.2, ((0, 8), (1, 32)), jnp.float32),
        "fractions": jnp.clip(1.0 * jax.random.uniform(streams_of[1], (N_GX, N_GY, 3, ATOMS_DEV), jnp.float32) ** level_of(streams_of[1], (N_GX, N_GY, 3, ATOMS_DEV), ((0, 8), (1, 32)), -0.2, 0.2), 0.0, 1.0),
        "cells": draw_cells(jax.random.fold_in(streams_of[3], 71), 0),
    }


restrict_taps = ((-3, -0.0625), (-1, 0.5625), (0, 1.0), (1, 0.5625), (3, -0.0625))

def spline_weights(frac):

    def near_weight(distance):
        return (1.0 - distance) * (1.0 + distance - 1.5 * distance * distance)

    def far_weight(distance):
        return -0.5 * (distance - 1.0) * (2.0 - distance) * (2.0 - distance)
    return [far_weight(1.0 + frac), near_weight(frac), near_weight(1.0 - frac), far_weight(2.0 - frac)]

def smooth_numpy(rho):
    return np.where(rho < 1.0, 1.875 - 1.25 * rho * rho + 0.375 * rho ** 4, 1.0 / np.maximum(rho, 1.0))

def smooth_jnp(rho):
    return jnp.where(rho < 1.0, 1.875 - 1.25 * rho * rho + 0.375 * rho ** 4, 1.0 / jnp.maximum(rho, 1.0))

def stencil_full(level, shape, dtype):
    offsets = np.arange(-3, 4)
    grid_a, grid_b, grid_c = np.meshgrid(offsets, offsets, offsets, indexing='ij')
    radius = np.sqrt(grid_a ** 2.0 + grid_b ** 2.0 + grid_c ** 2.0)
    values = (smooth_numpy(radius / 1.5) / 1.5 - smooth_numpy(radius / 3.0) / 3.0) / 2.0 ** (level - 1)
    full = jnp.zeros(shape, dtype)
    return full.at[(grid_a % shape[0]).ravel(), (grid_b % shape[1]).ravel(), (grid_c % shape[2]).ravel()].set(jnp.asarray(values.ravel(), dtype))

def signed_offsets(count, dtype):
    places = jnp.arange(count).astype(dtype)
    return jnp.where(places > count // 2, places - count, places)

def coarse_kernel(shape, dtype):
    first = signed_offsets(shape[0], dtype)[:, None, None]
    second = signed_offsets(shape[1], dtype)[None, :, None]
    third = signed_offsets(shape[2], dtype)[None, None, :]
    radius = jnp.sqrt(first * first + second * second + third * third)
    return smooth_jnp(radius / 1.5) / 12.0

def periodic_convolve(field, kernel):
    return jnp.fft.irfftn(jnp.fft.rfftn(field) * jnp.fft.rfftn(kernel), s=field.shape).astype(field.dtype)

def restrict_grid(field):
    for axis in range(3):
        total = jnp.zeros_like(field)
        for offset, weight in restrict_taps:
            total = total + weight * jnp.roll(field, -offset, axis=axis)
        field = lax.slice_in_dim(total, 0, field.shape[axis], 2, axis)
    return field

def prolong_grid(field):
    for axis in range(3):
        odd_rows = 0.5625 * (field + jnp.roll(field, -1, axis=axis)) - 0.0625 * (jnp.roll(field, 1, axis=axis) + jnp.roll(field, -2, axis=axis))
        stacked = jnp.stack([field, odd_rows], axis=axis + 1)
        shape = list(field.shape)
        shape[axis] = 2 * shape[axis]
        field = stacked.reshape(shape)
    return field

def reference(charges, fractions, cells):
    total_x = CX * N_GX
    total_y = CY * N_GY
    per_plane = ATOMS_DEV // CX
    plane = jnp.arange(ATOMS_DEV, dtype=jnp.int32) // per_plane
    base_x = jnp.arange(N_GX, dtype=jnp.int32)[:, None, None] * CX + plane[None, None, :] + jnp.zeros((N_GX, N_GY, ATOMS_DEV), jnp.int32)
    base_y = cells[:, :, 0] - 1
    base_z = cells[:, :, 1] - 1
    weights_x = spline_weights(fractions[:, :, 0])
    weights_y = spline_weights(fractions[:, :, 1])
    weights_z = spline_weights(fractions[:, :, 2])
    flat_points = []
    level_one = jnp.zeros((total_x * total_y * NZ,), fractions.dtype)
    for tap_x in range(4):
        for tap_y in range(4):
            for tap_z in range(4):
                flat = ((base_x + tap_x) % total_x * total_y + (base_y + tap_y) % total_y) * NZ + (base_z + tap_z) % NZ
                flat = flat.astype(jnp.int32)
                product = weights_x[tap_x] * weights_y[tap_y] * weights_z[tap_z]
                flat_points.append((flat, product))
                level_one = level_one.at[flat.ravel()].add((charges * product).ravel())
    grids = [level_one.reshape(total_x, total_y, NZ)]
    for level in range(3):
        grids.append(restrict_grid(grids[-1]))
    potential = periodic_convolve(grids[3], coarse_kernel(grids[3].shape, grids[3].dtype))
    for level in (3, 2, 1):
        field = grids[level - 1]
        potential = periodic_convolve(field, stencil_full(level, field.shape, field.dtype)) + prolong_grid(potential)
    flat_potential = potential.reshape(-1)
    atom_values = jnp.zeros_like(charges)
    for flat, product in flat_points:
        atom_values = atom_values + product * flat_potential[flat]
    return (potential, atom_values)
```

```python
import functools

import jax
import jax.numpy as jnp
import numpy as np
from jax import lax
from jax.experimental import pallas as pl
from jax.experimental.pallas import tpu as pltpu
from jax.sharding import PartitionSpec as P

CX = 32
CY = 16
NZ = 128
ATOMS_DEV = 16384
N_GX = 8
N_GY = 32
PLANE = ATOMS_DEV // CX
EX = CX + 3
EY = 24
MESH_IDS = pl.DeviceIdType.MESH
BF16 = jnp.bfloat16
F32 = jnp.float32
taps = ((-3, -0.0625), (-1, 0.5625), (0, 1.0), (1, 0.5625), (3, -0.0625))


def smooth_numpy(rho):
    return np.where(
        rho < 1.0, 1.875 - 1.25 * rho * rho + 0.375 * rho**4, 1.0 / np.maximum(rho, 1.0)
    )


def frequencies(count):
    inner = np.repeat(np.arange(1, count // 2), 2)
    return np.concatenate([[0], inner, [count // 2]])


def real_basis(count):
    wave = frequencies(count)
    angle = 2.0 * np.pi * wave[:, None] * np.arange(count)[None, :] / count
    is_sine = np.zeros(count, bool)
    is_sine[2:-1:2] = True
    basis = np.where(is_sine[:, None], np.sin(angle), np.cos(angle)) * np.sqrt(2.0 / count)
    basis[0] /= np.sqrt(2.0)
    basis[-1] /= np.sqrt(2.0)
    return basis


def restriction(count):
    matrix = np.zeros((count // 2, count))
    for row in range(count // 2):
        for offset, weight in taps:
            matrix[row, (2 * row + offset) % count] += weight
    return matrix


def stencil_table(level, extent):
    offsets = np.arange(-3, 4) * 1.0
    radius = np.sqrt(
        offsets[:, None, None] ** 2 + offsets[None, :, None] ** 2 + offsets[None, None, :] ** 2
    )
    stencil = (smooth_numpy(radius / 1.5) / 1.5 - smooth_numpy(radius / 3.0) / 3.0) / 2.0 ** (
        level - 1
    )
    waves = np.cos(2.0 * np.pi * offsets[:, None] * frequencies(extent)[None, :] / extent)
    table = np.zeros((16, 128))
    table[:, :extent] = (stencil[3:, 3:] @ waves).reshape(16, extent)
    return table.astype(np.float32)


def placed_at(block, row, column):
    matrix = np.zeros((128, 128))
    matrix[row : row + block.shape[0], column : column + block.shape[1]] = block
    return matrix


(
    C_M12,
    C_M23,
    C_BD0,
    C_BD1,
    C_NZ0,
    C_NZ1,
    C_M23T,
    C_M12T,
    C_UR,
    C_PU,
) = (0, 1, 5, 6, 7, 8, 9, 10, 11, 12)


@functools.cache
def split_constants():
    def down(count):
        return (real_basis(count // 2) @ restriction(count) @ real_basis(count).T).T

    m12, m23, m34 = down(128), down(64), down(32)
    stack = [placed_at(m12, 0, 0)]
    stack += [placed_at(m23, 0, 32 * place) for place in range(4)]
    for half in range(2):
        matrix = np.zeros((128, 128))
        for place in range(4):
            matrix += placed_at(m34, 32 * place, 64 * half + 16 * place)
        stack.append(matrix)
    for half in range(2):
        matrix = np.zeros((128, 128))
        for place in range(4):
            matrix += placed_at(m34.T, 64 * half + 16 * place, 0)
        stack.append(matrix)
    stack += [placed_at(m23.T, 0, 0), placed_at(m12.T, 0, 0)]
    along_x = restriction(64)
    columns = (np.arange(64) - 8) % 64
    stack.append(placed_at((real_basis(32) @ along_x)[:, columns], 0, 0))
    rows = (np.arange(16) - 2) % 64
    stack.append(placed_at((real_basis(32) @ along_x).T[rows], 0, 0))
    return split_pair(np.stack(stack))


def split_pair(matrix):
    high = matrix.astype(np.float32).astype(BF16)
    low = (matrix - high.astype(np.float64)).astype(np.float32).astype(BF16)
    return high, low


@functools.cache
def coarse_table():
    counts = (32, 64, 16)
    signed = [np.where(np.arange(c) > c // 2, np.arange(c) - c, np.arange(c)) for c in counts]
    radius = np.sqrt(
        signed[0][:, None, None] ** 2.0
        + signed[1][None, :, None] ** 2.0
        + signed[2][None, None, :] ** 2.0
    )
    kernel = smooth_numpy(radius / 1.5) / 12.0
    wave_x = np.cos(2.0 * np.pi * np.outer(frequencies(32), np.arange(32)) / 32)
    wave_z = np.cos(2.0 * np.pi * np.outer(frequencies(16), np.arange(16)) / 16)
    along_y = np.einsum("ax,xyz,bz->aby", wave_x, kernel, wave_z)
    down_y = restriction(128)
    differ = (np.arange(64)[:, None] - np.arange(64)[None, :]) % 64
    up_rows = down_y.T[(np.arange(4) - 2) % 128]
    folded = np.einsum("cm,abmn->abcn", up_rows, along_y[:, :, differ])
    folded = np.einsum("abcn,ny->abcy", folded, down_y)
    folded = folded.reshape(2, 16, 16, 4, 32, 4).transpose(3, 4, 1, 0, 5, 2)
    folded = folded.reshape(4, 32, 16, 128)
    extended = folded[:, (np.arange(34) - 2) % 32]
    return extended.astype(np.float32)


def split(value):
    high = value.astype(BF16)
    low = (value - high.astype(F32)).astype(BF16)
    return high, low


def mm(a, b):
    return jnp.dot(a, b, preferred_element_type=F32)


def times_const(value, high_w, low_w):
    high, low = split(value)
    return mm(high, high_w) + (mm(low, high_w) + mm(high, low_w))


def const_times(high_w, low_w, value):
    high, low = split(value)
    return mm(high_w, high) + (mm(high_w, low) + mm(low_w, high))


def spline_weights(frac):
    def near_weight(distance):
        return (1.0 - distance) * (1.0 + distance - 1.5 * distance * distance)

    def far_weight(distance):
        return -0.5 * (distance - 1.0) * (2.0 - distance) * (2.0 - distance)

    return (
        far_weight(1.0 + frac),
        near_weight(frac),
        near_weight(1.0 - frac),
        far_weight(2.0 - frac),
    )


def tap_table(distance, weights):
    result = jnp.zeros(distance.shape, F32)
    for tap in range(4):
        result = jnp.where(distance == tap, weights[tap], result)
    return result


def plane_tables(plane, fraction_ref, cell_ref, index_y):
    lanes = pl.ds(pl.multiple_of(plane * PLANE, PLANE), PLANE)
    weights = spline_weights(fraction_ref[:, lanes])
    cells = cell_ref[:, lanes]
    base_y = (cells[0:1] - (index_y * CY + 1)) & (CY * N_GY - 1)
    base_z = cells[1:2] - 1
    places_y = lax.broadcasted_iota(jnp.int32, (EY, PLANE), 0)
    places_z = lax.broadcasted_iota(jnp.int32, (NZ, PLANE), 0)
    table_y = tap_table(places_y - base_y, [w[1:2] for w in weights])
    table_z = tap_table((places_z - base_z) & (NZ - 1), [w[2:3] for w in weights])
    return lanes, [w[0:1] for w in weights], table_y, table_z


def deposit_kernel(charge_ref, fraction_ref, cell_ref, high_ref, low_ref, grid_ref, edge_ref, sums):
    index_y = lax.axis_index("gy")
    sums[...] = jnp.zeros_like(sums)

    def step(plane, carried):
        lanes, along_x, table_y, table_z = plane_tables(plane, fraction_ref, cell_ref, index_y)
        charge = charge_ref[:, lanes]
        spread = jnp.concatenate([table_y * (w * charge) for w in along_x], axis=0)
        spread_high, spread_low = split(spread)
        z_high, z_low = split(table_z)
        dims = (((1,), (1,)), ((), ()))
        both = jnp.concatenate([spread_high, spread_low], axis=0)
        first = lax.dot_general(both, z_high, dims, preferred_element_type=F32)
        second = lax.dot_general(spread_high, z_low, dims, preferred_element_type=F32)
        contrib = first[: 4 * EY] + first[4 * EY :] + second
        for tap in range(4):
            sums[plane + tap] = sums[plane + tap] + contrib[EY * tap : EY * (tap + 1)]
        return carried

    lax.fori_loop(0, CX, step, 0)
    flat = sums[...].reshape(EX * EY, NZ)
    grid_ref[...] = times_const(flat, high_ref[...], low_ref[...]).reshape(EX, EY, NZ)
    edge_ref[...] = grid_ref[:, 11:19, :]


def sample_kernel(
    field_ref, fraction_ref, cell_ref, high_ref, low_ref, grid_ref, atom_ref, window_ref
):
    index_y = lax.axis_index("gy")
    flat = field_ref[...].reshape(EX * EY, NZ)
    window_ref[...] = times_const(flat, high_ref[...], low_ref[...]).reshape(EX, EY, NZ)
    grid_ref[...] = window_ref[:CX, :CY, :]

    def step(plane, carried):
        lanes, along_x, table_y, table_z = plane_tables(plane, fraction_ref, cell_ref, index_y)
        window = window_ref[pl.ds(plane, 4)].reshape(4 * EY, NZ)
        high, low = split(window)
        z_high, z_low = split(table_z)
        projected = mm(
            jnp.concatenate([high, low], axis=1), jnp.concatenate([z_high, z_high], axis=0)
        ) + mm(high, z_low)
        total = jnp.zeros((EY, PLANE), F32)
        for tap in range(4):
            total = total + along_x[tap] * projected[EY * tap : EY * (tap + 1)]
        atom_ref[:, lanes] = jnp.sum(total * table_y, axis=0, keepdims=True)
        return carried

    lax.fori_loop(0, CX, step, 0)


NEIGHBOURS = ((1, 0), (-1, 0), (0, 1), (0, -1), (1, 1), (1, -1), (-1, 1), (-1, -1))
N_SEMS = 8 + 8 + 7 + 4 + 31


def prolonged_rows(get, row):
    middle = row // 2
    if row % 2 == 0:
        return get(middle)
    return 0.5625 * (get(middle) + get(middle + 1)) - 0.0625 * (get(middle - 1) + get(middle + 2))


def levels_kernel(
    own_ref,
    edge_ref,
    k1_ref,
    k2_ref,
    k3_ref,
    high_ref,
    low_ref,
    table_hbm,
    out_ref,
    from_x,
    from_y,
    from_corner,
    q1,
    sums1,
    smooth1,
    part1,
    q2,
    smooth2,
    part2,
    ring_x,
    halo,
    ring_y,
    q3,
    field3,
    up3,
    up2,
    table,
    table_sem,
    send_sems,
    recv_sems,
):
    index_x = lax.axis_index("gx")
    index_y = lax.axis_index("gy")

    def device(step_x, step_y):
        return (
            lax.rem(index_x + (step_x + N_GX), N_GX),
            lax.rem(index_y + (step_y + N_GY), N_GY),
        )

    table_copy = pltpu.make_async_copy(table_hbm, table, table_sem)
    table_copy.start()

    barrier = pltpu.get_barrier_semaphore()
    peers = [(x, 0) for x in range(1, N_GX)] + [(0, y) for y in range(1, N_GY)]
    peers += [(x, y) for x, y in NEIGHBOURS if x and y]
    for step_x, step_y in peers:
        pl.semaphore_signal(
            barrier, inc=1, device_id=device(step_x, step_y), device_id_type=MESH_IDS
        )
    pl.semaphore_wait(barrier, len(peers))

    started = []

    def send(number, source, target, step_x, step_y):
        copy = pltpu.make_async_remote_copy(
            src_ref=source,
            dst_ref=target,
            send_sem=send_sems.at[number],
            recv_sem=recv_sems.at[number],
            device_id=device(step_x, step_y),
            device_id_type=MESH_IDS,
        )
        copy.start()
        started.append(copy)
        return copy

    low_x, high_x = pl.ds(0, 6), pl.ds(29, 6)
    round1 = [
        send(0, own_ref.at[high_x], from_x.at[0], 1, 0),
        send(1, own_ref.at[low_x], from_x.at[1], -1, 0),
        send(2, edge_ref, from_y.at[0], 0, 1),
        send(3, own_ref.at[:, 0:8, :], from_y.at[1], 0, -1),
        send(4, edge_ref.at[high_x], from_corner.at[0], 1, 1),
        send(5, own_ref.at[high_x, 0:8, :], from_corner.at[1], 1, -1),
        send(6, edge_ref.at[low_x], from_corner.at[2], -1, 1),
        send(7, own_ref.at[low_x, 0:8, :], from_corner.at[3], -1, -1),
    ]

    zero_tile = jnp.zeros((8, NZ), F32)

    def clear(x, carried):
        q1[x, 0:8, :] = zero_tile
        q1[x, 32:40, :] = zero_tile
        return carried

    lax.fori_loop(0, 41, clear, 0)
    for x in (0, 1, 2, 38, 39, 40):
        q1[x, 8:32, :] = jnp.zeros((EY, NZ), F32)

    def copy_own(x, carried):
        q1[x + 3, 8:32, :] = own_ref[x]
        return carried

    lax.fori_loop(0, EX, copy_own, 0)
    q2[:, 24:32, :] = jnp.zeros((26, 8, NZ), F32)
    q3[:, 24:32, :] = jnp.zeros((15, 8, NZ), F32)

    for copy in round1:
        copy.wait_recv()

    def add_y(x, carried):
        q1[x + 3, 3:11, :] = q1[x + 3, 3:11, :] + from_y[0, x]
        q1[x + 3, 24:32, :] = q1[x + 3, 24:32, :] + from_y[1, x]
        return carried

    lax.fori_loop(0, EX, add_y, 0)
    for side, start in ((0, 0), (1, 35)):
        for x in range(6):
            row = start + x
            q1[row, 8:32, :] = q1[row, 8:32, :] + from_x[side, x]
            q1[row, 3:11, :] = q1[row, 3:11, :] + from_corner[2 * side, x]
            q1[row, 24:32, :] = q1[row, 24:32, :] + from_corner[2 * side + 1, x]

    def restrict_y(x, carried):
        total = jnp.zeros((8, NZ), F32)
        for offset, weight in taps:
            total = total + weight * q1[x, pl.ds(8 + offset, 8, stride=2), :]
        part1[x] = total
        return carried

    lax.fori_loop(0, 37, restrict_y, 0)
    rows = []
    for m in range(16):
        total = jnp.zeros((8, NZ), F32)
        for offset, weight in taps:
            total = total + weight * part1[2 * m + 3 + offset]
        rows.append(total)
    level2 = times_const(jnp.concatenate(rows, axis=0), high_ref[C_M12], low_ref[C_M12])
    q2[4:20, 8:16, :] = level2.reshape(16, 8, NZ)

    round2 = []
    for number, (step_x, step_y) in enumerate(NEIGHBOURS):
        source_x, target_x, count = {0: (4, 4, 16), 1: (16, 0, 4), -1: (4, 20, 6)}[step_x]
        target_y = {0: 8, 1: 0, -1: 16}[step_y]
        round2.append(
            send(
                8 + number,
                q2.at[pl.ds(source_x, count), 8:16, :],
                q2.at[pl.ds(target_x, count), pl.ds(target_y, 8), :],
                step_x,
                step_y,
            )
        )

    def sum_y(x, carried):
        for dy in range(1, 4):
            sums1[dy - 1, x] = q1[x, 8 + dy : 32 + dy, :] + q1[x, 8 - dy : 32 - dy, :]
        return carried

    lax.fori_loop(0, 41, sum_y, 0)

    def stencil1(x, carried):
        total = jnp.zeros((EY, NZ), F32)
        for dy in range(4):
            for dx in range(4):
                if dy == 0:
                    value = q1[x + 3 + dx, 8:32, :]
                    if dx:
                        value = value + q1[x + 3 - dx, 8:32, :]
                else:
                    value = sums1[dy - 1, x + 3 + dx]
                    if dx:
                        value = value + sums1[dy - 1, x + 3 - dx]
                total = total + k1_ref[4 * dx + dy : 4 * dx + dy + 1, :] * value
        smooth1[x] = total
        return carried

    lax.fori_loop(0, EX, stencil1, 0)

    for copy in round2:
        copy.wait_recv()

    for m in range(8):
        total = jnp.zeros((24, NZ), F32)
        for offset, weight in taps:
            total = total + weight * q2[2 * m + 4 + offset, 0:24, :]
        part2[24 * m : 24 * (m + 1), :] = total
    tile = jnp.zeros((8, NZ), F32)
    for n in range(4):
        total = jnp.zeros((8, NZ), F32)
        for offset, weight in taps:
            total = total + weight * part2[pl.ds(8 + 2 * n + offset, 8, stride=24), :]
        tile = tile + times_const(total, high_ref[C_M23 + n], low_ref[C_M23 + n])
    ring_x[1] = tile

    round3 = []
    for step in range(1, N_GX):
        place = (N_GX - step + 1) % N_GX
        round3.append(send(15 + step, ring_x.at[1], ring_x.at[place], step, 0))

    def stencil_small(source, row, start, count, k_ref):
        total = jnp.zeros((count, NZ), F32)
        for across in range(4):
            for along in range(4):
                value = None
                for sign_r in sorted({across, -across}):
                    for sign_s in sorted({along, -along}):
                        piece = source[row + sign_r, start + sign_s : start + sign_s + count, :]
                        value = piece if value is None else value + piece
                total = total + k_ref[4 * across + along : 4 * across + along + 1, :] * value
        return total

    def stencil2(x, carried):
        smooth2[x] = stencil_small(q2, x + 3, 7, 16, k2_ref)
        return carried

    lax.fori_loop(0, 20, stencil2, 0)

    for copy in round3:
        copy.wait_recv()

    round4 = []
    for number, step in enumerate((1, -1, 2, -2)):
        round4.append(send(23 + number, ring_x.at[0:3], halo.at[2 - step], 0, step))
    column = const_times(
        high_ref[C_UR, 0:32, 0:64], low_ref[C_UR, 0:32, 0:64], ring_x[...].reshape(64, NZ)
    )
    ring_y[0] = times_const(column[0:16], high_ref[C_BD0], low_ref[C_BD0]) + times_const(
        column[16:32], high_ref[C_BD1], low_ref[C_BD1]
    )
    round5 = []
    for step in range(1, N_GY):
        round5.append(send(26 + step, ring_y.at[0], ring_y.at[N_GY - step], 0, step))

    halo[2] = ring_x[0:3]
    for copy in round4:
        copy.wait_recv()
    for y in range(-5, 10):
        place = y % 4
        source = halo[y // 4 + 2].reshape(24, NZ)
        if place:
            source = pltpu.roll(source, NZ - 32 * place, axis=1)
        q3[y + 5, 0:24, :] = source

    def stencil3(y, carried):
        field3[y] = stencil_small(q3, y + 3, 6, 16, k3_ref)
        return carried

    lax.fori_loop(0, 9, stencil3, 0)

    table_copy.wait()
    for copy in round5:
        copy.wait_recv()
    coarse = []
    for row in range(9):
        kind, shift = row % 4, row // 4

        def add_slot(slot, total, kind=kind, shift=shift):
            return total + table[kind, slot + 2 - shift] * ring_y[slot]

        coarse.append(lax.fori_loop(0, N_GY, add_slot, jnp.zeros((16, NZ), F32), unroll=4))
    coarse = jnp.concatenate(coarse, axis=0)
    half0 = times_const(coarse, high_ref[C_NZ0], low_ref[C_NZ0])
    half1 = times_const(coarse, high_ref[C_NZ1], low_ref[C_NZ1])
    for row in range(9):
        both = jnp.concatenate(
            [half0[16 * row : 16 * (row + 1)], half1[16 * row : 16 * (row + 1)]], axis=0
        )
        field3[row] = field3[row] + const_times(
            high_ref[C_PU, 0:16, 0:32], low_ref[C_PU, 0:16, 0:32], both
        )

    fields = [prolonged_rows(lambda m: field3[m + 2], y) for y in range(-1, 11)]
    up3[...] = times_const(jnp.concatenate(fields, axis=0), high_ref[C_M23T], low_ref[C_M23T])

    def column3(m):
        return up3[pl.ds(m + 2, 12, stride=16), :]

    for x in range(-1, 19):
        smooth2[x + 1, 0:12, :] = smooth2[x + 1, 0:12, :] + prolonged_rows(column3, x)

    part = times_const(
        smooth2[...].reshape(20 * 16, NZ), high_ref[C_M12T], low_ref[C_M12T]
    ).reshape(20, 16, NZ)
    smooth2[...] = part

    def widen_y(x, carried):
        rows = [smooth2[x, n : n + 12, :] for n in range(4)]
        up2[x, pl.ds(0, 12, stride=2), :] = rows[1]
        up2[x, pl.ds(1, 12, stride=2), :] = 0.5625 * (rows[1] + rows[2]) - 0.0625 * (
            rows[0] + rows[3]
        )
        return carried

    lax.fori_loop(0, 20, widen_y, 0)

    def widen_x(m, carried):
        values = [up2[m + n] for n in range(4)]
        out_ref[2 * m] = smooth1[2 * m] + values[1]
        out_ref[2 * m + 1] = smooth1[2 * m + 1] + (
            0.5625 * (values[1] + values[2]) - 0.0625 * (values[0] + values[3])
        )
        return carried

    lax.fori_loop(0, 17, widen_x, 0)
    out_ref[34] = smooth1[34] + up2[18]

    for copy in started:
        copy.wait_send()


def in_vmem(count):
    return [pl.BlockSpec(memory_space=pltpu.VMEM)] * count


def local(charges, fractions, cells):
    charge = charges.reshape(1, ATOMS_DEV)
    fraction = fractions.reshape(3, ATOMS_DEV)
    cell = cells.reshape(2, ATOMS_DEV)
    forward = [jnp.asarray(part) for part in split_pair(real_basis(NZ).T)]
    inverse = [jnp.asarray(part) for part in split_pair(real_basis(NZ))]
    block = jax.ShapeDtypeStruct((EX, EY, NZ), F32)

    own, edge = pl.pallas_call(
        deposit_kernel,
        out_shape=(block, jax.ShapeDtypeStruct((EX, 8, NZ), F32)),
        in_specs=in_vmem(5),
        out_specs=in_vmem(2),
        scratch_shapes=[pltpu.VMEM((EX, EY, NZ), F32)],
        name="deposit",
    )(charge, fraction, cell, *forward)

    high, low = split_constants()
    field = pl.pallas_call(
        levels_kernel,
        out_shape=block,
        in_specs=in_vmem(7) + [pl.BlockSpec(memory_space=pl.ANY)],
        out_specs=pl.BlockSpec(memory_space=pltpu.VMEM),
        scratch_shapes=[
            pltpu.VMEM((2, 6, EY, NZ), F32),
            pltpu.VMEM((2, EX, 8, NZ), F32),
            pltpu.VMEM((4, 6, 8, NZ), F32),
            pltpu.VMEM((41, 40, NZ), F32),
            pltpu.VMEM((3, 41, EY, NZ), F32),
            pltpu.VMEM((EX, EY, NZ), F32),
            pltpu.VMEM((37, 8, NZ), F32),
            pltpu.VMEM((26, 32, NZ), F32),
            pltpu.VMEM((20, 16, NZ), F32),
            pltpu.VMEM((8 * 24, NZ), F32),
            pltpu.VMEM((N_GX, 8, NZ), F32),
            pltpu.VMEM((5, 3, 8, NZ), F32),
            pltpu.VMEM((N_GY, 16, NZ), F32),
            pltpu.VMEM((15, 32, NZ), F32),
            pltpu.VMEM((9, 16, NZ), F32),
            pltpu.VMEM((12 * 16, NZ), F32),
            pltpu.VMEM((20, EY, NZ), F32),
            pltpu.VMEM((4, 34, 16, NZ), F32),
            pltpu.SemaphoreType.DMA,
            pltpu.SemaphoreType.DMA((N_SEMS,)),
            pltpu.SemaphoreType.DMA((N_SEMS,)),
        ],
        compiler_params=pltpu.CompilerParams(collective_id=0, has_side_effects=True),
        name="levels",
    )(
        own,
        edge,
        jnp.asarray(stencil_table(1, 128)),
        jnp.asarray(stencil_table(2, 64)),
        jnp.asarray(stencil_table(3, 32)),
        jnp.asarray(high),
        jnp.asarray(low),
        jnp.asarray(coarse_table()),
    )

    potential, sampled = pl.pallas_call(
        sample_kernel,
        out_shape=(
            jax.ShapeDtypeStruct((CX, CY, NZ), F32),
            jax.ShapeDtypeStruct((1, ATOMS_DEV), F32),
        ),
        in_specs=in_vmem(5),
        out_specs=in_vmem(2),
        scratch_shapes=[pltpu.VMEM((EX, EY, NZ), F32)],
        name="sample",
    )(field, fraction, cell, *inverse)
    return potential, sampled.reshape(1, 1, ATOMS_DEV)


def solution(mesh):
    placed = (P("gx", "gy", None), P("gx", "gy", None, None), P("gx", "gy", None, None))
    return jax.shard_map(
        local,
        mesh=mesh,
        in_specs=placed,
        out_specs=(P("gx", "gy", None), P("gx", "gy", None)),
        check_vma=False,
    )
```

```python
import functools

import jax
import jax.numpy as jnp
import numpy as np
from jax import lax
from jax.experimental import pallas as pl
from jax.experimental.pallas import tpu as pltpu
from jax.sharding import PartitionSpec as P

CX = 32
CY = 16
NZ = 128
ATOMS_DEV = 16384
N_GX = 8
N_GY = 32
PLANE = ATOMS_DEV // CX
EX = CX + 3
EY = 24
MESH_IDS = pl.DeviceIdType.MESH
BF16 = jnp.bfloat16
F32 = jnp.float32
taps = ((-3, -0.0625), (-1, 0.5625), (0, 1.0), (1, 0.5625), (3, -0.0625))


def smooth_numpy(rho):
    return np.where(
        rho < 1.0, 1.875 - 1.25 * rho * rho + 0.375 * rho**4, 1.0 / np.maximum(rho, 1.0)
    )


def frequencies(count):
    inner = np.repeat(np.arange(1, count // 2), 2)
    return np.concatenate([[0], inner, [count // 2]])


def real_basis(count):
    wave = frequencies(count)
    angle = 2.0 * np.pi * wave[:, None] * np.arange(count)[None, :] / count
    is_sine = np.zeros(count, bool)
    is_sine[2:-1:2] = True
    basis = np.where(is_sine[:, None], np.sin(angle), np.cos(angle)) * np.sqrt(2.0 / count)
    basis[0] /= np.sqrt(2.0)
    basis[-1] /= np.sqrt(2.0)
    return basis


def restriction(count):
    matrix = np.zeros((count // 2, count))
    for row in range(count // 2):
        for offset, weight in taps:
            matrix[row, (2 * row + offset) % count] += weight
    return matrix


def stencil_table(level, extent):
    offsets = np.arange(-3, 4) * 1.0
    radius = np.sqrt(
        offsets[:, None, None] ** 2 + offsets[None, :, None] ** 2 + offsets[None, None, :] ** 2
    )
    stencil = (smooth_numpy(radius / 1.5) / 1.5 - smooth_numpy(radius / 3.0) / 3.0) / 2.0 ** (
        level - 1
    )
    waves = np.cos(2.0 * np.pi * offsets[:, None] * frequencies(extent)[None, :] / extent)
    table = np.zeros((16, 128))
    table[:, :extent] = (stencil[3:, 3:] @ waves).reshape(16, extent)
    return table.astype(np.float32)


def placed_at(block, row, column):
    matrix = np.zeros((128, 128))
    matrix[row : row + block.shape[0], column : column + block.shape[1]] = block
    return matrix


(
    C_M12,
    C_M23,
    C_BD0,
    C_BD1,
    C_NZ0,
    C_NZ1,
    C_M23T,
    C_M12T,
    C_UR,
    C_PU,
) = (0, 1, 5, 6, 7, 8, 9, 10, 11, 12)


@functools.cache
def split_constants():
    def down(count):
        return (real_basis(count // 2) @ restriction(count) @ real_basis(count).T).T

    m12, m23, m34 = down(128), down(64), down(32)
    stack = [placed_at(m12, 0, 0)]
    stack += [placed_at(m23, 0, 32 * place) for place in range(4)]
    for half in range(2):
        matrix = np.zeros((128, 128))
        for place in range(4):
            matrix += placed_at(m34, 32 * place, 64 * half + 16 * place)
        stack.append(matrix)
    for half in range(2):
        matrix = np.zeros((128, 128))
        for place in range(4):
            matrix += placed_at(m34.T, 64 * half + 16 * place, 0)
        stack.append(matrix)
    stack += [placed_at(m23.T, 0, 0), placed_at(m12.T, 0, 0)]
    along_x = restriction(64)
    columns = (np.arange(64) - 8) % 64
    stack.append(placed_at((real_basis(32) @ along_x)[:, columns], 0, 0))
    rows = (np.arange(16) - 2) % 64
    stack.append(placed_at((real_basis(32) @ along_x).T[rows], 0, 0))
    return split_pair(np.stack(stack))


def split_pair(matrix):
    high = matrix.astype(np.float32).astype(BF16)
    low = (matrix - high.astype(np.float64)).astype(np.float32).astype(BF16)
    return high, low


@functools.cache
def coarse_table():
    counts = (32, 64, 16)
    signed = [np.where(np.arange(c) > c // 2, np.arange(c) - c, np.arange(c)) for c in counts]
    radius = np.sqrt(
        signed[0][:, None, None] ** 2.0
        + signed[1][None, :, None] ** 2.0
        + signed[2][None, None, :] ** 2.0
    )
    kernel = smooth_numpy(radius / 1.5) / 12.0
    wave_x = np.cos(2.0 * np.pi * np.outer(frequencies(32), np.arange(32)) / 32)
    wave_z = np.cos(2.0 * np.pi * np.outer(frequencies(16), np.arange(16)) / 16)
    along_y = np.einsum("ax,xyz,bz->aby", wave_x, kernel, wave_z)
    down_y = restriction(128)
    differ = (np.arange(64)[:, None] - np.arange(64)[None, :]) % 64
    up_rows = down_y.T[(np.arange(4) - 2) % 128]
    folded = np.einsum("cm,abmn->abcn", up_rows, along_y[:, :, differ])
    folded = np.einsum("abcn,ny->abcy", folded, down_y)
    folded = folded.reshape(2, 16, 16, 4, 32, 4).transpose(3, 4, 1, 0, 5, 2)
    folded = folded.reshape(4, 32, 16, 128)
    extended = folded[:, (np.arange(34) - 2) % 32]
    return extended.astype(np.float32)


def split(value):
    high = value.astype(BF16)
    low = (value - high.astype(F32)).astype(BF16)
    return high, low


def mm(a, b):
    return jnp.dot(a, b, preferred_element_type=F32)


def times_const(value, high_w, low_w):
    high, low = split(value)
    return mm(high, high_w) + (mm(low, high_w) + mm(high, low_w))


def const_times(high_w, low_w, value):
    high, low = split(value)
    return mm(high_w, high) + (mm(high_w, low) + mm(low_w, high))


def spline_weights(frac):
    def near_weight(distance):
        return (1.0 - distance) * (1.0 + distance - 1.5 * distance * distance)

    def far_weight(distance):
        return -0.5 * (distance - 1.0) * (2.0 - distance) * (2.0 - distance)

    return (
        far_weight(1.0 + frac),
        near_weight(frac),
        near_weight(1.0 - frac),
        far_weight(2.0 - frac),
    )


def tap_table(distance, weights):
    result = jnp.zeros(distance.shape, F32)
    for tap in range(4):
        result = jnp.where(distance == tap, weights[tap], result)
    return result


def rows_of(row):
    packed = jnp.broadcast_to(row, (16, row.shape[1])).astype(BF16)
    return jnp.concatenate([packed] * (NZ // 16), axis=0)


def depth_tables(places_ref, base, weights):
    places = jnp.concatenate([places_ref[...]] * (base.shape[1] // 128), axis=1)
    high = low = jnp.zeros(places.shape, BF16)
    for tap in range(4):
        target = ((base + tap) & (NZ - 1)).astype(F32)
        here = places == rows_of(target)
        weight_high = weights[tap].astype(BF16).astype(F32)
        high = jnp.where(here, rows_of(weight_high), high)
        low = jnp.where(here, rows_of(weights[tap] - weight_high), low)
    return high, low


def plane_tables(plane, fraction_ref, cell_ref, places_ref, index_y):
    lanes = pl.ds(pl.multiple_of(plane * PLANE, PLANE), PLANE)
    fraction = jnp.concatenate([fraction_ref[k, :, lanes] for k in range(3)], axis=0)
    weights = spline_weights(fraction)
    cells = cell_ref[:, lanes]
    base_y = (cells[0:1] - (index_y * CY + 1)) & (CY * N_GY - 1)
    places_y = lax.broadcasted_iota(jnp.int32, (EY, PLANE), 0)
    table_y = tap_table(places_y - base_y, [w[1:2] for w in weights])
    tables_z = depth_tables(places_ref, cells[1:2] - 1, [w[2:3] for w in weights])
    return lanes, [w[0:1] for w in weights], table_y, tables_z


def deposit_plane(plane, charge_ref, fraction_ref, cell_ref, places_ref, sums, index_y):
    lanes, along_x, table_y, (z_high, z_low) = plane_tables(
        plane, fraction_ref, cell_ref, places_ref, index_y
    )
    charge = charge_ref[:, lanes]
    spread = jnp.concatenate([table_y * (w * charge) for w in along_x], axis=0)
    spread_high, spread_low = split(spread)
    dims = (((1,), (1,)), ((), ()))
    both = jnp.concatenate([spread_high, spread_low], axis=0)
    first = lax.dot_general(both, z_high, dims, preferred_element_type=F32)
    second = lax.dot_general(spread_high, z_low, dims, preferred_element_type=F32)
    contrib = first[: 4 * EY] + first[4 * EY :] + second
    for tap in range(4):
        sums[plane + tap] = sums[plane + tap] + contrib[EY * tap : EY * (tap + 1)]


def sample_kernel(
    field_ref,
    fraction_ref,
    cell_ref,
    places_ref,
    high_ref,
    low_ref,
    grid_ref,
    atom_ref,
    window_ref,
):
    index_y = lax.axis_index("gy")
    flat = field_ref[...].reshape(EX * EY, NZ)
    window_ref[...] = times_const(flat, high_ref[...], low_ref[...]).reshape(EX, EY, NZ)
    grid_ref[...] = window_ref[:CX, :CY, :]

    def step(plane, carried):
        lanes, along_x, table_y, (z_high, z_low) = plane_tables(
            plane, fraction_ref, cell_ref, places_ref, index_y
        )
        window = window_ref[pl.ds(plane, 4)].reshape(4 * EY, NZ)
        high, low = split(window)
        projected = mm(
            jnp.concatenate([high, low], axis=1), jnp.concatenate([z_high, z_high], axis=0)
        ) + mm(high, z_low)
        total = jnp.zeros((EY, PLANE), F32)
        for tap in range(4):
            total = total + along_x[tap] * projected[EY * tap : EY * (tap + 1)]
        atom_ref[:, lanes] = jnp.sum(total * table_y, axis=0, keepdims=True)
        return carried

    lax.fori_loop(0, CX, step, 0, unroll=2)


NEIGHBOURS = ((1, 0), (-1, 0), (0, 1), (0, -1), (1, 1), (1, -1), (-1, 1), (-1, -1))
N_SEMS = 16 + 8 + 7 + 4 + 31


def prolonged_rows(get, row):
    middle = row // 2
    if row % 2 == 0:
        return get(middle)
    return 0.5625 * (get(middle) + get(middle + 1)) - 0.0625 * (get(middle - 1) + get(middle + 2))


def levels_kernel(
    charge_ref,
    fraction_ref,
    cell_ref,
    places_ref,
    forward_high_ref,
    forward_low_ref,
    k1_ref,
    k2_ref,
    k3_ref,
    high_ref,
    low_ref,
    table_hbm,
    out_ref,
    sums,
    own,
    edge,
    from_x,
    from_y,
    from_corner,
    q1,
    sums1,
    smooth1,
    part1,
    q2,
    smooth2,
    part2,
    ring_x,
    halo,
    ring_y,
    q3,
    field3,
    up3,
    up2,
    table,
    table_sem,
    send_sems,
    recv_sems,
):
    index_x = lax.axis_index("gx")
    index_y = lax.axis_index("gy")

    def device(step_x, step_y):
        return (
            lax.rem(index_x + (step_x + N_GX), N_GX),
            lax.rem(index_y + (step_y + N_GY), N_GY),
        )

    table_copy = pltpu.make_async_copy(table_hbm, table, table_sem)
    table_copy.start()

    barrier = pltpu.get_barrier_semaphore()
    peers = [(x, 0) for x in range(1, N_GX)] + [(0, y) for y in range(1, N_GY)]
    peers += [(x, y) for x, y in NEIGHBOURS if x and y]
    for step_x, step_y in peers:
        pl.semaphore_signal(
            barrier, inc=1, device_id=device(step_x, step_y), device_id_type=MESH_IDS
        )

    started = []

    def send(number, source, target, step_x, step_y):
        copy = pltpu.make_async_remote_copy(
            src_ref=source,
            dst_ref=target,
            send_sem=send_sems.at[number],
            recv_sem=recv_sems.at[number],
            device_id=device(step_x, step_y),
            device_id_type=MESH_IDS,
        )
        copy.start()
        started.append(copy)
        return copy

    sums[...] = jnp.zeros_like(sums)

    def deposit(first, last, row, count):
        def step(plane, carried):
            deposit_plane(
                plane, charge_ref, fraction_ref, cell_ref, places_ref, sums, index_y
            )
            return carried

        lax.fori_loop(first, last, step, 0, unroll=2)
        flat = sums[row : row + count].reshape(count * EY, NZ)
        value = times_const(flat, forward_high_ref[...], forward_low_ref[...])
        own[row : row + count] = value.reshape(count, EY, NZ)
        edge[row : row + count] = own[row : row + count, 11:19, :]

    round1 = []

    def send_edges(number, row, count):
        rows = pl.ds(row, count)
        round1.append(send(number, edge.at[rows], from_y.at[0, rows], 0, 1))
        round1.append(send(number + 1, own.at[rows, 0:8, :], from_y.at[1, rows], 0, -1))

    deposit(26, 32, 29, 6)
    pl.semaphore_wait(barrier, len(peers))
    high_x = pl.ds(29, 6)
    round1.append(send(0, edge.at[high_x], from_corner.at[0], 1, 1))
    round1.append(send(1, own.at[high_x, 0:8, :], from_corner.at[1], 1, -1))
    round1.append(send(2, own.at[high_x], from_x.at[0], 1, 0))
    send_edges(6, 29, 6)
    deposit(0, 6, 0, 6)
    low_x = pl.ds(0, 6)
    round1.append(send(3, edge.at[low_x], from_corner.at[2], -1, 1))
    round1.append(send(4, own.at[low_x, 0:8, :], from_corner.at[3], -1, -1))
    round1.append(send(5, own.at[low_x], from_x.at[1], -1, 0))
    send_edges(8, 0, 6)
    deposit(6, 14, 6, 8)
    send_edges(10, 6, 8)
    deposit(14, 22, 14, 8)
    send_edges(12, 14, 8)
    deposit(22, 26, 22, 7)
    send_edges(14, 22, 7)

    zero_tile = jnp.zeros((8, NZ), F32)

    def clear(x, carried):
        q1[x, 0:8, :] = zero_tile
        q1[x, 32:40, :] = zero_tile
        return carried

    lax.fori_loop(0, 41, clear, 0)
    for x in (0, 1, 2, 38, 39, 40):
        q1[x, 8:32, :] = jnp.zeros((EY, NZ), F32)

    def copy_own(x, carried):
        q1[x + 3, 8:32, :] = own[x]
        return carried

    lax.fori_loop(0, EX, copy_own, 0)
    q2[:, 24:32, :] = jnp.zeros((26, 8, NZ), F32)
    q3[:, 24:32, :] = jnp.zeros((15, 8, NZ), F32)

    for copy in round1:
        copy.wait_recv()

    def add_y(x, carried):
        q1[x + 3, 3:11, :] = q1[x + 3, 3:11, :] + from_y[0, x]
        q1[x + 3, 24:32, :] = q1[x + 3, 24:32, :] + from_y[1, x]
        return carried

    lax.fori_loop(0, EX, add_y, 0)
    for side, start in ((0, 0), (1, 35)):
        for x in range(6):
            row = start + x
            q1[row, 8:32, :] = q1[row, 8:32, :] + from_x[side, x]
            q1[row, 3:11, :] = q1[row, 3:11, :] + from_corner[2 * side, x]
            q1[row, 24:32, :] = q1[row, 24:32, :] + from_corner[2 * side + 1, x]

    def restrict_y(x, carried):
        total = jnp.zeros((8, NZ), F32)
        for offset, weight in taps:
            total = total + weight * q1[x, pl.ds(8 + offset, 8, stride=2), :]
        part1[x] = total
        return carried

    lax.fori_loop(0, 37, restrict_y, 0)
    rows = []
    for m in range(16):
        total = jnp.zeros((8, NZ), F32)
        for offset, weight in taps:
            total = total + weight * part1[2 * m + 3 + offset]
        rows.append(total)
    level2 = times_const(jnp.concatenate(rows, axis=0), high_ref[C_M12], low_ref[C_M12])
    q2[4:20, 8:16, :] = level2.reshape(16, 8, NZ)

    round2 = []
    for number, (step_x, step_y) in enumerate(NEIGHBOURS):
        source_x, target_x, count = {0: (4, 4, 16), 1: (16, 0, 4), -1: (4, 20, 6)}[step_x]
        target_y = {0: 8, 1: 0, -1: 16}[step_y]
        round2.append(
            send(
                16 + number,
                q2.at[pl.ds(source_x, count), 8:16, :],
                q2.at[pl.ds(target_x, count), pl.ds(target_y, 8), :],
                step_x,
                step_y,
            )
        )

    def sum_y(x, carried):
        for dy in range(1, 4):
            sums1[dy - 1, x] = q1[x, 8 + dy : 32 + dy, :] + q1[x, 8 - dy : 32 - dy, :]
        return carried

    lax.fori_loop(0, 41, sum_y, 0)

    def stencil1(x, carried):
        total = jnp.zeros((EY, NZ), F32)
        for dy in range(4):
            for dx in range(4):
                if dy == 0:
                    value = q1[x + 3 + dx, 8:32, :]
                    if dx:
                        value = value + q1[x + 3 - dx, 8:32, :]
                else:
                    value = sums1[dy - 1, x + 3 + dx]
                    if dx:
                        value = value + sums1[dy - 1, x + 3 - dx]
                total = total + k1_ref[4 * dx + dy : 4 * dx + dy + 1, :] * value
        smooth1[x] = total
        return carried

    lax.fori_loop(0, EX, stencil1, 0)

    for copy in round2:
        copy.wait_recv()

    for m in range(8):
        total = jnp.zeros((24, NZ), F32)
        for offset, weight in taps:
            total = total + weight * q2[2 * m + 4 + offset, 0:24, :]
        part2[24 * m : 24 * (m + 1), :] = total
    tile = jnp.zeros((8, NZ), F32)
    for n in range(4):
        total = jnp.zeros((8, NZ), F32)
        for offset, weight in taps:
            total = total + weight * part2[pl.ds(8 + 2 * n + offset, 8, stride=24), :]
        tile = tile + times_const(total, high_ref[C_M23 + n], low_ref[C_M23 + n])
    ring_x[1] = tile

    round3 = []
    for step in range(1, N_GX):
        place = (N_GX - step + 1) % N_GX
        round3.append(send(23 + step, ring_x.at[1], ring_x.at[place], step, 0))

    def stencil_small(source, row, start, count, k_ref):
        total = jnp.zeros((count, NZ), F32)
        for across in range(4):
            for along in range(4):
                value = None
                for sign_r in sorted({across, -across}):
                    for sign_s in sorted({along, -along}):
                        piece = source[row + sign_r, start + sign_s : start + sign_s + count, :]
                        value = piece if value is None else value + piece
                total = total + k_ref[4 * across + along : 4 * across + along + 1, :] * value
        return total

    def stencil2(x, carried):
        smooth2[x] = stencil_small(q2, x + 3, 7, 16, k2_ref)
        return carried

    lax.fori_loop(0, 20, stencil2, 0)

    for copy in round3:
        copy.wait_recv()

    round4 = []
    for number, step in enumerate((1, -1, 2, -2)):
        round4.append(send(31 + number, ring_x.at[0:3], halo.at[2 - step], 0, step))
    column = const_times(
        high_ref[C_UR, 0:32, 0:64], low_ref[C_UR, 0:32, 0:64], ring_x[...].reshape(64, NZ)
    )
    ring_y[0] = times_const(column[0:16], high_ref[C_BD0], low_ref[C_BD0]) + times_const(
        column[16:32], high_ref[C_BD1], low_ref[C_BD1]
    )
    round5 = []
    for step in range(1, N_GY):
        round5.append(send(34 + step, ring_y.at[0], ring_y.at[N_GY - step], 0, step))

    halo[2] = ring_x[0:3]
    for copy in round4:
        copy.wait_recv()
    for y in range(-5, 10):
        place = y % 4
        source = halo[y // 4 + 2].reshape(24, NZ)
        if place:
            source = pltpu.roll(source, NZ - 32 * place, axis=1)
        q3[y + 5, 0:24, :] = source

    def stencil3(y, carried):
        field3[y] = stencil_small(q3, y + 3, 6, 16, k3_ref)
        return carried

    lax.fori_loop(0, 9, stencil3, 0)

    table_copy.wait()
    for copy in round5:
        copy.wait_recv()
    coarse = []
    for row in range(9):
        kind, shift = row % 4, row // 4

        def add_slot(slot, total, kind=kind, shift=shift):
            return total + table[kind, slot + 2 - shift] * ring_y[slot]

        coarse.append(lax.fori_loop(0, N_GY, add_slot, jnp.zeros((16, NZ), F32), unroll=4))
    coarse = jnp.concatenate(coarse, axis=0)
    half0 = times_const(coarse, high_ref[C_NZ0], low_ref[C_NZ0])
    half1 = times_const(coarse, high_ref[C_NZ1], low_ref[C_NZ1])
    for row in range(9):
        both = jnp.concatenate(
            [half0[16 * row : 16 * (row + 1)], half1[16 * row : 16 * (row + 1)]], axis=0
        )
        field3[row] = field3[row] + const_times(
            high_ref[C_PU, 0:16, 0:32], low_ref[C_PU, 0:16, 0:32], both
        )

    fields = [prolonged_rows(lambda m: field3[m + 2], y) for y in range(-1, 11)]
    up3[...] = times_const(jnp.concatenate(fields, axis=0), high_ref[C_M23T], low_ref[C_M23T])

    def column3(m):
        return up3[pl.ds(m + 2, 12, stride=16), :]

    for x in range(-1, 19):
        smooth2[x + 1, 0:12, :] = smooth2[x + 1, 0:12, :] + prolonged_rows(column3, x)

    part = times_const(
        smooth2[...].reshape(20 * 16, NZ), high_ref[C_M12T], low_ref[C_M12T]
    ).reshape(20, 16, NZ)
    smooth2[...] = part

    def widen_y(x, carried):
        rows = [smooth2[x, n : n + 12, :] for n in range(4)]
        up2[x, pl.ds(0, 12, stride=2), :] = rows[1]
        up2[x, pl.ds(1, 12, stride=2), :] = 0.5625 * (rows[1] + rows[2]) - 0.0625 * (
            rows[0] + rows[3]
        )
        return carried

    lax.fori_loop(0, 20, widen_y, 0)

    def widen_x(m, carried):
        values = [up2[m + n] for n in range(4)]
        out_ref[2 * m] = smooth1[2 * m] + values[1]
        out_ref[2 * m + 1] = smooth1[2 * m + 1] + (
            0.5625 * (values[1] + values[2]) - 0.0625 * (values[0] + values[3])
        )
        return carried

    lax.fori_loop(0, 17, widen_x, 0)
    out_ref[34] = smooth1[34] + up2[18]

    for copy in started:
        copy.wait_send()


def in_vmem(count):
    return [pl.BlockSpec(memory_space=pltpu.VMEM)] * count


def local(charges, fractions, cells):
    charge = charges.reshape(1, ATOMS_DEV)
    fraction = fractions.reshape(3, 1, ATOMS_DEV)
    cell = cells.reshape(2, ATOMS_DEV)
    places = jnp.asarray(np.tile(np.arange(NZ)[:, None], (1, 128)).astype(BF16))
    forward = [jnp.asarray(part) for part in split_pair(real_basis(NZ).T)]
    inverse = [jnp.asarray(part) for part in split_pair(real_basis(NZ))]
    block = jax.ShapeDtypeStruct((EX, EY, NZ), F32)

    high, low = split_constants()
    field = pl.pallas_call(
        levels_kernel,
        out_shape=block,
        in_specs=in_vmem(11) + [pl.BlockSpec(memory_space=pl.ANY)],
        out_specs=pl.BlockSpec(memory_space=pltpu.VMEM),
        scratch_shapes=[
            pltpu.VMEM((EX, EY, NZ), F32),
            pltpu.VMEM((EX, EY, NZ), F32),
            pltpu.VMEM((EX, 8, NZ), F32),
            pltpu.VMEM((2, 6, EY, NZ), F32),
            pltpu.VMEM((2, EX, 8, NZ), F32),
            pltpu.VMEM((4, 6, 8, NZ), F32),
            pltpu.VMEM((41, 40, NZ), F32),
            pltpu.VMEM((3, 41, EY, NZ), F32),
            pltpu.VMEM((EX, EY, NZ), F32),
            pltpu.VMEM((37, 8, NZ), F32),
            pltpu.VMEM((26, 32, NZ), F32),
            pltpu.VMEM((20, 16, NZ), F32),
            pltpu.VMEM((8 * 24, NZ), F32),
            pltpu.VMEM((N_GX, 8, NZ), F32),
            pltpu.VMEM((5, 3, 8, NZ), F32),
            pltpu.VMEM((N_GY, 16, NZ), F32),
            pltpu.VMEM((15, 32, NZ), F32),
            pltpu.VMEM((9, 16, NZ), F32),
            pltpu.VMEM((12 * 16, NZ), F32),
            pltpu.VMEM((20, EY, NZ), F32),
            pltpu.VMEM((4, 34, 16, NZ), F32),
            pltpu.SemaphoreType.DMA,
            pltpu.SemaphoreType.DMA((N_SEMS,)),
            pltpu.SemaphoreType.DMA((N_SEMS,)),
        ],
        compiler_params=pltpu.CompilerParams(collective_id=0, has_side_effects=True),
        name="levels",
    )(
        charge,
        fraction,
        cell,
        places,
        *forward,
        jnp.asarray(stencil_table(1, 128)),
        jnp.asarray(stencil_table(2, 64)),
        jnp.asarray(stencil_table(3, 32)),
        jnp.asarray(high),
        jnp.asarray(low),
        jnp.asarray(coarse_table()),
    )

    potential, sampled = pl.pallas_call(
        sample_kernel,
        out_shape=(
            jax.ShapeDtypeStruct((CX, CY, NZ), F32),
            jax.ShapeDtypeStruct((1, ATOMS_DEV), F32),
        ),
        in_specs=in_vmem(6),
        out_specs=in_vmem(2),
        scratch_shapes=[pltpu.VMEM((EX, EY, NZ), F32)],
        name="sample",
    )(field, fraction, cell, places, *inverse)
    return potential, sampled.reshape(1, 1, ATOMS_DEV)


def solution(mesh):
    placed = (P("gx", "gy", None), P("gx", "gy", None, None), P("gx", "gy", None, None))
    return jax.shard_map(
        local,
        mesh=mesh,
        in_specs=placed,
        out_specs=(P("gx", "gy", None), P("gx", "gy", None)),
        check_vma=False,
    )
```

```python
import functools

import jax
import jax.numpy as jnp
import numpy as np
from jax import lax
from jax.experimental import pallas as pl
from jax.experimental.pallas import tpu as pltpu
from jax.sharding import PartitionSpec as P

CX = 32
CY = 16
NZ = 128
ATOMS_DEV = 16384
N_GX = 8
N_GY = 32
PLANE = ATOMS_DEV // CX
EX = CX + 3
EY = 24
MESH_IDS = pl.DeviceIdType.MESH
BF16 = jnp.bfloat16
F32 = jnp.float32
taps = ((-3, -0.0625), (-1, 0.5625), (0, 1.0), (1, 0.5625), (3, -0.0625))


def smooth_numpy(rho):
    return np.where(
        rho < 1.0, 1.875 - 1.25 * rho * rho + 0.375 * rho**4, 1.0 / np.maximum(rho, 1.0)
    )


def frequencies(count):
    inner = np.repeat(np.arange(1, count // 2), 2)
    return np.concatenate([[0], inner, [count // 2]])


def real_basis(count):
    wave = frequencies(count)
    angle = 2.0 * np.pi * wave[:, None] * np.arange(count)[None, :] / count
    is_sine = np.zeros(count, bool)
    is_sine[2:-1:2] = True
    basis = np.where(is_sine[:, None], np.sin(angle), np.cos(angle)) * np.sqrt(2.0 / count)
    basis[0] /= np.sqrt(2.0)
    basis[-1] /= np.sqrt(2.0)
    return basis


def restriction(count):
    matrix = np.zeros((count // 2, count))
    for row in range(count // 2):
        for offset, weight in taps:
            matrix[row, (2 * row + offset) % count] += weight
    return matrix


def stencil_table(level, extent):
    offsets = np.arange(-3, 4) * 1.0
    radius = np.sqrt(
        offsets[:, None, None] ** 2 + offsets[None, :, None] ** 2 + offsets[None, None, :] ** 2
    )
    stencil = (smooth_numpy(radius / 1.5) / 1.5 - smooth_numpy(radius / 3.0) / 3.0) / 2.0 ** (
        level - 1
    )
    waves = np.cos(2.0 * np.pi * offsets[:, None] * frequencies(extent)[None, :] / extent)
    table = np.zeros((16, 128))
    table[:, :extent] = (stencil[3:, 3:] @ waves).reshape(16, extent)
    return table.astype(np.float32)


def placed_at(block, row, column):
    matrix = np.zeros((128, 128))
    matrix[row : row + block.shape[0], column : column + block.shape[1]] = block
    return matrix


(
    C_M12,
    C_M23,
    C_BD0,
    C_BD1,
    C_NZ0,
    C_NZ1,
    C_M23T,
    C_M12T,
    C_UR,
    C_PU,
    C_M12B,
) = (0, 1, 5, 6, 7, 8, 9, 10, 11, 12, 13)


@functools.cache
def split_constants():
    def down(count):
        return (real_basis(count // 2) @ restriction(count) @ real_basis(count).T).T

    m12, m23, m34 = down(128), down(64), down(32)
    stack = [placed_at(m12, 0, 0)]
    stack += [placed_at(m23, 0, 32 * place) for place in range(4)]
    for half in range(2):
        matrix = np.zeros((128, 128))
        for place in range(4):
            matrix += placed_at(m34, 32 * place, 64 * half + 16 * place)
        stack.append(matrix)
    for half in range(2):
        matrix = np.zeros((128, 128))
        for place in range(4):
            matrix += placed_at(m34.T, 64 * half + 16 * place, 0)
        stack.append(matrix)
    stack += [placed_at(m23.T, 0, 0), placed_at(m12.T, 0, 0)]
    along_x = restriction(64)
    columns = (np.arange(64) - 8) % 64
    stack.append(placed_at((real_basis(32) @ along_x)[:, columns], 0, 0))
    rows = (np.arange(16) - 2) % 64
    stack.append(placed_at((real_basis(32) @ along_x).T[rows], 0, 0))
    stack.append(placed_at(m12, 0, 64))
    return split_pair(np.stack(stack))


def split_pair(matrix):
    high = matrix.astype(np.float32).astype(BF16)
    low = (matrix - high.astype(np.float64)).astype(np.float32).astype(BF16)
    return high, low


@functools.cache
def coarse_table():
    counts = (32, 64, 16)
    signed = [np.where(np.arange(c) > c // 2, np.arange(c) - c, np.arange(c)) for c in counts]
    radius = np.sqrt(
        signed[0][:, None, None] ** 2.0
        + signed[1][None, :, None] ** 2.0
        + signed[2][None, None, :] ** 2.0
    )
    kernel = smooth_numpy(radius / 1.5) / 12.0
    wave_x = np.cos(2.0 * np.pi * np.outer(frequencies(32), np.arange(32)) / 32)
    wave_z = np.cos(2.0 * np.pi * np.outer(frequencies(16), np.arange(16)) / 16)
    along_y = np.einsum("ax,xyz,bz->aby", wave_x, kernel, wave_z)
    down_y = restriction(128)
    differ = (np.arange(64)[:, None] - np.arange(64)[None, :]) % 64
    up_rows = down_y.T[(np.arange(4) - 2) % 128]
    folded = np.einsum("cm,abmn->abcn", up_rows, along_y[:, :, differ])
    folded = np.einsum("abcn,ny->abcy", folded, down_y)
    folded = folded.reshape(2, 16, 16, 4, 32, 4).transpose(3, 4, 1, 0, 5, 2)
    folded = folded.reshape(4, 32, 16, 128)
    extended = folded[:, (np.arange(34) - 2) % 32]
    return extended.astype(np.float32)


def split(value):
    high = value.astype(BF16)
    low = (value - high.astype(F32)).astype(BF16)
    return high, low


def mm(a, b):
    return jnp.dot(a, b, preferred_element_type=F32)


def times_const(value, high_w, low_w):
    high, low = split(value)
    return mm(high, high_w) + (mm(low, high_w) + mm(high, low_w))


def const_times(high_w, low_w, value):
    high, low = split(value)
    return mm(high_w, high) + (mm(high_w, low) + mm(low_w, high))


def spline_weights(frac):
    def near_weight(distance):
        return (1.0 - distance) * (1.0 + distance - 1.5 * distance * distance)

    def far_weight(distance):
        return -0.5 * (distance - 1.0) * (2.0 - distance) * (2.0 - distance)

    return (
        far_weight(1.0 + frac),
        near_weight(frac),
        near_weight(1.0 - frac),
        far_weight(2.0 - frac),
    )


def tap_table(distance, weights):
    result = jnp.zeros(distance.shape, F32)
    for tap in range(4):
        result = jnp.where(distance == tap, weights[tap], result)
    return result


def rows_of(row):
    packed = jnp.broadcast_to(row, (16, row.shape[1])).astype(BF16)
    return jnp.concatenate([packed] * (NZ // 16), axis=0)


def depth_tables(places_ref, base, weights):
    places = jnp.concatenate([places_ref[...]] * (base.shape[1] // 128), axis=1)
    high = low = jnp.zeros(places.shape, BF16)
    for tap in range(4):
        target = ((base + tap) & (NZ - 1)).astype(F32)
        here = places == rows_of(target)
        weight_high = weights[tap].astype(BF16).astype(F32)
        high = jnp.where(here, rows_of(weight_high), high)
        low = jnp.where(here, rows_of(weights[tap] - weight_high), low)
    return high, low


def plane_tables(plane, fraction_ref, cell_ref, places_ref, index_y):
    lanes = pl.ds(pl.multiple_of(plane * PLANE, PLANE), PLANE)
    fraction = jnp.concatenate([fraction_ref[k, :, lanes] for k in range(3)], axis=0)
    weights = spline_weights(fraction)
    cells = cell_ref[:, lanes]
    base_y = (cells[0:1] - (index_y * CY + 1)) & (CY * N_GY - 1)
    places_y = lax.broadcasted_iota(jnp.int32, (EY, PLANE), 0)
    table_y = tap_table(places_y - base_y, [w[1:2] for w in weights])
    tables_z = depth_tables(places_ref, cells[1:2] - 1, [w[2:3] for w in weights])
    return lanes, [w[0:1] for w in weights], table_y, tables_z


def deposit_plane(plane, charge_ref, fraction_ref, cell_ref, places_ref, sums, index_y):
    lanes, along_x, table_y, (z_high, z_low) = plane_tables(
        plane, fraction_ref, cell_ref, places_ref, index_y
    )
    charge = charge_ref[:, lanes]
    spread = jnp.concatenate([table_y * (w * charge) for w in along_x], axis=0)
    spread_high, spread_low = split(spread)
    dims = (((1,), (1,)), ((), ()))
    both = jnp.concatenate([spread_high, spread_low], axis=0)
    first = lax.dot_general(both, z_high, dims, preferred_element_type=F32)
    second = lax.dot_general(spread_high, z_low, dims, preferred_element_type=F32)
    contrib = first[: 4 * EY] + first[4 * EY :] + second
    for tap in range(4):
        sums[plane + tap] = sums[plane + tap] + contrib[EY * tap : EY * (tap + 1)]


def sample_kernel(
    field_ref,
    fraction_ref,
    cell_ref,
    places_ref,
    high_ref,
    low_ref,
    grid_ref,
    atom_ref,
    window_ref,
):
    index_y = lax.axis_index("gy")
    flat = field_ref[...].reshape(EX * EY, NZ)
    window_ref[...] = times_const(flat, high_ref[...], low_ref[...]).reshape(EX, EY, NZ)
    grid_ref[...] = window_ref[:CX, :CY, :]

    def step(plane, carried):
        lanes, along_x, table_y, (z_high, z_low) = plane_tables(
            plane, fraction_ref, cell_ref, places_ref, index_y
        )
        window = window_ref[pl.ds(plane, 4)].reshape(4 * EY, NZ)
        high, low = split(window)
        projected = mm(
            jnp.concatenate([high, low], axis=1), jnp.concatenate([z_high, z_high], axis=0)
        ) + mm(high, z_low)
        total = jnp.zeros((EY, PLANE), F32)
        for tap in range(4):
            total = total + along_x[tap] * projected[EY * tap : EY * (tap + 1)]
        atom_ref[:, lanes] = jnp.sum(total * table_y, axis=0, keepdims=True)
        return carried

    lax.fori_loop(0, CX, step, 0, unroll=2)


NEIGHBOURS = ((1, 0), (-1, 0), (0, 1), (0, -1), (1, 1), (1, -1), (-1, 1), (-1, -1))
N_SEMS = 16 + 8 + 7 + 4 + 31


def prolonged_rows(get, row):
    middle = row // 2
    if row % 2 == 0:
        return get(middle)
    return 0.5625 * (get(middle) + get(middle + 1)) - 0.0625 * (get(middle - 1) + get(middle + 2))


def levels_kernel(
    charge_ref,
    fraction_ref,
    cell_ref,
    places_ref,
    forward_high_ref,
    forward_low_ref,
    k1_ref,
    k2_ref,
    k3_ref,
    high_ref,
    low_ref,
    table_hbm,
    out_ref,
    sums,
    own,
    edge,
    from_x,
    from_y,
    from_corner,
    from_x2,
    from_y2,
    from_corner2,
    own2,
    edge2,
    q1,
    sums1,
    smooth1,
    part1,
    q2,
    smooth2,
    part2,
    ring_x,
    halo,
    ring_y,
    q3,
    field3,
    up3,
    up2,
    table,
    table_sem,
    send_sems,
    recv_sems,
):
    index_x = lax.axis_index("gx")
    index_y = lax.axis_index("gy")

    def device(step_x, step_y):
        return (
            lax.rem(index_x + (step_x + N_GX), N_GX),
            lax.rem(index_y + (step_y + N_GY), N_GY),
        )

    table_copy = pltpu.make_async_copy(table_hbm, table, table_sem)
    table_copy.start()

    barrier = pltpu.get_barrier_semaphore()
    peers = [(x, 0) for x in range(1, N_GX)] + [(0, y) for y in range(1, N_GY)]
    peers += [(x, y) for x, y in NEIGHBOURS if x and y]
    for step_x, step_y in peers:
        pl.semaphore_signal(
            barrier, inc=1, device_id=device(step_x, step_y), device_id_type=MESH_IDS
        )

    started = []

    def send(number, source, target, step_x, step_y):
        copy = pltpu.make_async_remote_copy(
            src_ref=source,
            dst_ref=target,
            send_sem=send_sems.at[number],
            recv_sem=recv_sems.at[number],
            device_id=device(step_x, step_y),
            device_id_type=MESH_IDS,
        )
        copy.start()
        started.append(copy)
        return copy

    sums[...] = jnp.zeros_like(sums)

    def clear(x, carried):
        q1[x] = jnp.zeros((40, NZ), F32)
        return carried

    lax.fori_loop(0, 41, clear, 0)

    def deposit(first, last, row, count, send_finished):
        def step(plane, carried):
            deposit_plane(
                plane, charge_ref, fraction_ref, cell_ref, places_ref, sums, index_y
            )
            return carried

        lax.fori_loop(first, last, step, 0, unroll=2)
        flat = sums[row : row + count].reshape(count * EY, NZ)
        value = times_const(flat, forward_high_ref[...], forward_low_ref[...])
        own[row : row + count] = value.reshape(count, EY, NZ)
        edge[row : row + count] = own[row : row + count, 11:19, :]

        def restrict_y(x, carried):
            q1[x + 3, 8:32, :] = own[x]
            total = jnp.zeros((16, NZ), F32)
            for offset, weight in taps:
                total = total + weight * q1[x + 3, pl.ds(6 + offset, 16, stride=2), :]
            part1[x] = total
            return carried

        send_finished()
        lax.fori_loop(row, row + count, restrict_y, 0)

    round1 = []

    def send_edges(number, row, count):
        rows = pl.ds(row, count)
        round1.append(send(number, edge.at[rows], from_y.at[0, rows], 0, 1))
        round1.append(send(number + 1, own.at[rows, 0:8, :], from_y.at[1, rows], 0, -1))

    high_x, low_x = pl.ds(29, 6), pl.ds(0, 6)

    def send_high():
        pl.semaphore_wait(barrier, len(peers))
        round1.append(send(0, edge.at[high_x], from_corner.at[0], 1, 1))
        round1.append(send(1, own.at[high_x, 0:8, :], from_corner.at[1], 1, -1))
        round1.append(send(2, own.at[high_x], from_x.at[0], 1, 0))
        send_edges(6, 29, 6)

    def send_low():
        round1.append(send(3, edge.at[low_x], from_corner.at[2], -1, 1))
        round1.append(send(4, own.at[low_x, 0:8, :], from_corner.at[3], -1, -1))
        round1.append(send(5, own.at[low_x], from_x.at[1], -1, 0))
        send_edges(8, 0, 6)

    deposit(26, 32, 29, 6, send_high)
    deposit(0, 6, 0, 6, send_low)
    deposit(6, 14, 6, 8, lambda: send_edges(10, 6, 8))
    deposit(14, 22, 14, 8, lambda: send_edges(12, 14, 8))
    deposit(22, 26, 22, 7, lambda: send_edges(14, 22, 7))

    rows = []
    for m in range(-1, 19):
        total = jnp.zeros((16, NZ), F32)
        for offset, weight in taps:
            if 0 <= 2 * m + offset < EX:
                total = total + weight * part1[2 * m + offset]
        rows.append(total)
    level2 = times_const(
        jnp.concatenate(rows[0::2], axis=0), high_ref[C_M12], low_ref[C_M12]
    ) + times_const(jnp.concatenate(rows[1::2], axis=0), high_ref[C_M12B], low_ref[C_M12B])
    own2[...] = level2.reshape(10, 16, NZ)
    edge2[...] = own2[:, 5:13, :]

    round2 = []
    for number, (step_x, step_y) in enumerate(NEIGHBOURS):
        rows = {0: pl.ds(0, 10), 1: pl.ds(6, 4), -1: pl.ds(0, 4)}[step_x]
        if step_y == 0:
            source, target = own2.at[rows], from_x2.at[number]
        elif step_x == 0:
            source = edge2 if step_y == 1 else own2.at[:, 0:8, :]
            target = from_y2.at[number - 2]
        else:
            source = edge2.at[rows] if step_y == 1 else own2.at[rows, 0:8, :]
            target = from_corner2.at[number - 4]
        round2.append(send(16 + number, source, target, step_x, step_y))

    q2[...] = jnp.zeros_like(q2)
    q3[:, 24:32, :] = jnp.zeros((15, 8, NZ), F32)
    for pair in range(10):
        q2[3 + 2 * pair, 7:23, :] = own2[pair]
        q2[4 + 2 * pair, 7:23, :] = pltpu.roll(own2[pair], 64, axis=1)

    for copy in round2:
        copy.wait_recv()

    def add_to2(row, start, value):
        end = start + value.shape[0]
        for place, plane in ((row, value), (row + 1, pltpu.roll(value, 64, axis=1))):
            if 0 <= place < 26:
                q2[place, start:end, :] = q2[place, start:end, :] + plane

    for pair in range(10):
        add_to2(3 + 2 * pair, 4, from_y2[0, pair])
        add_to2(3 + 2 * pair, 15, from_y2[1, pair])
    for side, first in ((0, -1), (1, 19)):
        for pair in range(4):
            add_to2(first + 2 * pair, 7, from_x2[side, pair])
            add_to2(first + 2 * pair, 4, from_corner2[2 * side, pair])
            add_to2(first + 2 * pair, 15, from_corner2[2 * side + 1, pair])

    for m in range(8):
        total = jnp.zeros((24, NZ), F32)
        for offset, weight in taps:
            total = total + weight * q2[2 * m + 4 + offset, 0:24, :]
        part2[24 * m : 24 * (m + 1), :] = total
    tile = jnp.zeros((8, NZ), F32)
    for n in range(4):
        total = jnp.zeros((8, NZ), F32)
        for offset, weight in taps:
            total = total + weight * part2[pl.ds(8 + 2 * n + offset, 8, stride=24), :]
        tile = tile + times_const(total, high_ref[C_M23 + n], low_ref[C_M23 + n])
    ring_x[1] = tile

    round3 = []
    for step in range(1, N_GX):
        place = (N_GX - step + 1) % N_GX
        round3.append(send(23 + step, ring_x.at[1], ring_x.at[place], step, 0))

    def stencil_small(source, row, start, count, k_ref):
        total = jnp.zeros((count, NZ), F32)
        for across in range(4):
            for along in range(4):
                value = None
                for sign_r in sorted({across, -across}):
                    for sign_s in sorted({along, -along}):
                        piece = source[row + sign_r, start + sign_s : start + sign_s + count, :]
                        value = piece if value is None else value + piece
                total = total + k_ref[4 * across + along : 4 * across + along + 1, :] * value
        return total

    def stencil2(x, carried):
        smooth2[x] = stencil_small(q2, x + 3, 7, 16, k2_ref)
        return carried

    lax.fori_loop(0, 20, stencil2, 0)

    for copy in round3:
        copy.wait_recv()

    round4 = []
    for number, step in enumerate((1, -1, 2, -2)):
        round4.append(send(31 + number, ring_x.at[0:3], halo.at[2 - step], 0, step))
    column = const_times(
        high_ref[C_UR, 0:32, 0:64], low_ref[C_UR, 0:32, 0:64], ring_x[...].reshape(64, NZ)
    )
    ring_y[0] = times_const(column[0:16], high_ref[C_BD0], low_ref[C_BD0]) + times_const(
        column[16:32], high_ref[C_BD1], low_ref[C_BD1]
    )
    round5 = []
    for step in range(1, N_GY):
        round5.append(send(34 + step, ring_y.at[0], ring_y.at[N_GY - step], 0, step))

    for copy in round1:
        copy.wait_recv()

    def add_y(x, carried):
        q1[x + 3, 3:11, :] = q1[x + 3, 3:11, :] + from_y[0, x]
        q1[x + 3, 24:32, :] = q1[x + 3, 24:32, :] + from_y[1, x]
        return carried

    lax.fori_loop(0, EX, add_y, 0)
    for side, start in ((0, 0), (1, 35)):
        for x in range(6):
            row = start + x
            q1[row, 8:32, :] = q1[row, 8:32, :] + from_x[side, x]
            q1[row, 3:11, :] = q1[row, 3:11, :] + from_corner[2 * side, x]
            q1[row, 24:32, :] = q1[row, 24:32, :] + from_corner[2 * side + 1, x]

    def sum_y(x, carried):
        for dy in range(1, 4):
            sums1[dy - 1, x] = q1[x, 8 + dy : 32 + dy, :] + q1[x, 8 - dy : 32 - dy, :]
        return carried

    lax.fori_loop(0, 41, sum_y, 0)

    def stencil1(x, carried):
        total = jnp.zeros((EY, NZ), F32)
        for dy in range(4):
            for dx in range(4):
                if dy == 0:
                    value = q1[x + 3 + dx, 8:32, :]
                    if dx:
                        value = value + q1[x + 3 - dx, 8:32, :]
                else:
                    value = sums1[dy - 1, x + 3 + dx]
                    if dx:
                        value = value + sums1[dy - 1, x + 3 - dx]
                total = total + k1_ref[4 * dx + dy : 4 * dx + dy + 1, :] * value
        smooth1[x] = total
        return carried

    lax.fori_loop(0, EX, stencil1, 0)

    halo[2] = ring_x[0:3]
    for copy in round4:
        copy.wait_recv()
    for y in range(-5, 10):
        place = y % 4
        source = halo[y // 4 + 2].reshape(24, NZ)
        if place:
            source = pltpu.roll(source, NZ - 32 * place, axis=1)
        q3[y + 5, 0:24, :] = source

    def stencil3(y, carried):
        field3[y] = stencil_small(q3, y + 3, 6, 16, k3_ref)
        return carried

    lax.fori_loop(0, 9, stencil3, 0)

    table_copy.wait()
    for copy in round5:
        copy.wait_recv()

    def add_slot(slot, totals):
        values = ring_y[slot]
        return tuple(
            total + table[row % 4, slot + 2 - row // 4] * values for row, total in enumerate(totals)
        )

    coarse = lax.fori_loop(
        0, N_GY, add_slot, tuple(jnp.zeros((16, NZ), F32) for _ in range(9)), unroll=4
    )
    coarse = jnp.concatenate(coarse, axis=0)
    half0 = times_const(coarse, high_ref[C_NZ0], low_ref[C_NZ0])
    half1 = times_const(coarse, high_ref[C_NZ1], low_ref[C_NZ1])
    for row in range(9):
        both = jnp.concatenate(
            [half0[16 * row : 16 * (row + 1)], half1[16 * row : 16 * (row + 1)]], axis=0
        )
        field3[row] = field3[row] + const_times(
            high_ref[C_PU, 0:16, 0:32], low_ref[C_PU, 0:16, 0:32], both
        )

    fields = [prolonged_rows(lambda m: field3[m + 2], y) for y in range(-1, 11)]
    up3[...] = times_const(jnp.concatenate(fields, axis=0), high_ref[C_M23T], low_ref[C_M23T])

    def column3(m):
        return up3[pl.ds(m + 2, 12, stride=16), :]

    for x in range(-1, 19):
        smooth2[x + 1, 0:12, :] = smooth2[x + 1, 0:12, :] + prolonged_rows(column3, x)

    part = times_const(
        smooth2[...].reshape(20 * 16, NZ), high_ref[C_M12T], low_ref[C_M12T]
    ).reshape(20, 16, NZ)
    smooth2[...] = part

    def widen_y(x, carried):
        rows = [smooth2[x, n : n + 12, :] for n in range(4)]
        up2[x, pl.ds(0, 12, stride=2), :] = rows[1]
        up2[x, pl.ds(1, 12, stride=2), :] = 0.5625 * (rows[1] + rows[2]) - 0.0625 * (
            rows[0] + rows[3]
        )
        return carried

    lax.fori_loop(0, 20, widen_y, 0)

    def widen_x(m, carried):
        values = [up2[m + n] for n in range(4)]
        out_ref[2 * m] = smooth1[2 * m] + values[1]
        out_ref[2 * m + 1] = smooth1[2 * m + 1] + (
            0.5625 * (values[1] + values[2]) - 0.0625 * (values[0] + values[3])
        )
        return carried

    lax.fori_loop(0, 17, widen_x, 0)
    out_ref[34] = smooth1[34] + up2[18]

    for copy in started:
        copy.wait_send()


def in_vmem(count):
    return [pl.BlockSpec(memory_space=pltpu.VMEM)] * count


def local(charges, fractions, cells):
    charge = charges.reshape(1, ATOMS_DEV)
    fraction = fractions.reshape(3, 1, ATOMS_DEV)
    cell = cells.reshape(2, ATOMS_DEV)
    places = jnp.asarray(np.tile(np.arange(NZ)[:, None], (1, 128)).astype(BF16))
    forward = [jnp.asarray(part) for part in split_pair(real_basis(NZ).T)]
    inverse = [jnp.asarray(part) for part in split_pair(real_basis(NZ))]
    block = jax.ShapeDtypeStruct((EX, EY, NZ), F32)

    high, low = split_constants()
    field = pl.pallas_call(
        levels_kernel,
        out_shape=block,
        in_specs=in_vmem(11) + [pl.BlockSpec(memory_space=pl.ANY)],
        out_specs=pl.BlockSpec(memory_space=pltpu.VMEM),
        scratch_shapes=[
            pltpu.VMEM((EX, EY, NZ), F32),
            pltpu.VMEM((EX, EY, NZ), F32),
            pltpu.VMEM((EX, 8, NZ), F32),
            pltpu.VMEM((2, 6, EY, NZ), F32),
            pltpu.VMEM((2, EX, 8, NZ), F32),
            pltpu.VMEM((4, 6, 8, NZ), F32),
            pltpu.VMEM((2, 4, 16, NZ), F32),
            pltpu.VMEM((2, 10, 8, NZ), F32),
            pltpu.VMEM((4, 4, 8, NZ), F32),
            pltpu.VMEM((10, 16, NZ), F32),
            pltpu.VMEM((10, 8, NZ), F32),
            pltpu.VMEM((41, 40, NZ), F32),
            pltpu.VMEM((3, 41, EY, NZ), F32),
            pltpu.VMEM((EX, EY, NZ), F32),
            pltpu.VMEM((EX, 16, NZ), F32),
            pltpu.VMEM((26, 32, NZ), F32),
            pltpu.VMEM((20, 16, NZ), F32),
            pltpu.VMEM((8 * 24, NZ), F32),
            pltpu.VMEM((N_GX, 8, NZ), F32),
            pltpu.VMEM((5, 3, 8, NZ), F32),
            pltpu.VMEM((N_GY, 16, NZ), F32),
            pltpu.VMEM((15, 32, NZ), F32),
            pltpu.VMEM((9, 16, NZ), F32),
            pltpu.VMEM((12 * 16, NZ), F32),
            pltpu.VMEM((20, EY, NZ), F32),
            pltpu.VMEM((4, 34, 16, NZ), F32),
            pltpu.SemaphoreType.DMA,
            pltpu.SemaphoreType.DMA((N_SEMS,)),
            pltpu.SemaphoreType.DMA((N_SEMS,)),
        ],
        compiler_params=pltpu.CompilerParams(collective_id=0, has_side_effects=True),
        name="levels",
    )(
        charge,
        fraction,
        cell,
        places,
        *forward,
        jnp.asarray(stencil_table(1, 128)),
        jnp.asarray(stencil_table(2, 64)),
        jnp.asarray(stencil_table(3, 32)),
        jnp.asarray(high),
        jnp.asarray(low),
        jnp.asarray(coarse_table()),
    )

    potential, sampled = pl.pallas_call(
        sample_kernel,
        out_shape=(
            jax.ShapeDtypeStruct((CX, CY, NZ), F32),
            jax.ShapeDtypeStruct((1, ATOMS_DEV), F32),
        ),
        in_specs=in_vmem(6),
        out_specs=in_vmem(2),
        scratch_shapes=[pltpu.VMEM((EX, EY, NZ), F32)],
        name="sample",
    )(field, fraction, cell, places, *inverse)
    return potential, sampled.reshape(1, 1, ATOMS_DEV)


def solution(mesh):
    placed = (P("gx", "gy", None), P("gx", "gy", None, None), P("gx", "gy", None, None))
    return jax.shard_map(
        local,
        mesh=mesh,
        in_specs=placed,
        out_specs=(P("gx", "gy", None), P("gx", "gy", None)),
        check_vma=False,
    )
```

```python
import functools

import jax
import jax.numpy as jnp
import numpy as np
from jax import lax
from jax.experimental import pallas as pl
from jax.experimental.pallas import tpu as pltpu
from jax.sharding import PartitionSpec as P

CX = 32
CY = 16
NZ = 128
ATOMS_DEV = 16384
N_GX = 8
N_GY = 32
PLANE = ATOMS_DEV // CX
EX = CX + 3
EY = 24
MESH_IDS = pl.DeviceIdType.MESH
BF16 = jnp.bfloat16
F32 = jnp.float32
taps = ((-3, -0.0625), (-1, 0.5625), (0, 1.0), (1, 0.5625), (3, -0.0625))


def smooth_numpy(rho):
    return np.where(
        rho < 1.0, 1.875 - 1.25 * rho * rho + 0.375 * rho**4, 1.0 / np.maximum(rho, 1.0)
    )


def frequencies(count):
    inner = np.repeat(np.arange(1, count // 2), 2)
    return np.concatenate([[0], inner, [count // 2]])


def real_basis(count):
    wave = frequencies(count)
    angle = 2.0 * np.pi * wave[:, None] * np.arange(count)[None, :] / count
    is_sine = np.zeros(count, bool)
    is_sine[2:-1:2] = True
    basis = np.where(is_sine[:, None], np.sin(angle), np.cos(angle)) * np.sqrt(2.0 / count)
    basis[0] /= np.sqrt(2.0)
    basis[-1] /= np.sqrt(2.0)
    return basis


def restriction(count):
    matrix = np.zeros((count // 2, count))
    for row in range(count // 2):
        for offset, weight in taps:
            matrix[row, (2 * row + offset) % count] += weight
    return matrix


def stencil_table(level, extent):
    offsets = np.arange(-3, 4) * 1.0
    radius = np.sqrt(
        offsets[:, None, None] ** 2 + offsets[None, :, None] ** 2 + offsets[None, None, :] ** 2
    )
    stencil = (smooth_numpy(radius / 1.5) / 1.5 - smooth_numpy(radius / 3.0) / 3.0) / 2.0 ** (
        level - 1
    )
    waves = np.cos(2.0 * np.pi * offsets[:, None] * frequencies(extent)[None, :] / extent)
    table = np.zeros((16, 128))
    table[:, :extent] = (stencil[3:, 3:] @ waves).reshape(16, extent)
    return table.astype(np.float32)


def placed_at(block, row, column):
    matrix = np.zeros((128, 128))
    matrix[row : row + block.shape[0], column : column + block.shape[1]] = block
    return matrix


(
    C_M12,
    C_M23,
    C_BD0,
    C_BD1,
    C_NZ0,
    C_NZ1,
    C_M23T,
    C_M12T,
    C_UR,
    C_PU,
    C_M12B,
) = (0, 1, 5, 6, 7, 8, 9, 10, 11, 12, 13)


@functools.cache
def split_constants():
    def down(count):
        return (real_basis(count // 2) @ restriction(count) @ real_basis(count).T).T

    m12, m23, m34 = down(128), down(64), down(32)
    stack = [placed_at(m12, 0, 0)]
    stack += [placed_at(m23, 0, 32 * place) for place in range(4)]
    for half in range(2):
        matrix = np.zeros((128, 128))
        for place in range(4):
            matrix += placed_at(m34, 32 * place, 64 * half + 16 * place)
        stack.append(matrix)
    for half in range(2):
        matrix = np.zeros((128, 128))
        for place in range(4):
            matrix += placed_at(m34.T, 64 * half + 16 * place, 0)
        stack.append(matrix)
    stack += [placed_at(m23.T, 0, 0), placed_at(m12.T, 0, 0)]
    along_x = restriction(64)
    columns = (np.arange(64) - 8) % 64
    stack.append(placed_at((real_basis(32) @ along_x)[:, columns], 0, 0))
    rows = (np.arange(16) - 2) % 64
    stack.append(placed_at((real_basis(32) @ along_x).T[rows], 0, 0))
    stack.append(placed_at(m12, 0, 64))
    return split_pair(np.stack(stack))


def split_pair(matrix):
    high = matrix.astype(np.float32).astype(BF16)
    low = (matrix - high.astype(np.float64)).astype(np.float32).astype(BF16)
    return high, low


@functools.cache
def coarse_table():
    counts = (32, 64, 16)
    signed = [np.where(np.arange(c) > c // 2, np.arange(c) - c, np.arange(c)) for c in counts]
    radius = np.sqrt(
        signed[0][:, None, None] ** 2.0
        + signed[1][None, :, None] ** 2.0
        + signed[2][None, None, :] ** 2.0
    )
    kernel = smooth_numpy(radius / 1.5) / 12.0
    wave_x = np.cos(2.0 * np.pi * np.outer(frequencies(32), np.arange(32)) / 32)
    wave_z = np.cos(2.0 * np.pi * np.outer(frequencies(16), np.arange(16)) / 16)
    along_y = np.einsum("ax,xyz,bz->aby", wave_x, kernel, wave_z)
    down_y = restriction(128)
    differ = (np.arange(64)[:, None] - np.arange(64)[None, :]) % 64
    up_rows = down_y.T[(np.arange(4) - 2) % 128]
    folded = np.einsum("cm,abmn->abcn", up_rows, along_y[:, :, differ])
    folded = np.einsum("abcn,ny->abcy", folded, down_y)
    folded = folded.reshape(2, 16, 16, 4, 32, 4).transpose(3, 4, 1, 0, 5, 2)
    folded = folded.reshape(4, 32, 16, 128)
    extended = folded[:, (np.arange(34) - 2) % 32]
    return extended.astype(np.float32)


def split(value):
    high = value.astype(BF16)
    low = (value - high.astype(F32)).astype(BF16)
    return high, low


def mm(a, b):
    return jnp.dot(a, b, preferred_element_type=F32)


def times_const(value, high_w, low_w):
    high, low = split(value)
    return mm(high, high_w) + (mm(low, high_w) + mm(high, low_w))


def const_times(high_w, low_w, value):
    high, low = split(value)
    return mm(high_w, high) + (mm(high_w, low) + mm(low_w, high))


def spline_weights(frac):
    def near_weight(distance):
        return (1.0 - distance) * (1.0 + distance - 1.5 * distance * distance)

    def far_weight(distance):
        return -0.5 * (distance - 1.0) * (2.0 - distance) * (2.0 - distance)

    return (
        far_weight(1.0 + frac),
        near_weight(frac),
        near_weight(1.0 - frac),
        far_weight(2.0 - frac),
    )


def tap_table(distance, weights):
    result = jnp.zeros(distance.shape, F32)
    for tap in range(4):
        result = jnp.where(distance == tap, weights[tap], result)
    return result


def rows_of(row):
    packed = jnp.broadcast_to(row, (16, row.shape[1])).astype(BF16)
    return jnp.concatenate([packed] * (NZ // 16), axis=0)


def depth_tables(places_ref, base, weights):
    places = jnp.concatenate([places_ref[...]] * (base.shape[1] // 128), axis=1)
    high = low = jnp.zeros(places.shape, BF16)
    for tap in range(4):
        target = ((base + tap) & (NZ - 1)).astype(F32)
        here = places == rows_of(target)
        weight_high = weights[tap].astype(BF16).astype(F32)
        high = jnp.where(here, rows_of(weight_high), high)
        low = jnp.where(here, rows_of(weights[tap] - weight_high), low)
    return high, low


def plane_tables(plane, fraction_ref, cell_ref, places_ref, index_y):
    lanes = pl.ds(pl.multiple_of(plane * PLANE, PLANE), PLANE)
    fraction = jnp.concatenate([fraction_ref[k, :, lanes] for k in range(3)], axis=0)
    weights = spline_weights(fraction)
    cells = cell_ref[:, lanes]
    base_y = (cells[0:1] - (index_y * CY + 1)) & (CY * N_GY - 1)
    places_y = lax.broadcasted_iota(jnp.int32, (EY, PLANE), 0)
    table_y = tap_table(places_y - base_y, [w[1:2] for w in weights])
    tables_z = depth_tables(places_ref, cells[1:2] - 1, [w[2:3] for w in weights])
    return lanes, [w[0:1] for w in weights], table_y, tables_z


def deposit_plane(
    plane, charge_ref, fraction_ref, cell_ref, places_ref, sums, index_y, tables
):
    lanes, along_x, table_y, (z_high, z_low) = plane_tables(
        plane, fraction_ref, cell_ref, places_ref, index_y
    )
    keep_x, keep_y, keep_high, keep_low = tables
    keep_x[plane] = jnp.concatenate(along_x, axis=0)
    keep_y[plane] = table_y
    keep_high[plane] = z_high
    keep_low[plane] = z_low
    charge = charge_ref[:, lanes]
    spread = jnp.concatenate([table_y * (w * charge) for w in along_x], axis=0)
    spread_high, spread_low = split(spread)
    dims = (((1,), (1,)), ((), ()))
    both = jnp.concatenate([spread_high, spread_low], axis=0)
    first = lax.dot_general(both, z_high, dims, preferred_element_type=F32)
    second = lax.dot_general(spread_high, z_low, dims, preferred_element_type=F32)
    contrib = first[: 4 * EY] + first[4 * EY :] + second
    for tap in range(4):
        sums[plane + tap] = sums[plane + tap] + contrib[EY * tap : EY * (tap + 1)]


def sample_plane(plane, tables, window_ref, atom_ref):
    keep_x, keep_y, keep_high, keep_low = tables
    lanes = pl.ds(pl.multiple_of(plane * PLANE, PLANE), PLANE)
    high, low = split(window_ref[pl.ds(plane, 4)].reshape(4 * EY, NZ))
    z_high, z_low = keep_high[plane], keep_low[plane]
    projected = mm(
        jnp.concatenate([high, low], axis=1), jnp.concatenate([z_high, z_high], axis=0)
    ) + mm(high, z_low)
    total = jnp.zeros((EY, PLANE), F32)
    for tap in range(4):
        total = total + keep_x[plane, tap : tap + 1, :] * projected[EY * tap : EY * (tap + 1)]
    atom_ref[:, lanes] = jnp.sum(total * keep_y[plane], axis=0, keepdims=True)


NEIGHBOURS = ((1, 0), (-1, 0), (0, 1), (0, -1), (1, 1), (1, -1), (-1, 1), (-1, -1))
N_SEMS = 16 + 8 + 7 + 4 + 31


def prolonged_rows(get, row):
    middle = row // 2
    if row % 2 == 0:
        return get(middle)
    return 0.5625 * (get(middle) + get(middle + 1)) - 0.0625 * (get(middle - 1) + get(middle + 2))


N_IN = 14
N_FIRST = 6


def levels_entry(*refs):
    sources, outputs = refs[:N_IN], refs[N_IN : N_IN + 2]
    inputs, sems, rest = refs[N_IN + 2 : 2 * N_IN + 2], refs[2 * N_IN + 2], refs[2 * N_IN + 3 :]
    copies = [
        pltpu.make_async_copy(source, target, sems.at[number])
        for number, (source, target) in enumerate(zip(sources, inputs))
    ]
    for copy in copies:
        copy.start()
    levels_kernel(*inputs, *outputs, *rest, copies[:N_FIRST], copies[N_FIRST:])


def levels_kernel(
    charge_ref,
    fraction_ref,
    cell_ref,
    places_ref,
    forward_high_ref,
    forward_low_ref,
    inverse_high_ref,
    inverse_low_ref,
    k1_ref,
    k2_ref,
    k3_ref,
    high_ref,
    low_ref,
    table,
    grid_ref,
    atom_ref,
    keep_x,
    keep_y,
    keep_high,
    keep_low,
    window,
    sums,
    own,
    edge,
    from_x,
    from_y,
    from_corner,
    from_x2,
    from_y2,
    from_corner2,
    own2,
    edge2,
    q1,
    sums1,
    smooth1,
    part1,
    q2,
    smooth2,
    part2,
    ring_x,
    halo,
    ring_y,
    q3,
    field3,
    up3,
    up2,
    send_sems,
    recv_sems,
    first_copies,
    later_copies,
):
    index_x = lax.axis_index("gx")
    index_y = lax.axis_index("gy")
    tables = (keep_x, keep_y, keep_high, keep_low)

    def device(step_x, step_y):
        return (
            lax.rem(index_x + (step_x + N_GX), N_GX),
            lax.rem(index_y + (step_y + N_GY), N_GY),
        )

    barrier = pltpu.get_barrier_semaphore()
    peers = [(x, 0) for x in range(1, N_GX)] + [(0, y) for y in range(1, N_GY)]
    peers += [(x, y) for x, y in NEIGHBOURS if x and y]
    for step_x, step_y in peers:
        pl.semaphore_signal(
            barrier, inc=1, device_id=device(step_x, step_y), device_id_type=MESH_IDS
        )

    started = []

    def send(number, source, target, step_x, step_y):
        copy = pltpu.make_async_remote_copy(
            src_ref=source,
            dst_ref=target,
            send_sem=send_sems.at[number],
            recv_sem=recv_sems.at[number],
            device_id=device(step_x, step_y),
            device_id_type=MESH_IDS,
        )
        copy.start()
        started.append(copy)
        return copy

    sums[...] = jnp.zeros_like(sums)

    def clear(x, carried):
        q1[x] = jnp.zeros((40, NZ), F32)
        return carried

    lax.fori_loop(0, 41, clear, 0)

    for copy in first_copies:
        copy.wait()

    def deposit(first, last, row, count, send_finished):
        def step(plane, carried):
            deposit_plane(
                plane, charge_ref, fraction_ref, cell_ref, places_ref, sums, index_y, tables
            )
            return carried

        lax.fori_loop(first, last, step, 0, unroll=2)
        flat = sums[row : row + count].reshape(count * EY, NZ)
        value = times_const(flat, forward_high_ref[...], forward_low_ref[...])
        own[row : row + count] = value.reshape(count, EY, NZ)
        edge[row : row + count] = own[row : row + count, 11:19, :]

        def restrict_y(x, carried):
            q1[x + 3, 8:32, :] = own[x]
            total = jnp.zeros((16, NZ), F32)
            for offset, weight in taps:
                total = total + weight * q1[x + 3, pl.ds(6 + offset, 16, stride=2), :]
            part1[x] = total
            return carried

        send_finished()
        lax.fori_loop(row, row + count, restrict_y, 0)

    round1 = []

    def send_edges(number, row, count):
        rows = pl.ds(row, count)
        round1.append(send(number, edge.at[rows], from_y.at[0, rows], 0, 1))
        round1.append(send(number + 1, own.at[rows, 0:8, :], from_y.at[1, rows], 0, -1))

    high_x, low_x = pl.ds(29, 6), pl.ds(0, 6)

    def send_high():
        pl.semaphore_wait(barrier, len(peers))
        round1.append(send(0, edge.at[high_x], from_corner.at[0], 1, 1))
        round1.append(send(1, own.at[high_x, 0:8, :], from_corner.at[1], 1, -1))
        round1.append(send(2, own.at[high_x], from_x.at[0], 1, 0))
        send_edges(6, 29, 6)

    def send_low():
        round1.append(send(3, edge.at[low_x], from_corner.at[2], -1, 1))
        round1.append(send(4, own.at[low_x, 0:8, :], from_corner.at[3], -1, -1))
        round1.append(send(5, own.at[low_x], from_x.at[1], -1, 0))
        send_edges(8, 0, 6)

    deposit(26, 32, 29, 6, send_high)
    deposit(0, 6, 0, 6, send_low)
    deposit(6, 14, 6, 8, lambda: send_edges(10, 6, 8))
    deposit(14, 22, 14, 8, lambda: send_edges(12, 14, 8))
    deposit(22, 26, 22, 7, lambda: send_edges(14, 22, 7))

    for copy in later_copies:
        copy.wait()

    rows = []
    for m in range(-1, 19):
        total = jnp.zeros((16, NZ), F32)
        for offset, weight in taps:
            if 0 <= 2 * m + offset < EX:
                total = total + weight * part1[2 * m + offset]
        rows.append(total)
    level2 = times_const(
        jnp.concatenate(rows[0::2], axis=0), high_ref[C_M12], low_ref[C_M12]
    ) + times_const(jnp.concatenate(rows[1::2], axis=0), high_ref[C_M12B], low_ref[C_M12B])
    own2[...] = level2.reshape(10, 16, NZ)
    edge2[...] = own2[:, 5:13, :]

    round2 = []
    for number, (step_x, step_y) in enumerate(NEIGHBOURS):
        rows = {0: pl.ds(0, 10), 1: pl.ds(6, 4), -1: pl.ds(0, 4)}[step_x]
        if step_y == 0:
            source, target = own2.at[rows], from_x2.at[number]
        elif step_x == 0:
            source = edge2 if step_y == 1 else own2.at[:, 0:8, :]
            target = from_y2.at[number - 2]
        else:
            source = edge2.at[rows] if step_y == 1 else own2.at[rows, 0:8, :]
            target = from_corner2.at[number - 4]
        round2.append(send(16 + number, source, target, step_x, step_y))

    q2[...] = jnp.zeros_like(q2)
    q3[:, 24:32, :] = jnp.zeros((15, 8, NZ), F32)
    for pair in range(10):
        q2[3 + 2 * pair, 7:23, :] = own2[pair]
        q2[4 + 2 * pair, 7:23, :] = pltpu.roll(own2[pair], 64, axis=1)

    for copy in round2:
        copy.wait_recv()

    def add_to2(row, start, value):
        end = start + value.shape[0]
        for place, plane in ((row, value), (row + 1, pltpu.roll(value, 64, axis=1))):
            if 0 <= place < 26:
                q2[place, start:end, :] = q2[place, start:end, :] + plane

    for pair in range(10):
        add_to2(3 + 2 * pair, 4, from_y2[0, pair])
        add_to2(3 + 2 * pair, 15, from_y2[1, pair])
    for side, first in ((0, -1), (1, 19)):
        for pair in range(4):
            add_to2(first + 2 * pair, 7, from_x2[side, pair])
            add_to2(first + 2 * pair, 4, from_corner2[2 * side, pair])
            add_to2(first + 2 * pair, 15, from_corner2[2 * side + 1, pair])

    for m in range(8):
        total = jnp.zeros((24, NZ), F32)
        for offset, weight in taps:
            total = total + weight * q2[2 * m + 4 + offset, 0:24, :]
        part2[24 * m : 24 * (m + 1), :] = total
    tile = jnp.zeros((8, NZ), F32)
    for n in range(4):
        total = jnp.zeros((8, NZ), F32)
        for offset, weight in taps:
            total = total + weight * part2[pl.ds(8 + 2 * n + offset, 8, stride=24), :]
        tile = tile + times_const(total, high_ref[C_M23 + n], low_ref[C_M23 + n])
    ring_x[1] = tile

    round3 = []
    for step in range(1, N_GX):
        place = (N_GX - step + 1) % N_GX
        round3.append(send(23 + step, ring_x.at[1], ring_x.at[place], step, 0))

    def stencil_small(source, row, start, count, k_ref):
        total = jnp.zeros((count, NZ), F32)
        for across in range(4):
            for along in range(4):
                value = None
                for sign_r in sorted({across, -across}):
                    for sign_s in sorted({along, -along}):
                        piece = source[row + sign_r, start + sign_s : start + sign_s + count, :]
                        value = piece if value is None else value + piece
                total = total + k_ref[4 * across + along : 4 * across + along + 1, :] * value
        return total

    def stencil2(x, carried):
        smooth2[x] = stencil_small(q2, x + 3, 7, 16, k2_ref)
        return carried

    lax.fori_loop(0, 20, stencil2, 0)

    for copy in round3:
        copy.wait_recv()

    round4 = []
    for number, step in enumerate((1, -1, 2, -2)):
        round4.append(send(31 + number, ring_x.at[0:3], halo.at[2 - step], 0, step))
    column = const_times(
        high_ref[C_UR, 0:32, 0:64], low_ref[C_UR, 0:32, 0:64], ring_x[...].reshape(64, NZ)
    )
    ring_y[0] = times_const(column[0:16], high_ref[C_BD0], low_ref[C_BD0]) + times_const(
        column[16:32], high_ref[C_BD1], low_ref[C_BD1]
    )
    round5 = []
    for step in range(1, N_GY):
        round5.append(send(34 + step, ring_y.at[0], ring_y.at[N_GY - step], 0, step))

    for copy in round1:
        copy.wait_recv()

    def add_y(x, carried):
        q1[x + 3, 3:11, :] = q1[x + 3, 3:11, :] + from_y[0, x]
        q1[x + 3, 24:32, :] = q1[x + 3, 24:32, :] + from_y[1, x]
        return carried

    lax.fori_loop(0, EX, add_y, 0)
    for side, start in ((0, 0), (1, 35)):
        for x in range(6):
            row = start + x
            q1[row, 8:32, :] = q1[row, 8:32, :] + from_x[side, x]
            q1[row, 3:11, :] = q1[row, 3:11, :] + from_corner[2 * side, x]
            q1[row, 24:32, :] = q1[row, 24:32, :] + from_corner[2 * side + 1, x]

    def sum_y(x, carried):
        for dy in range(1, 4):
            sums1[dy - 1, x] = q1[x, 8 + dy : 32 + dy, :] + q1[x, 8 - dy : 32 - dy, :]
        return carried

    lax.fori_loop(0, 41, sum_y, 0)

    def stencil1(x, carried):
        total = jnp.zeros((EY, NZ), F32)
        for dy in range(4):
            for dx in range(4):
                if dy == 0:
                    value = q1[x + 3 + dx, 8:32, :]
                    if dx:
                        value = value + q1[x + 3 - dx, 8:32, :]
                else:
                    value = sums1[dy - 1, x + 3 + dx]
                    if dx:
                        value = value + sums1[dy - 1, x + 3 - dx]
                total = total + k1_ref[4 * dx + dy : 4 * dx + dy + 1, :] * value
        smooth1[x] = total
        return carried

    lax.fori_loop(0, EX, stencil1, 0)

    halo[2] = ring_x[0:3]
    for copy in round4:
        copy.wait_recv()
    for y in range(-5, 10):
        place = y % 4
        source = halo[y // 4 + 2].reshape(24, NZ)
        if place:
            source = pltpu.roll(source, NZ - 32 * place, axis=1)
        q3[y + 5, 0:24, :] = source

    def stencil3(y, carried):
        field3[y] = stencil_small(q3, y + 3, 6, 16, k3_ref)
        return carried

    lax.fori_loop(0, 9, stencil3, 0)

    for copy in round5:
        copy.wait_recv()

    def add_slot(slot, totals):
        values = ring_y[slot]
        return tuple(
            total + table[row % 4, slot + 2 - row // 4] * values for row, total in enumerate(totals)
        )

    coarse = lax.fori_loop(
        0, N_GY, add_slot, tuple(jnp.zeros((16, NZ), F32) for _ in range(9)), unroll=4
    )
    coarse = jnp.concatenate(coarse, axis=0)
    half0 = times_const(coarse, high_ref[C_NZ0], low_ref[C_NZ0])
    half1 = times_const(coarse, high_ref[C_NZ1], low_ref[C_NZ1])
    for row in range(9):
        both = jnp.concatenate(
            [half0[16 * row : 16 * (row + 1)], half1[16 * row : 16 * (row + 1)]], axis=0
        )
        field3[row] = field3[row] + const_times(
            high_ref[C_PU, 0:16, 0:32], low_ref[C_PU, 0:16, 0:32], both
        )

    fields = [prolonged_rows(lambda m: field3[m + 2], y) for y in range(-1, 11)]
    up3[...] = times_const(jnp.concatenate(fields, axis=0), high_ref[C_M23T], low_ref[C_M23T])

    def column3(m):
        return up3[pl.ds(m + 2, 12, stride=16), :]

    for x in range(-1, 19):
        smooth2[x + 1, 0:12, :] = smooth2[x + 1, 0:12, :] + prolonged_rows(column3, x)

    part = times_const(
        smooth2[...].reshape(20 * 16, NZ), high_ref[C_M12T], low_ref[C_M12T]
    ).reshape(20, 16, NZ)
    smooth2[...] = part

    def widen_y(x, carried):
        rows = [smooth2[x, n : n + 12, :] for n in range(4)]
        up2[x, pl.ds(0, 12, stride=2), :] = rows[1]
        up2[x, pl.ds(1, 12, stride=2), :] = 0.5625 * (rows[1] + rows[2]) - 0.0625 * (
            rows[0] + rows[3]
        )
        return carried

    lax.fori_loop(0, 20, widen_y, 0)

    def widen_x(m, carried):
        values = [up2[m + n] for n in range(4)]
        sums[2 * m] = smooth1[2 * m] + values[1]
        sums[2 * m + 1] = smooth1[2 * m + 1] + (
            0.5625 * (values[1] + values[2]) - 0.0625 * (values[0] + values[3])
        )
        return carried

    lax.fori_loop(0, 17, widen_x, 0)
    sums[34] = smooth1[34] + up2[18]

    flat = sums[...].reshape(EX * EY, NZ)
    value = times_const(flat, inverse_high_ref[...], inverse_low_ref[...])
    window[...] = value.reshape(EX, EY, NZ)
    grid_ref[...] = window[:CX, :CY, :]

    def sample(plane, carried):
        sample_plane(plane, tables, window, atom_ref)
        return carried

    lax.fori_loop(0, CX, sample, 0, unroll=2)

    for copy in started:
        copy.wait_send()


def finish_kernel(grid_in, atom_in, grid_out, atom_out, grid, atom, sems):
    pairs = ((grid_in, grid, grid_out), (atom_in, atom, atom_out))
    loads = [
        pltpu.make_async_copy(source, middle, sems.at[number])
        for number, (source, middle, target) in enumerate(pairs)
    ]
    stores = [
        pltpu.make_async_copy(middle, target, sems.at[2 + number])
        for number, (source, middle, target) in enumerate(pairs)
    ]
    for load in loads:
        load.start()
    for load, store in zip(loads, stores):
        load.wait()
        store.start()
    for store in stores:
        store.wait()


def in_vmem(count):
    return [pl.BlockSpec(memory_space=pltpu.VMEM)] * count


def local(charges, fractions, cells):
    charge = charges.reshape(1, ATOMS_DEV)
    fraction = fractions.reshape(3, 1, ATOMS_DEV)
    cell = cells.reshape(2, ATOMS_DEV)
    places = jnp.asarray(np.tile(np.arange(NZ)[:, None], (1, 128)).astype(BF16))
    forward = [jnp.asarray(part) for part in split_pair(real_basis(NZ).T)]
    inverse = [jnp.asarray(part) for part in split_pair(real_basis(NZ))]
    high, low = split_constants()
    inputs = [
        charge,
        fraction,
        cell,
        places,
        *forward,
        *inverse,
        jnp.asarray(stencil_table(1, 128)),
        jnp.asarray(stencil_table(2, 64)),
        jnp.asarray(stencil_table(3, 32)),
        jnp.asarray(high),
        jnp.asarray(low),
        jnp.asarray(coarse_table()),
    ]
    potential, sampled = pl.pallas_call(
        levels_entry,
        out_shape=(
            jax.ShapeDtypeStruct((CX, CY, NZ), F32),
            jax.ShapeDtypeStruct((1, ATOMS_DEV), F32),
        ),
        in_specs=[pl.BlockSpec(memory_space=pltpu.HBM)] * N_IN,
        out_specs=in_vmem(2),
        scratch_shapes=[pltpu.VMEM(value.shape, value.dtype) for value in inputs]
        + [
            pltpu.SemaphoreType.DMA((N_IN,)),
            pltpu.VMEM((CX, 4, PLANE), F32),
            pltpu.VMEM((CX, EY, PLANE), F32),
            pltpu.VMEM((CX, NZ, PLANE), BF16),
            pltpu.VMEM((CX, NZ, PLANE), BF16),
            pltpu.VMEM((EX, EY, NZ), F32),
            pltpu.VMEM((EX, EY, NZ), F32),
            pltpu.VMEM((EX, EY, NZ), F32),
            pltpu.VMEM((EX, 8, NZ), F32),
            pltpu.VMEM((2, 6, EY, NZ), F32),
            pltpu.VMEM((2, EX, 8, NZ), F32),
            pltpu.VMEM((4, 6, 8, NZ), F32),
            pltpu.VMEM((2, 4, 16, NZ), F32),
            pltpu.VMEM((2, 10, 8, NZ), F32),
            pltpu.VMEM((4, 4, 8, NZ), F32),
            pltpu.VMEM((10, 16, NZ), F32),
            pltpu.VMEM((10, 8, NZ), F32),
            pltpu.VMEM((41, 40, NZ), F32),
            pltpu.VMEM((3, 41, EY, NZ), F32),
            pltpu.VMEM((EX, EY, NZ), F32),
            pltpu.VMEM((EX, 16, NZ), F32),
            pltpu.VMEM((26, 32, NZ), F32),
            pltpu.VMEM((20, 16, NZ), F32),
            pltpu.VMEM((8 * 24, NZ), F32),
            pltpu.VMEM((N_GX, 8, NZ), F32),
            pltpu.VMEM((5, 3, 8, NZ), F32),
            pltpu.VMEM((N_GY, 16, NZ), F32),
            pltpu.VMEM((15, 32, NZ), F32),
            pltpu.VMEM((9, 16, NZ), F32),
            pltpu.VMEM((12 * 16, NZ), F32),
            pltpu.VMEM((20, EY, NZ), F32),
            pltpu.SemaphoreType.DMA((N_SEMS,)),
            pltpu.SemaphoreType.DMA((N_SEMS,)),
        ],
        compiler_params=pltpu.CompilerParams(collective_id=0, has_side_effects=True),
        name="levels",
    )(*inputs)
    potential, sampled = pl.pallas_call(
        finish_kernel,
        out_shape=(
            jax.ShapeDtypeStruct((CX, CY, NZ), F32),
            jax.ShapeDtypeStruct((1, ATOMS_DEV), F32),
        ),
        in_specs=[pl.BlockSpec(memory_space=pl.ANY)] * 2,
        out_specs=[pl.BlockSpec(memory_space=pl.ANY)] * 2,
        scratch_shapes=[
            pltpu.VMEM((CX, CY, NZ), F32),
            pltpu.VMEM((1, ATOMS_DEV), F32),
            pltpu.SemaphoreType.DMA((4,)),
        ],
        name="finish",
    )(potential, sampled)
    return potential, sampled.reshape(1, 1, ATOMS_DEV)


def solution(mesh):
    placed = (P("gx", "gy", None), P("gx", "gy", None, None), P("gx", "gy", None, None))
    return jax.shard_map(
        local,
        mesh=mesh,
        in_specs=placed,
        out_specs=(P("gx", "gy", None), P("gx", "gy", None)),
        check_vma=False,
    )
```

```python
import functools

import jax
import jax.numpy as jnp
import numpy as np
from jax import lax
from jax.experimental import pallas as pl
from jax.experimental.pallas import tpu as pltpu
from jax.sharding import PartitionSpec as P

CX = 32
CY = 16
NZ = 128
ATOMS_DEV = 16384
N_GX = 8
N_GY = 32
PLANE = ATOMS_DEV // CX
EX = CX + 3
EY = 24
MESH_IDS = pl.DeviceIdType.MESH
BF16 = jnp.bfloat16
F32 = jnp.float32
taps = ((-3, -0.0625), (-1, 0.5625), (0, 1.0), (1, 0.5625), (3, -0.0625))


def smooth_numpy(rho):
    return np.where(
        rho < 1.0, 1.875 - 1.25 * rho * rho + 0.375 * rho**4, 1.0 / np.maximum(rho, 1.0)
    )


def frequencies(count):
    inner = np.repeat(np.arange(1, count // 2), 2)
    return np.concatenate([[0], inner, [count // 2]])


def real_basis(count):
    wave = frequencies(count)
    angle = 2.0 * np.pi * wave[:, None] * np.arange(count)[None, :] / count
    is_sine = np.zeros(count, bool)
    is_sine[2:-1:2] = True
    basis = np.where(is_sine[:, None], np.sin(angle), np.cos(angle)) * np.sqrt(2.0 / count)
    basis[0] /= np.sqrt(2.0)
    basis[-1] /= np.sqrt(2.0)
    return basis


def restriction(count):
    matrix = np.zeros((count // 2, count))
    for row in range(count // 2):
        for offset, weight in taps:
            matrix[row, (2 * row + offset) % count] += weight
    return matrix


def stencil_table(level, extent):
    offsets = np.arange(-3, 4) * 1.0
    radius = np.sqrt(
        offsets[:, None, None] ** 2 + offsets[None, :, None] ** 2 + offsets[None, None, :] ** 2
    )
    stencil = (smooth_numpy(radius / 1.5) / 1.5 - smooth_numpy(radius / 3.0) / 3.0) / 2.0 ** (
        level - 1
    )
    waves = np.cos(2.0 * np.pi * offsets[:, None] * frequencies(extent)[None, :] / extent)
    table = np.zeros((16, 128))
    table[:, :extent] = (stencil[3:, 3:] @ waves).reshape(16, extent)
    return table.astype(np.float32)


def placed_at(block, row, column):
    matrix = np.zeros((128, 128))
    matrix[row : row + block.shape[0], column : column + block.shape[1]] = block
    return matrix


(
    C_M12,
    C_M23,
    C_BD0,
    C_BD1,
    C_NZ0,
    C_NZ1,
    C_M23T,
    C_M12T,
    C_UR,
    C_PU,
    C_M12B,
) = (0, 1, 5, 6, 7, 8, 9, 10, 11, 12, 13)


@functools.cache
def split_constants():
    def down(count):
        return (real_basis(count // 2) @ restriction(count) @ real_basis(count).T).T

    m12, m23, m34 = down(128), down(64), down(32)
    stack = [placed_at(m12, 0, 0)]
    stack += [placed_at(m23, 0, 32 * place) for place in range(4)]
    for half in range(2):
        matrix = np.zeros((128, 128))
        for place in range(4):
            matrix += placed_at(m34, 32 * place, 64 * half + 16 * place)
        stack.append(matrix)
    for half in range(2):
        matrix = np.zeros((128, 128))
        for place in range(4):
            matrix += placed_at(m34.T, 64 * half + 16 * place, 0)
        stack.append(matrix)
    stack += [placed_at(m23.T, 0, 0), placed_at(m12.T, 0, 0)]
    along_x = restriction(64)
    columns = (np.arange(64) - 8) % 64
    stack.append(placed_at((real_basis(32) @ along_x)[:, columns], 0, 0))
    rows = (np.arange(16) - 2) % 64
    stack.append(placed_at((real_basis(32) @ along_x).T[rows], 0, 0))
    stack.append(placed_at(m12, 0, 64))
    return split_pair(np.stack(stack))


def split_pair(matrix):
    high = matrix.astype(np.float32).astype(BF16)
    low = (matrix - high.astype(np.float64)).astype(np.float32).astype(BF16)
    return high, low


@functools.cache
def coarse_table():
    counts = (32, 64, 16)
    signed = [np.where(np.arange(c) > c // 2, np.arange(c) - c, np.arange(c)) for c in counts]
    radius = np.sqrt(
        signed[0][:, None, None] ** 2.0
        + signed[1][None, :, None] ** 2.0
        + signed[2][None, None, :] ** 2.0
    )
    kernel = smooth_numpy(radius / 1.5) / 12.0
    wave_x = np.cos(2.0 * np.pi * np.outer(frequencies(32), np.arange(32)) / 32)
    wave_z = np.cos(2.0 * np.pi * np.outer(frequencies(16), np.arange(16)) / 16)
    along_y = np.einsum("ax,xyz,bz->aby", wave_x, kernel, wave_z)
    down_y = restriction(128)
    differ = (np.arange(64)[:, None] - np.arange(64)[None, :]) % 64
    up_rows = down_y.T[(np.arange(4) - 2) % 128]
    folded = np.einsum("cm,abmn->abcn", up_rows, along_y[:, :, differ])
    folded = np.einsum("abcn,ny->abcy", folded, down_y)
    folded = folded.reshape(2, 16, 16, 4, 32, 4).transpose(3, 4, 1, 0, 5, 2)
    folded = folded.reshape(4, 32, 16, 128)
    extended = folded[:, (np.arange(35) - 3) % 32]
    return extended.astype(np.float32)


def split(value):
    high = value.astype(BF16)
    low = (value - high.astype(F32)).astype(BF16)
    return high, low


def mm(a, b):
    return jnp.dot(a, b, preferred_element_type=F32)


def times_const(value, high_w, low_w):
    high, low = split(value)
    return mm(high, high_w) + (mm(low, high_w) + mm(high, low_w))


def const_times(high_w, low_w, value):
    high, low = split(value)
    return mm(high_w, high) + (mm(high_w, low) + mm(low_w, high))


def spline_weights(frac):
    def near_weight(distance):
        return (1.0 - distance) * (1.0 + distance - 1.5 * distance * distance)

    def far_weight(distance):
        return -0.5 * (distance - 1.0) * (2.0 - distance) * (2.0 - distance)

    return (
        far_weight(1.0 + frac),
        near_weight(frac),
        near_weight(1.0 - frac),
        far_weight(2.0 - frac),
    )


def tap_table(distance, weights):
    result = jnp.zeros(distance.shape, F32)
    for tap in range(4):
        result = jnp.where(distance == tap, weights[tap], result)
    return result


def rows_of(row):
    packed = jnp.broadcast_to(row, (16, row.shape[1])).astype(BF16)
    return jnp.concatenate([packed] * (NZ // 16), axis=0)


def depth_tables(places_ref, base, weights):
    places = jnp.concatenate([places_ref[...]] * (base.shape[1] // 128), axis=1)
    high = low = jnp.zeros(places.shape, BF16)
    for tap in range(4):
        target = ((base + tap) & (NZ - 1)).astype(F32)
        here = places == rows_of(target)
        weight_high = weights[tap].astype(BF16).astype(F32)
        high = jnp.where(here, rows_of(weight_high), high)
        low = jnp.where(here, rows_of(weights[tap] - weight_high), low)
    return high, low


def plane_tables(plane, fraction_ref, cell_ref, places_ref, index_y):
    lanes = pl.ds(pl.multiple_of(plane * PLANE, PLANE), PLANE)
    fraction = jnp.concatenate([fraction_ref[k, :, lanes] for k in range(3)], axis=0)
    weights = spline_weights(fraction)
    cells = cell_ref[:, lanes]
    base_y = (cells[0:1] - (index_y * CY + 1)) & (CY * N_GY - 1)
    places_y = lax.broadcasted_iota(jnp.int32, (EY, PLANE), 0)
    table_y = tap_table(places_y - base_y, [w[1:2] for w in weights])
    tables_z = depth_tables(places_ref, cells[1:2] - 1, [w[2:3] for w in weights])
    return lanes, [w[0:1] for w in weights], table_y, tables_z


def deposit_plane(
    plane, charge_ref, fraction_ref, cell_ref, places_ref, sums, index_y, tables
):
    lanes, along_x, table_y, (z_high, z_low) = plane_tables(
        plane, fraction_ref, cell_ref, places_ref, index_y
    )
    keep_x, keep_y, keep_high, keep_low = tables
    keep_x[plane] = jnp.concatenate(along_x, axis=0)
    keep_y[plane] = table_y
    keep_high[plane] = z_high
    keep_low[plane] = z_low
    charge = charge_ref[:, lanes]
    spread = jnp.concatenate([table_y * (w * charge) for w in along_x], axis=0)
    spread_high, spread_low = split(spread)
    dims = (((1,), (1,)), ((), ()))
    both = jnp.concatenate([spread_high, spread_low], axis=0)
    first = lax.dot_general(both, z_high, dims, preferred_element_type=F32)
    second = lax.dot_general(spread_high, z_low, dims, preferred_element_type=F32)
    contrib = first[: 4 * EY] + first[4 * EY :] + second
    for tap in range(4):
        sums[plane + tap] = sums[plane + tap] + contrib[EY * tap : EY * (tap + 1)]


def sample_plane(plane, tables, window_ref, atom_ref):
    keep_x, keep_y, keep_high, keep_low = tables
    lanes = pl.ds(pl.multiple_of(plane * PLANE, PLANE), PLANE)
    high, low = split(window_ref[pl.ds(plane, 4)].reshape(4 * EY, NZ))
    z_high, z_low = keep_high[plane], keep_low[plane]
    projected = mm(
        jnp.concatenate([high, low], axis=1), jnp.concatenate([z_high, z_high], axis=0)
    ) + mm(high, z_low)
    total = jnp.zeros((EY, PLANE), F32)
    for tap in range(4):
        total = total + keep_x[plane, tap : tap + 1, :] * projected[EY * tap : EY * (tap + 1)]
    atom_ref[:, lanes] = jnp.sum(total * keep_y[plane], axis=0, keepdims=True)


NEIGHBOURS = ((1, 0), (-1, 0), (0, 1), (0, -1), (1, 1), (1, -1), (-1, 1), (-1, -1))
N_SEMS = 16 + 8 + 7 + 4 + 15 + 16
HALF_GY = N_GY // 2
FAR_FIRST = sorted(range(1, HALF_GY), key=lambda k: -min(k, HALF_GY - k))


def prolonged_rows(get, row):
    middle = row // 2
    if row % 2 == 0:
        return get(middle)
    return 0.5625 * (get(middle) + get(middle + 1)) - 0.0625 * (get(middle - 1) + get(middle + 2))


N_IN = 14
N_FIRST = 6


def levels_entry(*refs):
    sources, outputs = refs[:N_IN], refs[N_IN : N_IN + 2]
    inputs, sems, rest = refs[N_IN + 2 : 2 * N_IN + 2], refs[2 * N_IN + 2], refs[2 * N_IN + 3 :]
    copies = [
        pltpu.make_async_copy(source, target, sems.at[number])
        for number, (source, target) in enumerate(zip(sources, inputs))
    ]
    for copy in copies:
        copy.start()
    levels_kernel(*inputs, *outputs, *rest, copies[:N_FIRST], copies[N_FIRST:])


def levels_kernel(
    charge_ref,
    fraction_ref,
    cell_ref,
    places_ref,
    forward_high_ref,
    forward_low_ref,
    inverse_high_ref,
    inverse_low_ref,
    k1_ref,
    k2_ref,
    k3_ref,
    high_ref,
    low_ref,
    table,
    grid_ref,
    atom_ref,
    keep_x,
    keep_y,
    keep_high,
    keep_low,
    window,
    sums,
    own,
    edge,
    from_x,
    from_y,
    from_corner,
    from_x2,
    from_y2,
    from_corner2,
    own2,
    edge2,
    q1,
    sums1,
    smooth1,
    part1,
    q2,
    smooth2,
    part2,
    ring_x,
    halo,
    ring_y,
    q3,
    field3,
    up3,
    up2,
    send_sems,
    recv_sems,
    first_copies,
    later_copies,
):
    index_x = lax.axis_index("gx")
    index_y = lax.axis_index("gy")
    core = lax.rem(index_y, 2)
    tables = (keep_x, keep_y, keep_high, keep_low)

    def device(step_x, step_y):
        return (
            lax.rem(index_x + (step_x + N_GX), N_GX),
            lax.rem(index_y + (step_y + N_GY), N_GY),
        )

    barrier = pltpu.get_barrier_semaphore()
    peers = [(x, 0) for x in range(1, N_GX)]
    peers += [(0, y) for y in range(2, N_GY, 2)] + [(0, 1), (0, N_GY - 1)]
    peers += [(x, y) for x, y in NEIGHBOURS if x and y]
    for step_x, step_y in peers:
        pl.semaphore_signal(
            barrier, inc=1, device_id=device(step_x, step_y), device_id_type=MESH_IDS
        )

    started = []

    def send(number, source, target, step_x, step_y):
        copy = pltpu.make_async_remote_copy(
            src_ref=source,
            dst_ref=target,
            send_sem=send_sems.at[number],
            recv_sem=recv_sems.at[number],
            device_id=device(step_x, step_y),
            device_id_type=MESH_IDS,
        )
        copy.start()
        started.append(copy)
        return copy

    sums[...] = jnp.zeros_like(sums)

    def clear(x, carried):
        q1[x] = jnp.zeros((40, NZ), F32)
        return carried

    lax.fori_loop(0, 41, clear, 0)

    for copy in first_copies:
        copy.wait()

    def deposit(first, last, row, count, send_finished):
        def step(plane, carried):
            deposit_plane(
                plane, charge_ref, fraction_ref, cell_ref, places_ref, sums, index_y, tables
            )
            return carried

        lax.fori_loop(first, last, step, 0, unroll=2)
        flat = sums[row : row + count].reshape(count * EY, NZ)
        value = times_const(flat, forward_high_ref[...], forward_low_ref[...])
        own[row : row + count] = value.reshape(count, EY, NZ)
        edge[row : row + count] = own[row : row + count, 11:19, :]

        def restrict_y(x, carried):
            q1[x + 3, 8:32, :] = own[x]
            total = jnp.zeros((16, NZ), F32)
            for offset, weight in taps:
                total = total + weight * q1[x + 3, pl.ds(6 + offset, 16, stride=2), :]
            part1[x] = total
            return carried

        send_finished()
        lax.fori_loop(row, row + count, restrict_y, 0)

    round1 = []

    def send_edges(number, row, count):
        rows = pl.ds(row, count)
        round1.append(send(number, edge.at[rows], from_y.at[0, rows], 0, 1))
        round1.append(send(number + 1, own.at[rows, 0:8, :], from_y.at[1, rows], 0, -1))

    high_x, low_x = pl.ds(29, 6), pl.ds(0, 6)

    def send_high():
        pl.semaphore_wait(barrier, len(peers))
        round1.append(send(0, edge.at[high_x], from_corner.at[0], 1, 1))
        round1.append(send(1, own.at[high_x, 0:8, :], from_corner.at[1], 1, -1))
        round1.append(send(2, own.at[high_x], from_x.at[0], 1, 0))
        send_edges(6, 29, 6)

    def send_low():
        round1.append(send(3, edge.at[low_x], from_corner.at[2], -1, 1))
        round1.append(send(4, own.at[low_x, 0:8, :], from_corner.at[3], -1, -1))
        round1.append(send(5, own.at[low_x], from_x.at[1], -1, 0))
        send_edges(8, 0, 6)

    deposit(26, 32, 29, 6, send_high)
    deposit(0, 6, 0, 6, send_low)
    deposit(6, 14, 6, 8, lambda: send_edges(10, 6, 8))
    deposit(14, 22, 14, 8, lambda: send_edges(12, 14, 8))
    deposit(22, 26, 22, 7, lambda: send_edges(14, 22, 7))

    for copy in later_copies:
        copy.wait()

    rows = []
    for m in range(-1, 19):
        total = jnp.zeros((16, NZ), F32)
        for offset, weight in taps:
            if 0 <= 2 * m + offset < EX:
                total = total + weight * part1[2 * m + offset]
        rows.append(total)
    level2 = times_const(
        jnp.concatenate(rows[0::2], axis=0), high_ref[C_M12], low_ref[C_M12]
    ) + times_const(jnp.concatenate(rows[1::2], axis=0), high_ref[C_M12B], low_ref[C_M12B])
    own2[...] = level2.reshape(10, 16, NZ)
    edge2[...] = own2[:, 5:13, :]

    round2 = []
    for number in (4, 5, 6, 7, 0, 1, 2, 3):
        step_x, step_y = NEIGHBOURS[number]
        rows = {0: pl.ds(0, 10), 1: pl.ds(6, 4), -1: pl.ds(0, 4)}[step_x]
        if step_y == 0:
            source, target = own2.at[rows], from_x2.at[number]
        elif step_x == 0:
            source = edge2 if step_y == 1 else own2.at[:, 0:8, :]
            target = from_y2.at[number - 2]
        else:
            source = edge2.at[rows] if step_y == 1 else own2.at[rows, 0:8, :]
            target = from_corner2.at[number - 4]
        round2.append(send(16 + number, source, target, step_x, step_y))

    q2[...] = jnp.zeros_like(q2)
    q3[:, 24:32, :] = jnp.zeros((15, 8, NZ), F32)
    for pair in range(10):
        q2[3 + 2 * pair, 7:23, :] = own2[pair]
        q2[4 + 2 * pair, 7:23, :] = pltpu.roll(own2[pair], 64, axis=1)

    for copy in round2:
        copy.wait_recv()

    def add_to2(row, start, value):
        end = start + value.shape[0]
        for place, plane in ((row, value), (row + 1, pltpu.roll(value, 64, axis=1))):
            if 0 <= place < 26:
                q2[place, start:end, :] = q2[place, start:end, :] + plane

    for pair in range(10):
        add_to2(3 + 2 * pair, 4, from_y2[0, pair])
        add_to2(3 + 2 * pair, 15, from_y2[1, pair])
    for side, first in ((0, -1), (1, 19)):
        for pair in range(4):
            add_to2(first + 2 * pair, 7, from_x2[side, pair])
            add_to2(first + 2 * pair, 4, from_corner2[2 * side, pair])
            add_to2(first + 2 * pair, 15, from_corner2[2 * side + 1, pair])

    for m in range(8):
        total = jnp.zeros((24, NZ), F32)
        for offset, weight in taps:
            total = total + weight * q2[2 * m + 4 + offset, 0:24, :]
        part2[24 * m : 24 * (m + 1), :] = total
    tile = jnp.zeros((8, NZ), F32)
    for n in range(4):
        total = jnp.zeros((8, NZ), F32)
        for offset, weight in taps:
            total = total + weight * part2[pl.ds(8 + 2 * n + offset, 8, stride=24), :]
        tile = tile + times_const(total, high_ref[C_M23 + n], low_ref[C_M23 + n])
    ring_x[1] = tile

    round3 = []
    for step in (4, 5, 3, 6, 2, 7, 1):
        place = (N_GX - step + 1) % N_GX
        round3.append(send(23 + step, ring_x.at[1], ring_x.at[place], step, 0))

    def stencil_small(source, row, start, count, k_ref):
        total = jnp.zeros((count, NZ), F32)
        for across in range(4):
            for along in range(4):
                value = None
                for sign_r in sorted({across, -across}):
                    for sign_s in sorted({along, -along}):
                        piece = source[row + sign_r, start + sign_s : start + sign_s + count, :]
                        value = piece if value is None else value + piece
                total = total + k_ref[4 * across + along : 4 * across + along + 1, :] * value
        return total

    def stencil2(x, carried):
        smooth2[x] = stencil_small(q2, x + 3, 7, 16, k2_ref)
        return carried

    lax.fori_loop(0, 20, stencil2, 0)

    for copy in round3:
        copy.wait_recv()

    round4 = []
    for number, step in enumerate((1, -1, 2, -2)):
        round4.append(send(31 + number, ring_x.at[0:3], halo.at[2 - step], 0, step))
    column = const_times(
        high_ref[C_UR, 0:32, 0:64], low_ref[C_UR, 0:32, 0:64], ring_x[...].reshape(64, NZ)
    )
    ring_y[core] = times_const(column[0:16], high_ref[C_BD0], low_ref[C_BD0]) + times_const(
        column[16:32], high_ref[C_BD1], low_ref[C_BD1]
    )
    round5 = {}
    for step in FAR_FIRST:
        place = 2 * (HALF_GY - step) + core
        round5[step] = send(34 + step, ring_y.at[core], ring_y.at[place], 0, 2 * step)

    def hand_on(place):
        row = ring_y.at[2 * place + core]
        return send(50 + place, row, row, 0, 1 - 2 * core)

    handed = [hand_on(0)]

    for copy in round1:
        copy.wait_recv()

    def add_y(x, carried):
        q1[x + 3, 3:11, :] = q1[x + 3, 3:11, :] + from_y[0, x]
        q1[x + 3, 24:32, :] = q1[x + 3, 24:32, :] + from_y[1, x]
        return carried

    lax.fori_loop(0, EX, add_y, 0)
    for side, start in ((0, 0), (1, 35)):
        for x in range(6):
            row = start + x
            q1[row, 8:32, :] = q1[row, 8:32, :] + from_x[side, x]
            q1[row, 3:11, :] = q1[row, 3:11, :] + from_corner[2 * side, x]
            q1[row, 24:32, :] = q1[row, 24:32, :] + from_corner[2 * side + 1, x]

    def sum_y(x, carried):
        for dy in range(1, 4):
            sums1[dy - 1, x] = q1[x, 8 + dy : 32 + dy, :] + q1[x, 8 - dy : 32 - dy, :]
        return carried

    lax.fori_loop(0, 41, sum_y, 0)

    def stencil1(x, carried):
        total = jnp.zeros((EY, NZ), F32)
        for dy in range(4):
            for dx in range(4):
                if dy == 0:
                    value = q1[x + 3 + dx, 8:32, :]
                    if dx:
                        value = value + q1[x + 3 - dx, 8:32, :]
                else:
                    value = sums1[dy - 1, x + 3 + dx]
                    if dx:
                        value = value + sums1[dy - 1, x + 3 - dx]
                total = total + k1_ref[4 * dx + dy : 4 * dx + dy + 1, :] * value
        smooth1[x] = total
        return carried

    lax.fori_loop(0, EX, stencil1, 0)

    for step in reversed(FAR_FIRST):
        round5[step].wait_recv()
        handed.append(hand_on(HALF_GY - step))

    halo[2] = ring_x[0:3]
    for copy in round4:
        copy.wait_recv()
    for y in range(-5, 10):
        place = y % 4
        source = halo[y // 4 + 2].reshape(24, NZ)
        if place:
            source = pltpu.roll(source, NZ - 32 * place, axis=1)
        q3[y + 5, 0:24, :] = source

    def stencil3(y, carried):
        field3[y] = stencil_small(q3, y + 3, 6, 16, k3_ref)
        return carried

    lax.fori_loop(0, 9, stencil3, 0)

    for copy in handed:
        copy.wait_recv()

    def add_slot(slot, totals):
        values = ring_y[slot]
        return tuple(
            total + table[row % 4, slot + (3 - row // 4) - core] * values
            for row, total in enumerate(totals)
        )

    coarse = lax.fori_loop(
        0, N_GY, add_slot, tuple(jnp.zeros((16, NZ), F32) for _ in range(9)), unroll=4
    )
    coarse = jnp.concatenate(coarse, axis=0)
    half0 = times_const(coarse, high_ref[C_NZ0], low_ref[C_NZ0])
    half1 = times_const(coarse, high_ref[C_NZ1], low_ref[C_NZ1])
    for row in range(9):
        both = jnp.concatenate(
            [half0[16 * row : 16 * (row + 1)], half1[16 * row : 16 * (row + 1)]], axis=0
        )
        field3[row] = field3[row] + const_times(
            high_ref[C_PU, 0:16, 0:32], low_ref[C_PU, 0:16, 0:32], both
        )

    fields = [prolonged_rows(lambda m: field3[m + 2], y) for y in range(-1, 11)]
    up3[...] = times_const(jnp.concatenate(fields, axis=0), high_ref[C_M23T], low_ref[C_M23T])

    def column3(m):
        return up3[pl.ds(m + 2, 12, stride=16), :]

    for x in range(-1, 19):
        smooth2[x + 1, 0:12, :] = smooth2[x + 1, 0:12, :] + prolonged_rows(column3, x)

    part = times_const(
        smooth2[...].reshape(20 * 16, NZ), high_ref[C_M12T], low_ref[C_M12T]
    ).reshape(20, 16, NZ)
    smooth2[...] = part

    def widen_y(x, carried):
        rows = [smooth2[x, n : n + 12, :] for n in range(4)]
        up2[x, pl.ds(0, 12, stride=2), :] = rows[1]
        up2[x, pl.ds(1, 12, stride=2), :] = 0.5625 * (rows[1] + rows[2]) - 0.0625 * (
            rows[0] + rows[3]
        )
        return carried

    lax.fori_loop(0, 20, widen_y, 0)

    def widen_x(m, carried):
        values = [up2[m + n] for n in range(4)]
        sums[2 * m] = smooth1[2 * m] + values[1]
        sums[2 * m + 1] = smooth1[2 * m + 1] + (
            0.5625 * (values[1] + values[2]) - 0.0625 * (values[0] + values[3])
        )
        return carried

    lax.fori_loop(0, 17, widen_x, 0)
    sums[34] = smooth1[34] + up2[18]

    flat = sums[...].reshape(EX * EY, NZ)
    value = times_const(flat, inverse_high_ref[...], inverse_low_ref[...])
    window[...] = value.reshape(EX, EY, NZ)
    grid_ref[...] = window[:CX, :CY, :]

    def sample(plane, carried):
        sample_plane(plane, tables, window, atom_ref)
        return carried

    lax.fori_loop(0, CX, sample, 0, unroll=2)

    for copy in started:
        copy.wait_send()


def finish_kernel(grid_in, atom_in, grid_out, atom_out, grid, atom, sems):
    pairs = ((grid_in, grid, grid_out), (atom_in, atom, atom_out))
    loads = [
        pltpu.make_async_copy(source, middle, sems.at[number])
        for number, (source, middle, target) in enumerate(pairs)
    ]
    stores = [
        pltpu.make_async_copy(middle, target, sems.at[2 + number])
        for number, (source, middle, target) in enumerate(pairs)
    ]
    for load in loads:
        load.start()
    for load, store in zip(loads, stores):
        load.wait()
        store.start()
    for store in stores:
        store.wait()


def in_vmem(count):
    return [pl.BlockSpec(memory_space=pltpu.VMEM)] * count


def local(charges, fractions, cells):
    charge = charges.reshape(1, ATOMS_DEV)
    fraction = fractions.reshape(3, 1, ATOMS_DEV)
    cell = cells.reshape(2, ATOMS_DEV)
    places = jnp.asarray(np.tile(np.arange(NZ)[:, None], (1, 128)).astype(BF16))
    forward = [jnp.asarray(part) for part in split_pair(real_basis(NZ).T)]
    inverse = [jnp.asarray(part) for part in split_pair(real_basis(NZ))]
    high, low = split_constants()
    inputs = [
        charge,
        fraction,
        cell,
        places,
        *forward,
        *inverse,
        jnp.asarray(stencil_table(1, 128)),
        jnp.asarray(stencil_table(2, 64)),
        jnp.asarray(stencil_table(3, 32)),
        jnp.asarray(high),
        jnp.asarray(low),
        jnp.asarray(coarse_table()),
    ]
    potential, sampled = pl.pallas_call(
        levels_entry,
        out_shape=(
            jax.ShapeDtypeStruct((CX, CY, NZ), F32),
            jax.ShapeDtypeStruct((1, ATOMS_DEV), F32),
        ),
        in_specs=[pl.BlockSpec(memory_space=pltpu.HBM)] * N_IN,
        out_specs=in_vmem(2),
        scratch_shapes=[pltpu.VMEM(value.shape, value.dtype) for value in inputs]
        + [
            pltpu.SemaphoreType.DMA((N_IN,)),
            pltpu.VMEM((CX, 4, PLANE), F32),
            pltpu.VMEM((CX, EY, PLANE), F32),
            pltpu.VMEM((CX, NZ, PLANE), BF16),
            pltpu.VMEM((CX, NZ, PLANE), BF16),
            pltpu.VMEM((EX, EY, NZ), F32),
            pltpu.VMEM((EX, EY, NZ), F32),
            pltpu.VMEM((EX, EY, NZ), F32),
            pltpu.VMEM((EX, 8, NZ), F32),
            pltpu.VMEM((2, 6, EY, NZ), F32),
            pltpu.VMEM((2, EX, 8, NZ), F32),
            pltpu.VMEM((4, 6, 8, NZ), F32),
            pltpu.VMEM((2, 4, 16, NZ), F32),
            pltpu.VMEM((2, 10, 8, NZ), F32),
            pltpu.VMEM((4, 4, 8, NZ), F32),
            pltpu.VMEM((10, 16, NZ), F32),
            pltpu.VMEM((10, 8, NZ), F32),
            pltpu.VMEM((41, 40, NZ), F32),
            pltpu.VMEM((3, 41, EY, NZ), F32),
            pltpu.VMEM((EX, EY, NZ), F32),
            pltpu.VMEM((EX, 16, NZ), F32),
            pltpu.VMEM((26, 32, NZ), F32),
            pltpu.VMEM((20, 16, NZ), F32),
            pltpu.VMEM((8 * 24, NZ), F32),
            pltpu.VMEM((N_GX, 8, NZ), F32),
            pltpu.VMEM((5, 3, 8, NZ), F32),
            pltpu.VMEM((N_GY, 16, NZ), F32),
            pltpu.VMEM((15, 32, NZ), F32),
            pltpu.VMEM((9, 16, NZ), F32),
            pltpu.VMEM((12 * 16, NZ), F32),
            pltpu.VMEM((20, EY, NZ), F32),
            pltpu.SemaphoreType.DMA((N_SEMS,)),
            pltpu.SemaphoreType.DMA((N_SEMS,)),
        ],
        compiler_params=pltpu.CompilerParams(collective_id=0, has_side_effects=True),
        name="levels",
    )(*inputs)
    potential, sampled = pl.pallas_call(
        finish_kernel,
        out_shape=(
            jax.ShapeDtypeStruct((CX, CY, NZ), F32),
            jax.ShapeDtypeStruct((1, ATOMS_DEV), F32),
        ),
        in_specs=[pl.BlockSpec(memory_space=pl.ANY)] * 2,
        out_specs=[pl.BlockSpec(memory_space=pl.ANY)] * 2,
        scratch_shapes=[
            pltpu.VMEM((CX, CY, NZ), F32),
            pltpu.VMEM((1, ATOMS_DEV), F32),
            pltpu.SemaphoreType.DMA((4,)),
        ],
        name="finish",
    )(potential, sampled)
    return potential, sampled.reshape(1, 1, ATOMS_DEV)


def solution(mesh):
    placed = (P("gx", "gy", None), P("gx", "gy", None, None), P("gx", "gy", None, None))
    return jax.shard_map(
        local,
        mesh=mesh,
        in_specs=placed,
        out_specs=(P("gx", "gy", None), P("gx", "gy", None)),
        check_vma=False,
    )
```

```python
import functools

import jax
import jax.numpy as jnp
import numpy as np
from jax import lax
from jax.experimental import pallas as pl
from jax.experimental.pallas import tpu as pltpu
from jax.sharding import PartitionSpec as P

CX = 32
CY = 16
NZ = 128
ATOMS_DEV = 16384
N_GX = 8
N_GY = 32
PLANE = ATOMS_DEV // CX
EX = CX + 3
EY = 24
MESH_IDS = pl.DeviceIdType.MESH
BF16 = jnp.bfloat16
F32 = jnp.float32
taps = ((-3, -0.0625), (-1, 0.5625), (0, 1.0), (1, 0.5625), (3, -0.0625))


def smooth_numpy(rho):
    return np.where(
        rho < 1.0, 1.875 - 1.25 * rho * rho + 0.375 * rho**4, 1.0 / np.maximum(rho, 1.0)
    )


def frequencies(count):
    inner = np.repeat(np.arange(1, count // 2), 2)
    return np.concatenate([[0], inner, [count // 2]])


def real_basis(count):
    wave = frequencies(count)
    angle = 2.0 * np.pi * wave[:, None] * np.arange(count)[None, :] / count
    is_sine = np.zeros(count, bool)
    is_sine[2:-1:2] = True
    basis = np.where(is_sine[:, None], np.sin(angle), np.cos(angle)) * np.sqrt(2.0 / count)
    basis[0] /= np.sqrt(2.0)
    basis[-1] /= np.sqrt(2.0)
    return basis


def restriction(count):
    matrix = np.zeros((count // 2, count))
    for row in range(count // 2):
        for offset, weight in taps:
            matrix[row, (2 * row + offset) % count] += weight
    return matrix


def stencil_table(level, extent):
    offsets = np.arange(-3, 4) * 1.0
    radius = np.sqrt(
        offsets[:, None, None] ** 2 + offsets[None, :, None] ** 2 + offsets[None, None, :] ** 2
    )
    stencil = (smooth_numpy(radius / 1.5) / 1.5 - smooth_numpy(radius / 3.0) / 3.0) / 2.0 ** (
        level - 1
    )
    waves = np.cos(2.0 * np.pi * offsets[:, None] * frequencies(extent)[None, :] / extent)
    table = np.zeros((16, 128))
    table[:, :extent] = (stencil[3:, 3:] @ waves).reshape(16, extent)
    return table.astype(np.float32)


def placed_at(block, row, column):
    matrix = np.zeros((128, 128))
    matrix[row : row + block.shape[0], column : column + block.shape[1]] = block
    return matrix


(
    C_M12,
    C_M23,
    C_BD0,
    C_BD1,
    C_NZ0,
    C_NZ1,
    C_M23T,
    C_M12T,
    C_UR,
    C_PU,
    C_M12B,
) = (0, 1, 5, 6, 7, 8, 9, 10, 11, 12, 13)


@functools.cache
def split_constants():
    def down(count):
        return (real_basis(count // 2) @ restriction(count) @ real_basis(count).T).T

    m12, m23, m34 = down(128), down(64), down(32)
    stack = [placed_at(m12, 0, 0)]
    stack += [placed_at(m23, 0, 32 * place) for place in range(4)]
    for half in range(2):
        matrix = np.zeros((128, 128))
        for place in range(4):
            matrix += placed_at(m34, 32 * place, 64 * half + 16 * place)
        stack.append(matrix)
    for half in range(2):
        matrix = np.zeros((128, 128))
        for place in range(4):
            matrix += placed_at(m34.T, 64 * half + 16 * place, 0)
        stack.append(matrix)
    stack += [placed_at(m23.T, 0, 0), placed_at(m12.T, 0, 0)]
    along_x = restriction(64)
    columns = (np.arange(64) - 8) % 64
    stack.append(placed_at((real_basis(32) @ along_x)[:, columns], 0, 0))
    rows = (np.arange(16) - 2) % 64
    stack.append(placed_at((real_basis(32) @ along_x).T[rows], 0, 0))
    stack.append(placed_at(m12, 0, 64))
    return split_pair(np.stack(stack))


def split_pair(matrix):
    high = matrix.astype(np.float32).astype(BF16)
    low = (matrix - high.astype(np.float64)).astype(np.float32).astype(BF16)
    return high, low


@functools.cache
def coarse_table():
    counts = (32, 64, 16)
    signed = [np.where(np.arange(c) > c // 2, np.arange(c) - c, np.arange(c)) for c in counts]
    radius = np.sqrt(
        signed[0][:, None, None] ** 2.0
        + signed[1][None, :, None] ** 2.0
        + signed[2][None, None, :] ** 2.0
    )
    kernel = smooth_numpy(radius / 1.5) / 12.0
    wave_x = np.cos(2.0 * np.pi * np.outer(frequencies(32), np.arange(32)) / 32)
    wave_z = np.cos(2.0 * np.pi * np.outer(frequencies(16), np.arange(16)) / 16)
    along_y = np.einsum("ax,xyz,bz->aby", wave_x, kernel, wave_z)
    down_y = restriction(128)
    differ = (np.arange(64)[:, None] - np.arange(64)[None, :]) % 64
    up_rows = down_y.T[(np.arange(4) - 2) % 128]
    folded = np.einsum("cm,abmn->abcn", up_rows, along_y[:, :, differ])
    folded = np.einsum("abcn,ny->abcy", folded, down_y)
    folded = folded.reshape(2, 16, 16, 4, 32, 4).transpose(3, 4, 1, 0, 5, 2)
    folded = folded.reshape(4, 32, 16, 128)
    extended = folded[:, (np.arange(35) - 3) % 32]
    return extended.astype(np.float32)


def split(value):
    high = value.astype(BF16)
    low = (value - high.astype(F32)).astype(BF16)
    return high, low


def mm(a, b):
    return jnp.dot(a, b, preferred_element_type=F32)


def times_const(value, high_w, low_w):
    high, low = split(value)
    return mm(high, high_w) + (mm(low, high_w) + mm(high, low_w))


def const_times(high_w, low_w, value):
    high, low = split(value)
    return mm(high_w, high) + (mm(high_w, low) + mm(low_w, high))


def spline_weights(frac):
    def near_weight(distance):
        return (1.0 - distance) * (1.0 + distance - 1.5 * distance * distance)

    def far_weight(distance):
        return -0.5 * (distance - 1.0) * (2.0 - distance) * (2.0 - distance)

    return (
        far_weight(1.0 + frac),
        near_weight(frac),
        near_weight(1.0 - frac),
        far_weight(2.0 - frac),
    )


BY_ROW = lax.GatherDimensionNumbers(
    offset_dims=(),
    collapsed_slice_dims=(0,),
    start_index_map=(0,),
    operand_batching_dims=(1,),
    start_indices_batching_dims=(1,),
)


def picked(table, index):
    return jnp.concatenate(
        [
            lax.gather(
                table[:, lane : lane + 128],
                index[:, lane : lane + 128, None],
                BY_ROW,
                slice_sizes=(1, 1),
                mode=lax.GatherScatterMode.PROMISE_IN_BOUNDS,
            )
            for lane in range(0, table.shape[1], 128)
        ],
        axis=1,
    )


def eight_rows(rows):
    return jnp.concatenate(rows + [jnp.zeros((4, rows[0].shape[1]), F32)], axis=0)


def index_rows(base, first, period):
    places = lax.broadcasted_iota(jnp.int32, (8, base.shape[1]), 0) + first
    return jnp.minimum((places - base) & (period - 1), 7)


def depth_tables(base, weights):
    rounded = [w.astype(BF16).astype(F32) for w in weights]
    high_rows = eight_rows(rounded)
    low_rows = eight_rows([w - r for w, r in zip(weights, rounded)])
    highs, lows = [], []
    for first in range(0, NZ, 16):
        indices = [index_rows(base, first + part, NZ) for part in (0, 8)]
        for rows, result in ((high_rows, highs), (low_rows, lows)):
            pair = jnp.concatenate([picked(rows, index) for index in indices], axis=0)
            result.append(pair.astype(BF16))
    return jnp.concatenate(highs, axis=0), jnp.concatenate(lows, axis=0)


def plane_tables(plane, fraction_ref, cell_ref, index_y):
    lanes = pl.ds(pl.multiple_of(plane * PLANE, PLANE), PLANE)
    fraction = jnp.concatenate([fraction_ref[k, :, lanes] for k in range(3)], axis=0)
    weights = spline_weights(fraction)
    cells = cell_ref[:, lanes]
    base_y = (cells[0:1] - (index_y * CY + 1)) & (CY * N_GY - 1)
    rows_y = eight_rows([w[1:2] for w in weights])
    table_y = jnp.concatenate(
        [picked(rows_y, index_rows(base_y, first, 32)) for first in range(0, EY, 8)], axis=0
    )
    tables_z = depth_tables(cells[1:2] - 1, [w[2:3] for w in weights])
    return lanes, [w[0:1] for w in weights], table_y, tables_z


def deposit_plane(
    plane, charge_ref, fraction_ref, cell_ref, sums, index_y, tables
):
    lanes, along_x, table_y, (z_high, z_low) = plane_tables(
        plane, fraction_ref, cell_ref, index_y
    )
    keep_x, keep_y, keep_high, keep_low = tables
    keep_x[plane] = jnp.concatenate(along_x, axis=0)
    keep_y[plane] = table_y
    keep_high[plane] = z_high
    keep_low[plane] = z_low
    charge = charge_ref[:, lanes]
    spread = jnp.concatenate([table_y * (w * charge) for w in along_x], axis=0)
    spread_high, spread_low = split(spread)
    dims = (((1,), (1,)), ((), ()))
    both = jnp.concatenate([spread_high, spread_low], axis=0)
    first = lax.dot_general(both, z_high, dims, preferred_element_type=F32)
    second = lax.dot_general(spread_high, z_low, dims, preferred_element_type=F32)
    contrib = first[: 4 * EY] + first[4 * EY :] + second
    for tap in range(4):
        sums[plane + tap] = sums[plane + tap] + contrib[EY * tap : EY * (tap + 1)]


def sample_plane(plane, tables, window_ref, atom_ref):
    keep_x, keep_y, keep_high, keep_low = tables
    lanes = pl.ds(pl.multiple_of(plane * PLANE, PLANE), PLANE)
    high, low = split(window_ref[pl.ds(plane, 4)].reshape(4 * EY, NZ))
    z_high, z_low = keep_high[plane], keep_low[plane]
    projected = mm(
        jnp.concatenate([high, low], axis=1), jnp.concatenate([z_high, z_high], axis=0)
    ) + mm(high, z_low)
    total = jnp.zeros((EY, PLANE), F32)
    for tap in range(4):
        total = total + keep_x[plane, tap : tap + 1, :] * projected[EY * tap : EY * (tap + 1)]
    atom_ref[:, lanes] = jnp.sum(total * keep_y[plane], axis=0, keepdims=True)


NEIGHBOURS = ((1, 0), (-1, 0), (0, 1), (0, -1), (1, 1), (1, -1), (-1, 1), (-1, -1))
N_SEMS = 16 + 8 + 7 + 4 + 15 + 16
HALF_GY = N_GY // 2
FAR_FIRST = sorted(range(1, HALF_GY), key=lambda k: -min(k, HALF_GY - k))


def prolonged_rows(get, row):
    middle = row // 2
    if row % 2 == 0:
        return get(middle)
    return 0.5625 * (get(middle) + get(middle + 1)) - 0.0625 * (get(middle - 1) + get(middle + 2))


N_IN = 13
N_FIRST = 5


def levels_entry(*refs):
    sources, outputs = refs[:N_IN], refs[N_IN : N_IN + 2]
    inputs, sems, rest = refs[N_IN + 2 : 2 * N_IN + 2], refs[2 * N_IN + 2], refs[2 * N_IN + 3 :]
    copies = [
        pltpu.make_async_copy(source, target, sems.at[number])
        for number, (source, target) in enumerate(zip(sources, inputs))
    ]
    for copy in copies:
        copy.start()
    levels_kernel(*inputs, *outputs, *rest, copies[:N_FIRST], copies[N_FIRST:])


def levels_kernel(
    charge_ref,
    fraction_ref,
    cell_ref,
    forward_high_ref,
    forward_low_ref,
    inverse_high_ref,
    inverse_low_ref,
    k1_ref,
    k2_ref,
    k3_ref,
    high_ref,
    low_ref,
    table,
    grid_ref,
    atom_ref,
    keep_x,
    keep_y,
    keep_high,
    keep_low,
    window,
    sums,
    own,
    edge,
    from_x,
    from_y,
    from_corner,
    from_x2,
    from_y2,
    from_corner2,
    own2,
    edge2,
    q1,
    sums1,
    smooth1,
    part1,
    q2,
    smooth2,
    part2,
    ring_x,
    halo,
    ring_y,
    q3,
    field3,
    up3,
    up2,
    send_sems,
    recv_sems,
    first_copies,
    later_copies,
):
    index_x = lax.axis_index("gx")
    index_y = lax.axis_index("gy")
    core = lax.rem(index_y, 2)
    tables = (keep_x, keep_y, keep_high, keep_low)

    def device(step_x, step_y):
        return (
            lax.rem(index_x + (step_x + N_GX), N_GX),
            lax.rem(index_y + (step_y + N_GY), N_GY),
        )

    barrier = pltpu.get_barrier_semaphore()
    peers = [(x, 0) for x in range(1, N_GX)]
    peers += [(0, y) for y in range(2, N_GY, 2)] + [(0, 1), (0, N_GY - 1)]
    peers += [(x, y) for x, y in NEIGHBOURS if x and y]
    for step_x, step_y in peers:
        pl.semaphore_signal(
            barrier, inc=1, device_id=device(step_x, step_y), device_id_type=MESH_IDS
        )

    started = []

    def send(number, source, target, step_x, step_y):
        copy = pltpu.make_async_remote_copy(
            src_ref=source,
            dst_ref=target,
            send_sem=send_sems.at[number],
            recv_sem=recv_sems.at[number],
            device_id=device(step_x, step_y),
            device_id_type=MESH_IDS,
        )
        copy.start()
        started.append(copy)
        return copy

    sums[...] = jnp.zeros_like(sums)

    def clear(x, carried):
        q1[x] = jnp.zeros((40, NZ), F32)
        return carried

    lax.fori_loop(0, 41, clear, 0)

    for copy in first_copies:
        copy.wait()

    def deposit(first, last, row, count, send_finished):
        def step(plane, carried):
            deposit_plane(
                plane, charge_ref, fraction_ref, cell_ref, sums, index_y, tables
            )
            return carried

        lax.fori_loop(first, last, step, 0, unroll=2)
        flat = sums[row : row + count].reshape(count * EY, NZ)
        value = times_const(flat, forward_high_ref[...], forward_low_ref[...])
        own[row : row + count] = value.reshape(count, EY, NZ)
        edge[row : row + count] = own[row : row + count, 11:19, :]

        def restrict_y(x, carried):
            q1[x + 3, 8:32, :] = own[x]
            total = jnp.zeros((16, NZ), F32)
            for offset, weight in taps:
                total = total + weight * q1[x + 3, pl.ds(6 + offset, 16, stride=2), :]
            part1[x] = total
            return carried

        send_finished()
        lax.fori_loop(row, row + count, restrict_y, 0)

    round1 = []

    def send_edges(number, row, count):
        rows = pl.ds(row, count)
        round1.append(send(number, edge.at[rows], from_y.at[0, rows], 0, 1))
        round1.append(send(number + 1, own.at[rows, 0:8, :], from_y.at[1, rows], 0, -1))

    high_x, low_x = pl.ds(29, 6), pl.ds(0, 6)

    def send_high():
        pl.semaphore_wait(barrier, len(peers))
        round1.append(send(0, edge.at[high_x], from_corner.at[0], 1, 1))
        round1.append(send(1, own.at[high_x, 0:8, :], from_corner.at[1], 1, -1))
        round1.append(send(2, own.at[high_x], from_x.at[0], 1, 0))
        send_edges(6, 29, 6)

    def send_low():
        round1.append(send(3, edge.at[low_x], from_corner.at[2], -1, 1))
        round1.append(send(4, own.at[low_x, 0:8, :], from_corner.at[3], -1, -1))
        round1.append(send(5, own.at[low_x], from_x.at[1], -1, 0))
        send_edges(8, 0, 6)

    deposit(26, 32, 29, 6, send_high)
    deposit(0, 6, 0, 6, send_low)
    deposit(6, 14, 6, 8, lambda: send_edges(10, 6, 8))
    deposit(14, 22, 14, 8, lambda: send_edges(12, 14, 8))
    deposit(22, 26, 22, 7, lambda: send_edges(14, 22, 7))

    for copy in later_copies:
        copy.wait()

    rows = []
    for m in range(-1, 19):
        total = jnp.zeros((16, NZ), F32)
        for offset, weight in taps:
            if 0 <= 2 * m + offset < EX:
                total = total + weight * part1[2 * m + offset]
        rows.append(total)
    level2 = times_const(
        jnp.concatenate(rows[0::2], axis=0), high_ref[C_M12], low_ref[C_M12]
    ) + times_const(jnp.concatenate(rows[1::2], axis=0), high_ref[C_M12B], low_ref[C_M12B])
    own2[...] = level2.reshape(10, 16, NZ)
    edge2[...] = own2[:, 5:13, :]

    round2 = []
    for number in (4, 5, 6, 7, 0, 1, 2, 3):
        step_x, step_y = NEIGHBOURS[number]
        rows = {0: pl.ds(0, 10), 1: pl.ds(6, 4), -1: pl.ds(0, 4)}[step_x]
        if step_y == 0:
            source, target = own2.at[rows], from_x2.at[number]
        elif step_x == 0:
            source = edge2 if step_y == 1 else own2.at[:, 0:8, :]
            target = from_y2.at[number - 2]
        else:
            source = edge2.at[rows] if step_y == 1 else own2.at[rows, 0:8, :]
            target = from_corner2.at[number - 4]
        round2.append(send(16 + number, source, target, step_x, step_y))

    q2[...] = jnp.zeros_like(q2)
    q3[:, 24:32, :] = jnp.zeros((15, 8, NZ), F32)
    for pair in range(10):
        q2[3 + 2 * pair, 7:23, :] = own2[pair]
        q2[4 + 2 * pair, 7:23, :] = pltpu.roll(own2[pair], 64, axis=1)

    for copy in round2:
        copy.wait_recv()

    def add_to2(row, start, value):
        end = start + value.shape[0]
        for place, plane in ((row, value), (row + 1, pltpu.roll(value, 64, axis=1))):
            if 0 <= place < 26:
                q2[place, start:end, :] = q2[place, start:end, :] + plane

    for pair in range(10):
        add_to2(3 + 2 * pair, 4, from_y2[0, pair])
        add_to2(3 + 2 * pair, 15, from_y2[1, pair])
    for side, first in ((0, -1), (1, 19)):
        for pair in range(4):
            add_to2(first + 2 * pair, 7, from_x2[side, pair])
            add_to2(first + 2 * pair, 4, from_corner2[2 * side, pair])
            add_to2(first + 2 * pair, 15, from_corner2[2 * side + 1, pair])

    for m in range(8):
        total = jnp.zeros((24, NZ), F32)
        for offset, weight in taps:
            total = total + weight * q2[2 * m + 4 + offset, 0:24, :]
        part2[24 * m : 24 * (m + 1), :] = total
    tile = jnp.zeros((8, NZ), F32)
    for n in range(4):
        total = jnp.zeros((8, NZ), F32)
        for offset, weight in taps:
            total = total + weight * part2[pl.ds(8 + 2 * n + offset, 8, stride=24), :]
        tile = tile + times_const(total, high_ref[C_M23 + n], low_ref[C_M23 + n])
    ring_x[1] = tile

    round3 = []
    for step in (4, 5, 3, 6, 2, 7, 1):
        place = (N_GX - step + 1) % N_GX
        round3.append(send(23 + step, ring_x.at[1], ring_x.at[place], step, 0))

    def stencil_small(source, row, start, count, k_ref):
        total = jnp.zeros((count, NZ), F32)
        for across in range(4):
            for along in range(4):
                value = None
                for sign_r in sorted({across, -across}):
                    for sign_s in sorted({along, -along}):
                        piece = source[row + sign_r, start + sign_s : start + sign_s + count, :]
                        value = piece if value is None else value + piece
                total = total + k_ref[4 * across + along : 4 * across + along + 1, :] * value
        return total

    def stencil2(x, carried):
        smooth2[x] = stencil_small(q2, x + 3, 7, 16, k2_ref)
        return carried

    lax.fori_loop(0, 20, stencil2, 0)

    for copy in round3:
        copy.wait_recv()

    round4 = []
    for number, step in enumerate((1, -1, 2, -2)):
        round4.append(send(31 + number, ring_x.at[0:3], halo.at[2 - step], 0, step))
    column = const_times(
        high_ref[C_UR, 0:32, 0:64], low_ref[C_UR, 0:32, 0:64], ring_x[...].reshape(64, NZ)
    )
    ring_y[core] = times_const(column[0:16], high_ref[C_BD0], low_ref[C_BD0]) + times_const(
        column[16:32], high_ref[C_BD1], low_ref[C_BD1]
    )
    round5 = {}
    for step in FAR_FIRST:
        place = 2 * (HALF_GY - step) + core
        round5[step] = send(34 + step, ring_y.at[core], ring_y.at[place], 0, 2 * step)

    def hand_on(place):
        row = ring_y.at[2 * place + core]
        return send(50 + place, row, row, 0, 1 - 2 * core)

    handed = [hand_on(0)]

    for copy in round1:
        copy.wait_recv()

    def add_y(x, carried):
        q1[x + 3, 3:11, :] = q1[x + 3, 3:11, :] + from_y[0, x]
        q1[x + 3, 24:32, :] = q1[x + 3, 24:32, :] + from_y[1, x]
        return carried

    lax.fori_loop(0, EX, add_y, 0)
    for side, start in ((0, 0), (1, 35)):
        for x in range(6):
            row = start + x
            q1[row, 8:32, :] = q1[row, 8:32, :] + from_x[side, x]
            q1[row, 3:11, :] = q1[row, 3:11, :] + from_corner[2 * side, x]
            q1[row, 24:32, :] = q1[row, 24:32, :] + from_corner[2 * side + 1, x]

    def sum_y(x, carried):
        for dy in range(1, 4):
            sums1[dy - 1, x] = q1[x, 8 + dy : 32 + dy, :] + q1[x, 8 - dy : 32 - dy, :]
        return carried

    lax.fori_loop(0, 41, sum_y, 0)

    def stencil1(x, carried):
        total = jnp.zeros((EY, NZ), F32)
        for dy in range(4):
            for dx in range(4):
                if dy == 0:
                    value = q1[x + 3 + dx, 8:32, :]
                    if dx:
                        value = value + q1[x + 3 - dx, 8:32, :]
                else:
                    value = sums1[dy - 1, x + 3 + dx]
                    if dx:
                        value = value + sums1[dy - 1, x + 3 - dx]
                total = total + k1_ref[4 * dx + dy : 4 * dx + dy + 1, :] * value
        smooth1[x] = total
        return carried

    lax.fori_loop(0, EX, stencil1, 0)

    for step in reversed(FAR_FIRST):
        round5[step].wait_recv()
        handed.append(hand_on(HALF_GY - step))

    halo[2] = ring_x[0:3]
    for copy in round4:
        copy.wait_recv()
    for y in range(-5, 10):
        place = y % 4
        source = halo[y // 4 + 2].reshape(24, NZ)
        if place:
            source = pltpu.roll(source, NZ - 32 * place, axis=1)
        q3[y + 5, 0:24, :] = source

    def stencil3(y, carried):
        field3[y] = stencil_small(q3, y + 3, 6, 16, k3_ref)
        return carried

    lax.fori_loop(0, 9, stencil3, 0)

    for copy in handed:
        copy.wait_recv()

    def add_slot(slot, totals):
        values = ring_y[slot]
        return tuple(
            total + table[row % 4, slot + (3 - row // 4) - core] * values
            for row, total in enumerate(totals)
        )

    coarse = lax.fori_loop(
        0, N_GY, add_slot, tuple(jnp.zeros((16, NZ), F32) for _ in range(9)), unroll=4
    )
    coarse = jnp.concatenate(coarse, axis=0)
    half0 = times_const(coarse, high_ref[C_NZ0], low_ref[C_NZ0])
    half1 = times_const(coarse, high_ref[C_NZ1], low_ref[C_NZ1])
    for row in range(9):
        both = jnp.concatenate(
            [half0[16 * row : 16 * (row + 1)], half1[16 * row : 16 * (row + 1)]], axis=0
        )
        field3[row] = field3[row] + const_times(
            high_ref[C_PU, 0:16, 0:32], low_ref[C_PU, 0:16, 0:32], both
        )

    fields = [prolonged_rows(lambda m: field3[m + 2], y) for y in range(-1, 11)]
    up3[...] = times_const(jnp.concatenate(fields, axis=0), high_ref[C_M23T], low_ref[C_M23T])

    def column3(m):
        return up3[pl.ds(m + 2, 12, stride=16), :]

    for x in range(-1, 19):
        smooth2[x + 1, 0:12, :] = smooth2[x + 1, 0:12, :] + prolonged_rows(column3, x)

    part = times_const(
        smooth2[...].reshape(20 * 16, NZ), high_ref[C_M12T], low_ref[C_M12T]
    ).reshape(20, 16, NZ)
    smooth2[...] = part

    def widen_y(x, carried):
        rows = [smooth2[x, n : n + 12, :] for n in range(4)]
        up2[x, pl.ds(0, 12, stride=2), :] = rows[1]
        up2[x, pl.ds(1, 12, stride=2), :] = 0.5625 * (rows[1] + rows[2]) - 0.0625 * (
            rows[0] + rows[3]
        )
        return carried

    lax.fori_loop(0, 20, widen_y, 0)

    def widen_x(m, carried):
        values = [up2[m + n] for n in range(4)]
        sums[2 * m] = smooth1[2 * m] + values[1]
        sums[2 * m + 1] = smooth1[2 * m + 1] + (
            0.5625 * (values[1] + values[2]) - 0.0625 * (values[0] + values[3])
        )
        return carried

    lax.fori_loop(0, 17, widen_x, 0)
    sums[34] = smooth1[34] + up2[18]

    flat = sums[...].reshape(EX * EY, NZ)
    value = times_const(flat, inverse_high_ref[...], inverse_low_ref[...])
    window[...] = value.reshape(EX, EY, NZ)
    grid_ref[...] = window[:CX, :CY, :]

    def sample(plane, carried):
        sample_plane(plane, tables, window, atom_ref)
        return carried

    lax.fori_loop(0, CX, sample, 0, unroll=2)

    for copy in started:
        copy.wait_send()


def finish_kernel(grid_in, atom_in, grid_out, atom_out, grid, atom, sems):
    pairs = ((grid_in, grid, grid_out), (atom_in, atom, atom_out))
    loads = [
        pltpu.make_async_copy(source, middle, sems.at[number])
        for number, (source, middle, target) in enumerate(pairs)
    ]
    stores = [
        pltpu.make_async_copy(middle, target, sems.at[2 + number])
        for number, (source, middle, target) in enumerate(pairs)
    ]
    for load in loads:
        load.start()
    for load, store in zip(loads, stores):
        load.wait()
        store.start()
    for store in stores:
        store.wait()


def in_vmem(count):
    return [pl.BlockSpec(memory_space=pltpu.VMEM)] * count


def local(charges, fractions, cells):
    charge = charges.reshape(1, ATOMS_DEV)
    fraction = fractions.reshape(3, 1, ATOMS_DEV)
    cell = cells.reshape(2, ATOMS_DEV)
    forward = [jnp.asarray(part) for part in split_pair(real_basis(NZ).T)]
    inverse = [jnp.asarray(part) for part in split_pair(real_basis(NZ))]
    high, low = split_constants()
    inputs = [
        charge,
        fraction,
        cell,
        *forward,
        *inverse,
        jnp.asarray(stencil_table(1, 128)),
        jnp.asarray(stencil_table(2, 64)),
        jnp.asarray(stencil_table(3, 32)),
        jnp.asarray(high),
        jnp.asarray(low),
        jnp.asarray(coarse_table()),
    ]
    potential, sampled = pl.pallas_call(
        levels_entry,
        out_shape=(
            jax.ShapeDtypeStruct((CX, CY, NZ), F32),
            jax.ShapeDtypeStruct((1, ATOMS_DEV), F32),
        ),
        in_specs=[pl.BlockSpec(memory_space=pltpu.HBM)] * N_IN,
        out_specs=in_vmem(2),
        scratch_shapes=[pltpu.VMEM(value.shape, value.dtype) for value in inputs]
        + [
            pltpu.SemaphoreType.DMA((N_IN,)),
            pltpu.VMEM((CX, 4, PLANE), F32),
            pltpu.VMEM((CX, EY, PLANE), F32),
            pltpu.VMEM((CX, NZ, PLANE), BF16),
            pltpu.VMEM((CX, NZ, PLANE), BF16),
            pltpu.VMEM((EX, EY, NZ), F32),
            pltpu.VMEM((EX, EY, NZ), F32),
            pltpu.VMEM((EX, EY, NZ), F32),
            pltpu.VMEM((EX, 8, NZ), F32),
            pltpu.VMEM((2, 6, EY, NZ), F32),
            pltpu.VMEM((2, EX, 8, NZ), F32),
            pltpu.VMEM((4, 6, 8, NZ), F32),
            pltpu.VMEM((2, 4, 16, NZ), F32),
            pltpu.VMEM((2, 10, 8, NZ), F32),
            pltpu.VMEM((4, 4, 8, NZ), F32),
            pltpu.VMEM((10, 16, NZ), F32),
            pltpu.VMEM((10, 8, NZ), F32),
            pltpu.VMEM((41, 40, NZ), F32),
            pltpu.VMEM((3, 41, EY, NZ), F32),
            pltpu.VMEM((EX, EY, NZ), F32),
            pltpu.VMEM((EX, 16, NZ), F32),
            pltpu.VMEM((26, 32, NZ), F32),
            pltpu.VMEM((20, 16, NZ), F32),
            pltpu.VMEM((8 * 24, NZ), F32),
            pltpu.VMEM((N_GX, 8, NZ), F32),
            pltpu.VMEM((5, 3, 8, NZ), F32),
            pltpu.VMEM((N_GY, 16, NZ), F32),
            pltpu.VMEM((15, 32, NZ), F32),
            pltpu.VMEM((9, 16, NZ), F32),
            pltpu.VMEM((12 * 16, NZ), F32),
            pltpu.VMEM((20, EY, NZ), F32),
            pltpu.SemaphoreType.DMA((N_SEMS,)),
            pltpu.SemaphoreType.DMA((N_SEMS,)),
        ],
        compiler_params=pltpu.CompilerParams(collective_id=0, has_side_effects=True),
        name="levels",
    )(*inputs)
    potential, sampled = pl.pallas_call(
        finish_kernel,
        out_shape=(
            jax.ShapeDtypeStruct((CX, CY, NZ), F32),
            jax.ShapeDtypeStruct((1, ATOMS_DEV), F32),
        ),
        in_specs=[pl.BlockSpec(memory_space=pl.ANY)] * 2,
        out_specs=[pl.BlockSpec(memory_space=pl.ANY)] * 2,
        scratch_shapes=[
            pltpu.VMEM((CX, CY, NZ), F32),
            pltpu.VMEM((1, ATOMS_DEV), F32),
            pltpu.SemaphoreType.DMA((4,)),
        ],
        name="finish",
    )(potential, sampled)
    return potential, sampled.reshape(1, 1, ATOMS_DEV)


def solution(mesh):
    placed = (P("gx", "gy", None), P("gx", "gy", None, None), P("gx", "gy", None, None))
    return jax.shard_map(
        local,
        mesh=mesh,
        in_specs=placed,
        out_specs=(P("gx", "gy", None), P("gx", "gy", None)),
        check_vma=False,
    )
```

```python
import functools

import jax
import jax.numpy as jnp
import numpy as np
from jax import lax
from jax.experimental import pallas as pl
from jax.experimental.pallas import tpu as pltpu
from jax.sharding import PartitionSpec as P

CX = 32
CY = 16
NZ = 128
ATOMS_DEV = 16384
N_GX = 8
N_GY = 32
PLANE = ATOMS_DEV // CX
EX = CX + 3
EY = 24
MESH_IDS = pl.DeviceIdType.MESH
BF16 = jnp.bfloat16
F32 = jnp.float32
taps = ((-3, -0.0625), (-1, 0.5625), (0, 1.0), (1, 0.5625), (3, -0.0625))


def smooth_numpy(rho):
    return np.where(
        rho < 1.0, 1.875 - 1.25 * rho * rho + 0.375 * rho**4, 1.0 / np.maximum(rho, 1.0)
    )


def frequencies(count):
    inner = np.repeat(np.arange(1, count // 2), 2)
    return np.concatenate([[0], inner, [count // 2]])


def real_basis(count):
    wave = frequencies(count)
    angle = 2.0 * np.pi * wave[:, None] * np.arange(count)[None, :] / count
    is_sine = np.zeros(count, bool)
    is_sine[2:-1:2] = True
    basis = np.where(is_sine[:, None], np.sin(angle), np.cos(angle)) * np.sqrt(2.0 / count)
    basis[0] /= np.sqrt(2.0)
    basis[-1] /= np.sqrt(2.0)
    return basis


def restriction(count):
    matrix = np.zeros((count // 2, count))
    for row in range(count // 2):
        for offset, weight in taps:
            matrix[row, (2 * row + offset) % count] += weight
    return matrix


def stencil_table(level, extent):
    offsets = np.arange(-3, 4) * 1.0
    radius = np.sqrt(
        offsets[:, None, None] ** 2 + offsets[None, :, None] ** 2 + offsets[None, None, :] ** 2
    )
    stencil = (smooth_numpy(radius / 1.5) / 1.5 - smooth_numpy(radius / 3.0) / 3.0) / 2.0 ** (
        level - 1
    )
    waves = np.cos(2.0 * np.pi * offsets[:, None] * frequencies(extent)[None, :] / extent)
    table = np.zeros((16, 128))
    table[:, :extent] = (stencil[3:, 3:] @ waves).reshape(16, extent)
    return table.astype(np.float32)


def placed_at(block, row, column):
    matrix = np.zeros((128, 128))
    matrix[row : row + block.shape[0], column : column + block.shape[1]] = block
    return matrix


(
    C_M12,
    C_M23,
    C_BD0,
    C_BD1,
    C_NZ0,
    C_NZ1,
    C_M23T,
    C_M12T,
    C_UR,
    C_PU,
    C_M12B,
) = (0, 1, 5, 6, 7, 8, 9, 10, 11, 12, 13)


@functools.cache
def split_constants():
    def down(count):
        return (real_basis(count // 2) @ restriction(count) @ real_basis(count).T).T

    m12, m23, m34 = down(128), down(64), down(32)
    stack = [placed_at(m12, 0, 0)]
    stack += [placed_at(m23, 0, 32 * place) for place in range(4)]
    for half in range(2):
        matrix = np.zeros((128, 128))
        for place in range(4):
            matrix += placed_at(m34, 32 * place, 64 * half + 16 * place)
        stack.append(matrix)
    for half in range(2):
        matrix = np.zeros((128, 128))
        for place in range(4):
            matrix += placed_at(m34.T, 64 * half + 16 * place, 0)
        stack.append(matrix)
    stack += [placed_at(m23.T, 0, 0), placed_at(m12.T, 0, 0)]
    along_x = restriction(64)
    columns = (np.arange(64) - 8) % 64
    stack.append(placed_at((real_basis(32) @ along_x)[:, columns], 0, 0))
    rows = (np.arange(16) - 2) % 64
    stack.append(placed_at((real_basis(32) @ along_x).T[rows], 0, 0))
    stack.append(placed_at(m12, 0, 64))
    return split_pair(np.stack(stack))


def split_pair(matrix):
    high = matrix.astype(np.float32).astype(BF16)
    low = (matrix - high.astype(np.float64)).astype(np.float32).astype(BF16)
    return high, low


@functools.cache
def coarse_table():
    counts = (32, 64, 16)
    signed = [np.where(np.arange(c) > c // 2, np.arange(c) - c, np.arange(c)) for c in counts]
    radius = np.sqrt(
        signed[0][:, None, None] ** 2.0
        + signed[1][None, :, None] ** 2.0
        + signed[2][None, None, :] ** 2.0
    )
    kernel = smooth_numpy(radius / 1.5) / 12.0
    wave_x = np.cos(2.0 * np.pi * np.outer(frequencies(32), np.arange(32)) / 32)
    wave_z = np.cos(2.0 * np.pi * np.outer(frequencies(16), np.arange(16)) / 16)
    along_y = np.einsum("ax,xyz,bz->aby", wave_x, kernel, wave_z)
    down_y = restriction(128)
    differ = (np.arange(64)[:, None] - np.arange(64)[None, :]) % 64
    up_rows = down_y.T[(np.arange(4) - 2) % 128]
    folded = np.einsum("cm,abmn->abcn", up_rows, along_y[:, :, differ])
    folded = np.einsum("abcn,ny->abcy", folded, down_y)
    folded = folded.reshape(2, 16, 16, 4, 32, 4).transpose(3, 4, 1, 0, 5, 2)
    folded = folded.reshape(4, 32, 16, 128)
    extended = folded[:, (np.arange(35) - 3) % 32]
    return extended.astype(np.float32)


def split(value):
    high = value.astype(BF16)
    low = (value - high.astype(F32)).astype(BF16)
    return high, low


def mm(a, b):
    return jnp.dot(a, b, preferred_element_type=F32)


def times_const(value, high_w, low_w):
    high, low = split(value)
    return mm(high, high_w) + (mm(low, high_w) + mm(high, low_w))


def const_times(high_w, low_w, value):
    high, low = split(value)
    return mm(high_w, high) + (mm(high_w, low) + mm(low_w, high))


def spline_weights(frac):
    def near_weight(distance):
        return (1.0 - distance) * (1.0 + distance - 1.5 * distance * distance)

    def far_weight(distance):
        return -0.5 * (distance - 1.0) * (2.0 - distance) * (2.0 - distance)

    return (
        far_weight(1.0 + frac),
        near_weight(frac),
        near_weight(1.0 - frac),
        far_weight(2.0 - frac),
    )


BY_ROW = lax.GatherDimensionNumbers(
    offset_dims=(),
    collapsed_slice_dims=(0,),
    start_index_map=(0,),
    operand_batching_dims=(1,),
    start_indices_batching_dims=(1,),
)


def picked(table, index):
    return jnp.concatenate(
        [
            lax.gather(
                table[:, lane : lane + 128],
                index[:, lane : lane + 128, None],
                BY_ROW,
                slice_sizes=(1, 1),
                mode=lax.GatherScatterMode.PROMISE_IN_BOUNDS,
            )
            for lane in range(0, table.shape[1], 128)
        ],
        axis=1,
    )


def eight_rows(rows):
    return jnp.concatenate(rows + [jnp.zeros((4, rows[0].shape[1]), F32)], axis=0)


def index_rows(base, first, period):
    places = lax.broadcasted_iota(jnp.int32, (8, base.shape[1]), 0) + first
    return jnp.minimum((places - base) & (period - 1), 7)


def depth_tables(base, weights):
    rounded = [w.astype(BF16).astype(F32) for w in weights]
    high_rows = eight_rows(rounded)
    low_rows = eight_rows([w - r for w, r in zip(weights, rounded)])
    highs, lows = [], []
    for first in range(0, NZ, 16):
        indices = [index_rows(base, first + part, NZ) for part in (0, 8)]
        for rows, result in ((high_rows, highs), (low_rows, lows)):
            pair = jnp.concatenate([picked(rows, index) for index in indices], axis=0)
            result.append(pair.astype(BF16))
    return jnp.concatenate(highs, axis=0), jnp.concatenate(lows, axis=0)


def plane_tables(plane, fraction_ref, cell_ref, index_y):
    lanes = pl.ds(pl.multiple_of(plane * PLANE, PLANE), PLANE)
    fraction = jnp.concatenate([fraction_ref[k, :, lanes] for k in range(3)], axis=0)
    weights = spline_weights(fraction)
    cells = cell_ref[:, lanes]
    base_y = (cells[0:1] - (index_y * CY + 1)) & (CY * N_GY - 1)
    rows_y = eight_rows([w[1:2] for w in weights])
    table_y = jnp.concatenate(
        [picked(rows_y, index_rows(base_y, first, 32)) for first in range(0, EY, 8)], axis=0
    )
    tables_z = depth_tables(cells[1:2] - 1, [w[2:3] for w in weights])
    return lanes, [w[0:1] for w in weights], table_y, tables_z


def deposit_plane(
    plane, charge_ref, fraction_ref, cell_ref, sums, index_y, tables
):
    lanes, along_x, table_y, (z_high, z_low) = plane_tables(
        plane, fraction_ref, cell_ref, index_y
    )
    keep_x, keep_y, keep_high, keep_low = tables
    keep_x[plane] = jnp.concatenate(along_x, axis=0)
    keep_y[plane] = table_y
    keep_high[plane] = z_high
    keep_low[plane] = z_low
    charge = charge_ref[:, lanes]
    spread = jnp.concatenate([table_y * (w * charge) for w in along_x], axis=0)
    spread_high, spread_low = split(spread)
    dims = (((1,), (1,)), ((), ()))
    both = jnp.concatenate([spread_high, spread_low], axis=0)
    first = lax.dot_general(both, z_high, dims, preferred_element_type=F32)
    second = lax.dot_general(spread_high, z_low, dims, preferred_element_type=F32)
    contrib = first[: 4 * EY] + first[4 * EY :] + second
    for tap in range(4):
        sums[plane + tap] = sums[plane + tap] + contrib[EY * tap : EY * (tap + 1)]


def sample_plane(plane, tables, window_ref, atom_ref):
    keep_x, keep_y, keep_high, keep_low = tables
    lanes = pl.ds(pl.multiple_of(plane * PLANE, PLANE), PLANE)
    high, low = split(window_ref[pl.ds(plane, 4)].reshape(4 * EY, NZ))
    z_high, z_low = keep_high[plane], keep_low[plane]
    projected = mm(
        jnp.concatenate([high, low], axis=1), jnp.concatenate([z_high, z_high], axis=0)
    ) + mm(high, z_low)
    total = jnp.zeros((EY, PLANE), F32)
    for tap in range(4):
        total = total + keep_x[plane, tap : tap + 1, :] * projected[EY * tap : EY * (tap + 1)]
    atom_ref[:, lanes] = jnp.sum(total * keep_y[plane], axis=0, keepdims=True)


NEIGHBOURS = ((1, 0), (-1, 0), (0, 1), (0, -1), (1, 1), (1, -1), (-1, 1), (-1, -1))
N_SEMS = 16 + 8 + 7 + 4 + 15 + 16
HALF_GY = N_GY // 2
FAR_FIRST = sorted(range(1, HALF_GY), key=lambda k: -min(k, HALF_GY - k))


def prolonged_rows(get, row):
    middle = row // 2
    if row % 2 == 0:
        return get(middle)
    return 0.5625 * (get(middle) + get(middle + 1)) - 0.0625 * (get(middle - 1) + get(middle + 2))


N_IN = 13
N_FIRST = 5


def levels_entry(*refs):
    sources, outputs = refs[:N_IN], refs[N_IN : N_IN + 2]
    inputs, sems, rest = refs[N_IN + 2 : 2 * N_IN + 2], refs[2 * N_IN + 2], refs[2 * N_IN + 3 :]
    copies = [
        pltpu.make_async_copy(source, target, sems.at[number])
        for number, (source, target) in enumerate(zip(sources, inputs))
    ]
    for copy in copies:
        copy.start()
    levels_kernel(*inputs, *outputs, *rest, copies[:N_FIRST], copies[N_FIRST:])


def levels_kernel(
    charge_ref,
    fraction_ref,
    cell_ref,
    forward_high_ref,
    forward_low_ref,
    inverse_high_ref,
    inverse_low_ref,
    k1_ref,
    k2_ref,
    k3_ref,
    high_ref,
    low_ref,
    table,
    grid_ref,
    atom_ref,
    keep_x,
    keep_y,
    keep_high,
    keep_low,
    window,
    sums,
    own,
    edge,
    from_x,
    from_y,
    from_corner,
    from_x2,
    from_y2,
    from_corner2,
    own2,
    edge2,
    q1,
    sums1,
    smooth1,
    part1,
    q2,
    smooth2,
    part2,
    ring_x,
    halo,
    ring_y,
    q3,
    field3,
    up3,
    up2,
    send_sems,
    recv_sems,
    first_copies,
    later_copies,
):
    index_x = lax.axis_index("gx")
    index_y = lax.axis_index("gy")
    core = lax.rem(index_y, 2)
    tables = (keep_x, keep_y, keep_high, keep_low)

    def device(step_x, step_y):
        return (
            lax.rem(index_x + (step_x + N_GX), N_GX),
            lax.rem(index_y + (step_y + N_GY), N_GY),
        )

    barrier = pltpu.get_barrier_semaphore()
    peers = [(x, 0) for x in range(1, N_GX)]
    peers += [(0, y) for y in range(2, N_GY, 2)] + [(0, 1), (0, N_GY - 1)]
    peers += [(x, y) for x, y in NEIGHBOURS if x and y]
    for step_x, step_y in peers:
        pl.semaphore_signal(
            barrier, inc=1, device_id=device(step_x, step_y), device_id_type=MESH_IDS
        )

    started = []

    def send(number, source, target, step_x, step_y):
        copy = pltpu.make_async_remote_copy(
            src_ref=source,
            dst_ref=target,
            send_sem=send_sems.at[number],
            recv_sem=recv_sems.at[number],
            device_id=device(step_x, step_y),
            device_id_type=MESH_IDS,
        )
        copy.start()
        started.append(copy)
        return copy

    sums[...] = jnp.zeros_like(sums)

    def clear(x, carried):
        q1[x] = jnp.zeros((40, NZ), F32)
        return carried

    lax.fori_loop(0, 41, clear, 0)

    for copy in first_copies:
        copy.wait()

    def deposit(first, last, row, count, send_finished):
        def step(plane, carried):
            deposit_plane(
                plane, charge_ref, fraction_ref, cell_ref, sums, index_y, tables
            )
            return carried

        lax.fori_loop(first, last, step, 0, unroll=2)
        flat = sums[row : row + count].reshape(count * EY, NZ)
        value = times_const(flat, forward_high_ref[...], forward_low_ref[...])
        own[row : row + count] = value.reshape(count, EY, NZ)
        edge[row : row + count] = own[row : row + count, 11:19, :]

        def restrict_y(x, carried):
            q1[x + 3, 8:32, :] = own[x]
            total = jnp.zeros((16, NZ), F32)
            for offset, weight in taps:
                total = total + weight * q1[x + 3, pl.ds(6 + offset, 16, stride=2), :]
            part1[x] = total
            return carried

        send_finished()
        lax.fori_loop(row, row + count, restrict_y, 0)

    round1 = []

    def send_edges(number, row, count):
        rows = pl.ds(row, count)
        round1.append(send(number, edge.at[rows], from_y.at[0, rows], 0, 1))
        round1.append(send(number + 1, own.at[rows, 0:8, :], from_y.at[1, rows], 0, -1))

    high_x, low_x = pl.ds(29, 6), pl.ds(0, 6)

    def send_high():
        pl.semaphore_wait(barrier, len(peers))
        round1.append(send(0, edge.at[high_x], from_corner.at[0], 1, 1))
        round1.append(send(1, own.at[high_x, 0:8, :], from_corner.at[1], 1, -1))
        round1.append(send(2, own.at[high_x], from_x.at[0], 1, 0))
        send_edges(6, 29, 6)

    def send_low():
        round1.append(send(3, edge.at[low_x], from_corner.at[2], -1, 1))
        round1.append(send(4, own.at[low_x, 0:8, :], from_corner.at[3], -1, -1))
        round1.append(send(5, own.at[low_x], from_x.at[1], -1, 0))
        send_edges(8, 0, 6)

    deposit(26, 32, 29, 6, send_high)
    deposit(0, 6, 0, 6, send_low)
    deposit(6, 14, 6, 8, lambda: send_edges(10, 6, 8))
    deposit(14, 22, 14, 8, lambda: send_edges(12, 14, 8))
    deposit(22, 26, 22, 7, lambda: None)

    for copy in later_copies:
        copy.wait()

    rows = []
    for m in range(-1, 19):
        total = jnp.zeros((16, NZ), F32)
        for offset, weight in taps:
            if 0 <= 2 * m + offset < EX:
                total = total + weight * part1[2 * m + offset]
        rows.append(total)
    level2 = times_const(
        jnp.concatenate(rows[0::2], axis=0), high_ref[C_M12], low_ref[C_M12]
    ) + times_const(jnp.concatenate(rows[1::2], axis=0), high_ref[C_M12B], low_ref[C_M12B])
    own2[...] = level2.reshape(10, 16, NZ)
    edge2[...] = own2[:, 5:13, :]

    round2 = []
    for number in (4, 5, 6, 7, 0, 1, 2, 3):
        step_x, step_y = NEIGHBOURS[number]
        rows = {0: pl.ds(0, 10), 1: pl.ds(6, 4), -1: pl.ds(0, 4)}[step_x]
        if step_y == 0:
            source, target = own2.at[rows], from_x2.at[number]
        elif step_x == 0:
            source = edge2 if step_y == 1 else own2.at[:, 0:8, :]
            target = from_y2.at[number - 2]
        else:
            source = edge2.at[rows] if step_y == 1 else own2.at[rows, 0:8, :]
            target = from_corner2.at[number - 4]
        round2.append(send(16 + number, source, target, step_x, step_y))
    send_edges(14, 22, 7)

    q2[...] = jnp.zeros_like(q2)
    q3[:, 24:32, :] = jnp.zeros((15, 8, NZ), F32)
    for pair in range(10):
        q2[3 + 2 * pair, 7:23, :] = own2[pair]
        q2[4 + 2 * pair, 7:23, :] = pltpu.roll(own2[pair], 64, axis=1)

    for copy in round2:
        copy.wait_recv()

    def add_to2(row, start, value):
        end = start + value.shape[0]
        for place, plane in ((row, value), (row + 1, pltpu.roll(value, 64, axis=1))):
            if 0 <= place < 26:
                q2[place, start:end, :] = q2[place, start:end, :] + plane

    for pair in range(10):
        add_to2(3 + 2 * pair, 4, from_y2[0, pair])
        add_to2(3 + 2 * pair, 15, from_y2[1, pair])
    for side, first in ((0, -1), (1, 19)):
        for pair in range(4):
            add_to2(first + 2 * pair, 7, from_x2[side, pair])
            add_to2(first + 2 * pair, 4, from_corner2[2 * side, pair])
            add_to2(first + 2 * pair, 15, from_corner2[2 * side + 1, pair])

    for m in range(8):
        total = jnp.zeros((24, NZ), F32)
        for offset, weight in taps:
            total = total + weight * q2[2 * m + 4 + offset, 0:24, :]
        part2[24 * m : 24 * (m + 1), :] = total
    tile = jnp.zeros((8, NZ), F32)
    for n in range(4):
        total = jnp.zeros((8, NZ), F32)
        for offset, weight in taps:
            total = total + weight * part2[pl.ds(8 + 2 * n + offset, 8, stride=24), :]
        tile = tile + times_const(total, high_ref[C_M23 + n], low_ref[C_M23 + n])
    ring_x[1] = tile

    round3 = []
    for step in (4, 5, 3, 6, 2, 7, 1):
        place = (N_GX - step + 1) % N_GX
        round3.append(send(23 + step, ring_x.at[1], ring_x.at[place], step, 0))

    def stencil_small(source, row, start, count, k_ref):
        total = jnp.zeros((count, NZ), F32)
        for across in range(4):
            for along in range(4):
                value = None
                for sign_r in sorted({across, -across}):
                    for sign_s in sorted({along, -along}):
                        piece = source[row + sign_r, start + sign_s : start + sign_s + count, :]
                        value = piece if value is None else value + piece
                total = total + k_ref[4 * across + along : 4 * across + along + 1, :] * value
        return total

    def stencil2(x, carried):
        smooth2[x] = stencil_small(q2, x + 3, 7, 16, k2_ref)
        return carried

    lax.fori_loop(0, 20, stencil2, 0)

    for copy in round3:
        copy.wait_recv()

    column = const_times(
        high_ref[C_UR, 0:32, 0:64], low_ref[C_UR, 0:32, 0:64], ring_x[...].reshape(64, NZ)
    )
    ring_y[core] = times_const(column[0:16], high_ref[C_BD0], low_ref[C_BD0]) + times_const(
        column[16:32], high_ref[C_BD1], low_ref[C_BD1]
    )
    round5 = {}
    for step in FAR_FIRST:
        place = 2 * (HALF_GY - step) + core
        round5[step] = send(34 + step, ring_y.at[core], ring_y.at[place], 0, 2 * step)

    def hand_on(place):
        row = ring_y.at[2 * place + core]
        return send(50 + place, row, row, 0, 1 - 2 * core)

    handed = [hand_on(0)]
    round4 = []
    for number, step in enumerate((1, -1, 2, -2)):
        round4.append(send(31 + number, ring_x.at[0:3], halo.at[2 - step], 0, step))

    for copy in round1:
        copy.wait_recv()

    def add_y(x, carried):
        q1[x + 3, 3:11, :] = q1[x + 3, 3:11, :] + from_y[0, x]
        q1[x + 3, 24:32, :] = q1[x + 3, 24:32, :] + from_y[1, x]
        return carried

    lax.fori_loop(0, EX, add_y, 0)
    for side, start in ((0, 0), (1, 35)):
        for x in range(6):
            row = start + x
            q1[row, 8:32, :] = q1[row, 8:32, :] + from_x[side, x]
            q1[row, 3:11, :] = q1[row, 3:11, :] + from_corner[2 * side, x]
            q1[row, 24:32, :] = q1[row, 24:32, :] + from_corner[2 * side + 1, x]

    def sum_y(x, carried):
        for dy in range(1, 4):
            sums1[dy - 1, x] = q1[x, 8 + dy : 32 + dy, :] + q1[x, 8 - dy : 32 - dy, :]
        return carried

    lax.fori_loop(0, 41, sum_y, 0)

    def stencil1(x, carried):
        total = jnp.zeros((EY, NZ), F32)
        for dy in range(4):
            for dx in range(4):
                if dy == 0:
                    value = q1[x + 3 + dx, 8:32, :]
                    if dx:
                        value = value + q1[x + 3 - dx, 8:32, :]
                else:
                    value = sums1[dy - 1, x + 3 + dx]
                    if dx:
                        value = value + sums1[dy - 1, x + 3 - dx]
                total = total + k1_ref[4 * dx + dy : 4 * dx + dy + 1, :] * value
        smooth1[x] = total
        return carried

    lax.fori_loop(0, EX, stencil1, 0)

    for step in reversed(FAR_FIRST):
        round5[step].wait_recv()
        handed.append(hand_on(HALF_GY - step))

    halo[2] = ring_x[0:3]
    for copy in round4:
        copy.wait_recv()
    for y in range(-5, 10):
        place = y % 4
        source = halo[y // 4 + 2].reshape(24, NZ)
        if place:
            source = pltpu.roll(source, NZ - 32 * place, axis=1)
        q3[y + 5, 0:24, :] = source

    def stencil3(y, carried):
        field3[y] = stencil_small(q3, y + 3, 6, 16, k3_ref)
        return carried

    lax.fori_loop(0, 9, stencil3, 0)

    for copy in handed:
        copy.wait_recv()

    def add_slot(slot, totals):
        values = ring_y[slot]
        return tuple(
            total + table[row % 4, slot + (3 - row // 4) - core] * values
            for row, total in enumerate(totals)
        )

    coarse = lax.fori_loop(
        0, N_GY, add_slot, tuple(jnp.zeros((16, NZ), F32) for _ in range(9)), unroll=4
    )
    coarse = jnp.concatenate(coarse, axis=0)
    half0 = times_const(coarse, high_ref[C_NZ0], low_ref[C_NZ0])
    half1 = times_const(coarse, high_ref[C_NZ1], low_ref[C_NZ1])
    for row in range(9):
        both = jnp.concatenate(
            [half0[16 * row : 16 * (row + 1)], half1[16 * row : 16 * (row + 1)]], axis=0
        )
        field3[row] = field3[row] + const_times(
            high_ref[C_PU, 0:16, 0:32], low_ref[C_PU, 0:16, 0:32], both
        )

    fields = [prolonged_rows(lambda m: field3[m + 2], y) for y in range(-1, 11)]
    up3[...] = times_const(jnp.concatenate(fields, axis=0), high_ref[C_M23T], low_ref[C_M23T])

    def column3(m):
        return up3[pl.ds(m + 2, 12, stride=16), :]

    for x in range(-1, 19):
        smooth2[x + 1, 0:12, :] = smooth2[x + 1, 0:12, :] + prolonged_rows(column3, x)

    part = times_const(
        smooth2[...].reshape(20 * 16, NZ), high_ref[C_M12T], low_ref[C_M12T]
    ).reshape(20, 16, NZ)
    smooth2[...] = part

    def widen_y(x, carried):
        rows = [smooth2[x, n : n + 12, :] for n in range(4)]
        up2[x, pl.ds(0, 12, stride=2), :] = rows[1]
        up2[x, pl.ds(1, 12, stride=2), :] = 0.5625 * (rows[1] + rows[2]) - 0.0625 * (
            rows[0] + rows[3]
        )
        return carried

    lax.fori_loop(0, 20, widen_y, 0)

    def widen_x(m, carried):
        values = [up2[m + n] for n in range(4)]
        sums[2 * m] = smooth1[2 * m] + values[1]
        sums[2 * m + 1] = smooth1[2 * m + 1] + (
            0.5625 * (values[1] + values[2]) - 0.0625 * (values[0] + values[3])
        )
        return carried

    lax.fori_loop(0, 17, widen_x, 0)
    sums[34] = smooth1[34] + up2[18]

    flat = sums[...].reshape(EX * EY, NZ)
    value = times_const(flat, inverse_high_ref[...], inverse_low_ref[...])
    window[...] = value.reshape(EX, EY, NZ)
    grid_ref[...] = window[:CX, :CY, :]

    def sample(plane, carried):
        sample_plane(plane, tables, window, atom_ref)
        return carried

    lax.fori_loop(0, CX, sample, 0, unroll=2)

    for copy in started:
        copy.wait_send()


def finish_kernel(grid_in, atom_in, grid_out, atom_out, grid, atom, sems):
    pairs = ((grid_in, grid, grid_out), (atom_in, atom, atom_out))
    loads = [
        pltpu.make_async_copy(source, middle, sems.at[number])
        for number, (source, middle, target) in enumerate(pairs)
    ]
    stores = [
        pltpu.make_async_copy(middle, target, sems.at[2 + number])
        for number, (source, middle, target) in enumerate(pairs)
    ]
    for load in loads:
        load.start()
    for load, store in zip(loads, stores):
        load.wait()
        store.start()
    for store in stores:
        store.wait()


def in_vmem(count):
    return [pl.BlockSpec(memory_space=pltpu.VMEM)] * count


def local(charges, fractions, cells):
    charge = charges.reshape(1, ATOMS_DEV)
    fraction = fractions.reshape(3, 1, ATOMS_DEV)
    cell = cells.reshape(2, ATOMS_DEV)
    forward = [jnp.asarray(part) for part in split_pair(real_basis(NZ).T)]
    inverse = [jnp.asarray(part) for part in split_pair(real_basis(NZ))]
    high, low = split_constants()
    inputs = [
        charge,
        fraction,
        cell,
        *forward,
        *inverse,
        jnp.asarray(stencil_table(1, 128)),
        jnp.asarray(stencil_table(2, 64)),
        jnp.asarray(stencil_table(3, 32)),
        jnp.asarray(high),
        jnp.asarray(low),
        jnp.asarray(coarse_table()),
    ]
    potential, sampled = pl.pallas_call(
        levels_entry,
        out_shape=(
            jax.ShapeDtypeStruct((CX, CY, NZ), F32),
            jax.ShapeDtypeStruct((1, ATOMS_DEV), F32),
        ),
        in_specs=[pl.BlockSpec(memory_space=pltpu.HBM)] * N_IN,
        out_specs=in_vmem(2),
        scratch_shapes=[pltpu.VMEM(value.shape, value.dtype) for value in inputs]
        + [
            pltpu.SemaphoreType.DMA((N_IN,)),
            pltpu.VMEM((CX, 4, PLANE), F32),
            pltpu.VMEM((CX, EY, PLANE), F32),
            pltpu.VMEM((CX, NZ, PLANE), BF16),
            pltpu.VMEM((CX, NZ, PLANE), BF16),
            pltpu.VMEM((EX, EY, NZ), F32),
            pltpu.VMEM((EX, EY, NZ), F32),
            pltpu.VMEM((EX, EY, NZ), F32),
            pltpu.VMEM((EX, 8, NZ), F32),
            pltpu.VMEM((2, 6, EY, NZ), F32),
            pltpu.VMEM((2, EX, 8, NZ), F32),
            pltpu.VMEM((4, 6, 8, NZ), F32),
            pltpu.VMEM((2, 4, 16, NZ), F32),
            pltpu.VMEM((2, 10, 8, NZ), F32),
            pltpu.VMEM((4, 4, 8, NZ), F32),
            pltpu.VMEM((10, 16, NZ), F32),
            pltpu.VMEM((10, 8, NZ), F32),
            pltpu.VMEM((41, 40, NZ), F32),
            pltpu.VMEM((3, 41, EY, NZ), F32),
            pltpu.VMEM((EX, EY, NZ), F32),
            pltpu.VMEM((EX, 16, NZ), F32),
            pltpu.VMEM((26, 32, NZ), F32),
            pltpu.VMEM((20, 16, NZ), F32),
            pltpu.VMEM((8 * 24, NZ), F32),
            pltpu.VMEM((N_GX, 8, NZ), F32),
            pltpu.VMEM((5, 3, 8, NZ), F32),
            pltpu.VMEM((N_GY, 16, NZ), F32),
            pltpu.VMEM((15, 32, NZ), F32),
            pltpu.VMEM((9, 16, NZ), F32),
            pltpu.VMEM((12 * 16, NZ), F32),
            pltpu.VMEM((20, EY, NZ), F32),
            pltpu.SemaphoreType.DMA((N_SEMS,)),
            pltpu.SemaphoreType.DMA((N_SEMS,)),
        ],
        compiler_params=pltpu.CompilerParams(collective_id=0, has_side_effects=True),
        name="levels",
    )(*inputs)
    potential, sampled = pl.pallas_call(
        finish_kernel,
        out_shape=(
            jax.ShapeDtypeStruct((CX, CY, NZ), F32),
            jax.ShapeDtypeStruct((1, ATOMS_DEV), F32),
        ),
        in_specs=[pl.BlockSpec(memory_space=pl.ANY)] * 2,
        out_specs=[pl.BlockSpec(memory_space=pl.ANY)] * 2,
        scratch_shapes=[
            pltpu.VMEM((CX, CY, NZ), F32),
            pltpu.VMEM((1, ATOMS_DEV), F32),
            pltpu.SemaphoreType.DMA((4,)),
        ],
        name="finish",
    )(potential, sampled)
    return potential, sampled.reshape(1, 1, ATOMS_DEV)


def solution(mesh):
    placed = (P("gx", "gy", None), P("gx", "gy", None, None), P("gx", "gy", None, None))
    return jax.shard_map(
        local,
        mesh=mesh,
        in_specs=placed,
        out_specs=(P("gx", "gy", None), P("gx", "gy", None)),
        check_vma=False,
    )
```

```python
import functools

import jax
import jax.numpy as jnp
import numpy as np
from jax import lax
from jax.experimental import pallas as pl
from jax.experimental.pallas import tpu as pltpu
from jax.sharding import PartitionSpec as P

CX = 32
CY = 16
NZ = 128
ATOMS_DEV = 16384
N_GX = 8
N_GY = 32
PLANE = ATOMS_DEV // CX
EX = CX + 3
EY = 24
MESH_IDS = pl.DeviceIdType.MESH
BF16 = jnp.bfloat16
F32 = jnp.float32
taps = ((-3, -0.0625), (-1, 0.5625), (0, 1.0), (1, 0.5625), (3, -0.0625))


def smooth_numpy(rho):
    return np.where(
        rho < 1.0, 1.875 - 1.25 * rho * rho + 0.375 * rho**4, 1.0 / np.maximum(rho, 1.0)
    )


def frequencies(count):
    inner = np.repeat(np.arange(1, count // 2), 2)
    return np.concatenate([[0], inner, [count // 2]])


def real_basis(count):
    wave = frequencies(count)
    angle = 2.0 * np.pi * wave[:, None] * np.arange(count)[None, :] / count
    is_sine = np.zeros(count, bool)
    is_sine[2:-1:2] = True
    basis = np.where(is_sine[:, None], np.sin(angle), np.cos(angle)) * np.sqrt(2.0 / count)
    basis[0] /= np.sqrt(2.0)
    basis[-1] /= np.sqrt(2.0)
    return basis


def restriction(count):
    matrix = np.zeros((count // 2, count))
    for row in range(count // 2):
        for offset, weight in taps:
            matrix[row, (2 * row + offset) % count] += weight
    return matrix


def stencil_table(level, extent):
    offsets = np.arange(-3, 4) * 1.0
    radius = np.sqrt(
        offsets[:, None, None] ** 2 + offsets[None, :, None] ** 2 + offsets[None, None, :] ** 2
    )
    stencil = (smooth_numpy(radius / 1.5) / 1.5 - smooth_numpy(radius / 3.0) / 3.0) / 2.0 ** (
        level - 1
    )
    waves = np.cos(2.0 * np.pi * offsets[:, None] * frequencies(extent)[None, :] / extent)
    table = np.zeros((16, 128))
    table[:, :extent] = (stencil[3:, 3:] @ waves).reshape(16, extent)
    return table.astype(np.float32)


def placed_at(block, row, column):
    matrix = np.zeros((128, 128))
    matrix[row : row + block.shape[0], column : column + block.shape[1]] = block
    return matrix


(
    C_M12,
    C_M23,
    C_BD0,
    C_BD1,
    C_NZ0,
    C_NZ1,
    C_M23T,
    C_M12T,
    C_UR,
    C_PU,
    C_M12B,
) = (0, 1, 5, 6, 7, 8, 9, 10, 11, 12, 13)


@functools.cache
def split_constants():
    def down(count):
        return (real_basis(count // 2) @ restriction(count) @ real_basis(count).T).T

    m12, m23, m34 = down(128), down(64), down(32)
    stack = [placed_at(m12, 0, 0)]
    stack += [placed_at(m23, 0, 32 * place) for place in range(4)]
    for half in range(2):
        matrix = np.zeros((128, 128))
        for place in range(4):
            matrix += placed_at(m34, 32 * place, 64 * half + 16 * place)
        stack.append(matrix)
    for half in range(2):
        matrix = np.zeros((128, 128))
        for place in range(4):
            matrix += placed_at(m34.T, 64 * half + 16 * place, 0)
        stack.append(matrix)
    stack += [placed_at(m23.T, 0, 0), placed_at(m12.T, 0, 0)]
    along_x = restriction(64)
    columns = (np.arange(64) - 8) % 64
    stack.append(placed_at((real_basis(32) @ along_x)[:, columns], 0, 0))
    rows = (np.arange(16) - 2) % 64
    stack.append(placed_at((real_basis(32) @ along_x).T[rows], 0, 0))
    stack.append(placed_at(m12, 0, 64))
    return split_pair(np.stack(stack))


def split_pair(matrix):
    high = matrix.astype(np.float32).astype(BF16)
    low = (matrix - high.astype(np.float64)).astype(np.float32).astype(BF16)
    return high, low


@functools.cache
def coarse_table():
    counts = (32, 64, 16)
    signed = [np.where(np.arange(c) > c // 2, np.arange(c) - c, np.arange(c)) for c in counts]
    radius = np.sqrt(
        signed[0][:, None, None] ** 2.0
        + signed[1][None, :, None] ** 2.0
        + signed[2][None, None, :] ** 2.0
    )
    kernel = smooth_numpy(radius / 1.5) / 12.0
    wave_x = np.cos(2.0 * np.pi * np.outer(frequencies(32), np.arange(32)) / 32)
    wave_z = np.cos(2.0 * np.pi * np.outer(frequencies(16), np.arange(16)) / 16)
    along_y = np.einsum("ax,xyz,bz->aby", wave_x, kernel, wave_z)
    down_y = restriction(128)
    differ = (np.arange(64)[:, None] - np.arange(64)[None, :]) % 64
    up_rows = down_y.T[(np.arange(4) - 2) % 128]
    folded = np.einsum("cm,abmn->abcn", up_rows, along_y[:, :, differ])
    folded = np.einsum("abcn,ny->abcy", folded, down_y)
    folded = folded.reshape(2, 16, 16, 4, 32, 4).transpose(3, 4, 1, 0, 5, 2)
    folded = folded.reshape(4, 32, 16, 128)
    extended = folded[:, (np.arange(35) - 3) % 32]
    return extended.astype(np.float32)


def split(value):
    high = value.astype(BF16)
    low = (value - high.astype(F32)).astype(BF16)
    return high, low


def mm(a, b):
    return jnp.dot(a, b, preferred_element_type=F32)


def times_const(value, high_w, low_w):
    high, low = split(value)
    return mm(high, high_w) + (mm(low, high_w) + mm(high, low_w))


def const_times(high_w, low_w, value):
    high, low = split(value)
    return mm(high_w, high) + (mm(high_w, low) + mm(low_w, high))


def spline_weights(frac):
    def near_weight(distance):
        return (1.0 - distance) * (1.0 + distance - 1.5 * distance * distance)

    def far_weight(distance):
        return -0.5 * (distance - 1.0) * (2.0 - distance) * (2.0 - distance)

    return (
        far_weight(1.0 + frac),
        near_weight(frac),
        near_weight(1.0 - frac),
        far_weight(2.0 - frac),
    )


BY_ROW = lax.GatherDimensionNumbers(
    offset_dims=(),
    collapsed_slice_dims=(0,),
    start_index_map=(0,),
    operand_batching_dims=(1,),
    start_indices_batching_dims=(1,),
)


def picked(table, index):
    return jnp.concatenate(
        [
            lax.gather(
                table[:, lane : lane + 128],
                index[:, lane : lane + 128, None],
                BY_ROW,
                slice_sizes=(1, 1),
                mode=lax.GatherScatterMode.PROMISE_IN_BOUNDS,
            )
            for lane in range(0, table.shape[1], 128)
        ],
        axis=1,
    )


def eight_rows(rows):
    return jnp.concatenate(rows + [jnp.zeros((4, rows[0].shape[1]), F32)], axis=0)


def index_rows(base, first, period):
    places = lax.broadcasted_iota(jnp.int32, (8, base.shape[1]), 0) + first
    return jnp.minimum((places - base) & (period - 1), 7)


def depth_tables(base, weights):
    rounded = [w.astype(BF16).astype(F32) for w in weights]
    high_rows = eight_rows(rounded)
    low_rows = eight_rows([w - r for w, r in zip(weights, rounded)])
    highs, lows = [], []
    for first in range(0, NZ, 16):
        indices = [index_rows(base, first + part, NZ) for part in (0, 8)]
        for rows, result in ((high_rows, highs), (low_rows, lows)):
            pair = jnp.concatenate([picked(rows, index) for index in indices], axis=0)
            result.append(pair.astype(BF16))
    return jnp.concatenate(highs, axis=0), jnp.concatenate(lows, axis=0)


def plane_tables(plane, fraction_ref, cell_ref, index_y):
    lanes = pl.ds(pl.multiple_of(plane * PLANE, PLANE), PLANE)
    fraction = jnp.concatenate([fraction_ref[k, :, lanes] for k in range(3)], axis=0)
    weights = spline_weights(fraction)
    cells = cell_ref[:, lanes]
    base_y = (cells[0:1] - (index_y * CY + 1)) & (CY * N_GY - 1)
    rows_y = eight_rows([w[1:2] for w in weights])
    table_y = jnp.concatenate(
        [picked(rows_y, index_rows(base_y, first, 32)) for first in range(0, EY, 8)], axis=0
    )
    tables_z = depth_tables(cells[1:2] - 1, [w[2:3] for w in weights])
    return lanes, [w[0:1] for w in weights], table_y, tables_z


def deposit_plane(
    plane, charge_ref, fraction_ref, cell_ref, sums, index_y, tables
):
    lanes, along_x, table_y, (z_high, z_low) = plane_tables(
        plane, fraction_ref, cell_ref, index_y
    )
    keep_x, keep_y, keep_high, keep_low = tables
    keep_x[plane] = jnp.concatenate(along_x, axis=0)
    keep_y[plane] = table_y
    keep_high[plane] = z_high
    keep_low[plane] = z_low
    charge = charge_ref[:, lanes]
    spread = jnp.concatenate([table_y * (w * charge) for w in along_x], axis=0)
    spread_high, spread_low = split(spread)
    dims = (((1,), (1,)), ((), ()))
    both = jnp.concatenate([spread_high, spread_low], axis=0)
    first = lax.dot_general(both, z_high, dims, preferred_element_type=F32)
    second = lax.dot_general(spread_high, z_low, dims, preferred_element_type=F32)
    contrib = first[: 4 * EY] + first[4 * EY :] + second
    for tap in range(4):
        sums[plane + tap] = sums[plane + tap] + contrib[EY * tap : EY * (tap + 1)]


def sample_plane(plane, tables, window_ref, atom_ref):
    keep_x, keep_y, keep_high, keep_low = tables
    lanes = pl.ds(pl.multiple_of(plane * PLANE, PLANE), PLANE)
    high, low = split(window_ref[pl.ds(plane, 4)].reshape(4 * EY, NZ))
    z_high, z_low = keep_high[plane], keep_low[plane]
    projected = mm(
        jnp.concatenate([high, low], axis=1), jnp.concatenate([z_high, z_high], axis=0)
    ) + mm(high, z_low)
    total = jnp.zeros((EY, PLANE), F32)
    for tap in range(4):
        total = total + keep_x[plane, tap : tap + 1, :] * projected[EY * tap : EY * (tap + 1)]
    atom_ref[:, lanes] = jnp.sum(total * keep_y[plane], axis=0, keepdims=True)


NEIGHBOURS = ((1, 0), (-1, 0), (0, 1), (0, -1), (1, 1), (1, -1), (-1, 1), (-1, -1))
N_SEMS = 16 + 8 + 7 + 4 + 15 + 16
HALF_GY = N_GY // 2
FAR_FIRST = sorted(range(1, HALF_GY), key=lambda k: -min(k, HALF_GY - k))


def prolonged_rows(get, row):
    middle = row // 2
    if row % 2 == 0:
        return get(middle)
    return 0.5625 * (get(middle) + get(middle + 1)) - 0.0625 * (get(middle - 1) + get(middle + 2))


N_IN = 13
N_FIRST = 5


def levels_entry(*refs):
    sources, outputs = refs[:N_IN], refs[N_IN : N_IN + 2]
    inputs, sems, rest = refs[N_IN + 2 : 2 * N_IN + 2], refs[2 * N_IN + 2], refs[2 * N_IN + 3 :]
    copies = [
        pltpu.make_async_copy(source, target, sems.at[number])
        for number, (source, target) in enumerate(zip(sources, inputs))
    ]
    for copy in copies:
        copy.start()
    levels_kernel(*inputs, *outputs, *rest, copies[:N_FIRST], copies[N_FIRST:])


def levels_kernel(
    charge_ref,
    fraction_ref,
    cell_ref,
    forward_high_ref,
    forward_low_ref,
    inverse_high_ref,
    inverse_low_ref,
    k1_ref,
    k2_ref,
    k3_ref,
    high_ref,
    low_ref,
    table,
    grid_ref,
    atom_ref,
    keep_x,
    keep_y,
    keep_high,
    keep_low,
    window,
    sums,
    own,
    edge,
    from_x,
    from_y,
    from_corner,
    from_x2,
    from_y2,
    from_corner2,
    own2,
    edge2,
    q1,
    sums1,
    smooth1,
    part1,
    q2,
    smooth2,
    part2,
    ring_x,
    halo,
    ring_y,
    q3,
    field3,
    up3,
    up2,
    send_sems,
    recv_sems,
    first_copies,
    later_copies,
):
    index_x = lax.axis_index("gx")
    index_y = lax.axis_index("gy")
    core = lax.rem(index_y, 2)
    tables = (keep_x, keep_y, keep_high, keep_low)

    def device(step_x, step_y):
        return (
            lax.rem(index_x + (step_x + N_GX), N_GX),
            lax.rem(index_y + (step_y + N_GY), N_GY),
        )

    barrier = pltpu.get_barrier_semaphore()
    peers = [(x, 0) for x in range(1, N_GX)]
    peers += [(0, y) for y in range(2, N_GY, 2)] + [(0, 1), (0, N_GY - 1)]
    peers += [(x, y) for x, y in NEIGHBOURS if x and y]
    for step_x, step_y in peers:
        pl.semaphore_signal(
            barrier, inc=1, device_id=device(step_x, step_y), device_id_type=MESH_IDS
        )

    started = []

    def send(number, source, target, step_x, step_y):
        copy = pltpu.make_async_remote_copy(
            src_ref=source,
            dst_ref=target,
            send_sem=send_sems.at[number],
            recv_sem=recv_sems.at[number],
            device_id=device(step_x, step_y),
            device_id_type=MESH_IDS,
        )
        copy.start()
        started.append(copy)
        return copy

    sums[...] = jnp.zeros_like(sums)

    def clear(x, carried):
        q1[x] = jnp.zeros((40, NZ), F32)
        return carried

    lax.fori_loop(0, 41, clear, 0)

    for copy in first_copies:
        copy.wait()

    def deposit(first, last, row, count, send_finished):
        def step(plane, carried):
            deposit_plane(
                plane, charge_ref, fraction_ref, cell_ref, sums, index_y, tables
            )
            return carried

        lax.fori_loop(first, last, step, 0, unroll=2)
        flat = sums[row : row + count].reshape(count * EY, NZ)
        value = times_const(flat, forward_high_ref[...], forward_low_ref[...])
        own[row : row + count] = value.reshape(count, EY, NZ)
        edge[row : row + count] = own[row : row + count, 11:19, :]

        def restrict_y(x, carried):
            q1[x + 3, 8:32, :] = own[x]
            total = jnp.zeros((16, NZ), F32)
            for offset, weight in taps:
                total = total + weight * q1[x + 3, pl.ds(6 + offset, 16, stride=2), :]
            part1[x] = total
            return carried

        send_finished()
        lax.fori_loop(row, row + count, restrict_y, 0)

    round1 = []

    def send_edges(number, row, count):
        rows = pl.ds(row, count)
        round1.append(send(number, edge.at[rows], from_y.at[0, rows], 0, 1))
        round1.append(send(number + 1, own.at[rows, 0:8, :], from_y.at[1, rows], 0, -1))

    high_x, low_x = pl.ds(29, 6), pl.ds(0, 6)

    def send_high():
        pl.semaphore_wait(barrier, len(peers))
        round1.append(send(0, edge.at[high_x], from_corner.at[0], 1, 1))
        round1.append(send(1, own.at[high_x, 0:8, :], from_corner.at[1], 1, -1))
        round1.append(send(2, own.at[high_x], from_x.at[0], 1, 0))
        send_edges(6, 29, 6)

    def send_low():
        round1.append(send(3, edge.at[low_x], from_corner.at[2], -1, 1))
        round1.append(send(4, own.at[low_x, 0:8, :], from_corner.at[3], -1, -1))
        round1.append(send(5, own.at[low_x], from_x.at[1], -1, 0))
        send_edges(8, 0, 6)

    deposit(26, 32, 29, 6, send_high)
    deposit(0, 6, 0, 6, send_low)
    deposit(6, 14, 6, 8, lambda: send_edges(10, 6, 8))
    deposit(14, 22, 14, 8, lambda: None)
    deposit(22, 26, 22, 7, lambda: None)

    for copy in later_copies:
        copy.wait()

    rows = []
    for m in range(-1, 19):
        total = jnp.zeros((16, NZ), F32)
        for offset, weight in taps:
            if 0 <= 2 * m + offset < EX:
                total = total + weight * part1[2 * m + offset]
        rows.append(total)
    level2 = times_const(
        jnp.concatenate(rows[0::2], axis=0), high_ref[C_M12], low_ref[C_M12]
    ) + times_const(jnp.concatenate(rows[1::2], axis=0), high_ref[C_M12B], low_ref[C_M12B])
    own2[...] = level2.reshape(10, 16, NZ)
    edge2[...] = own2[:, 5:13, :]

    round2 = []
    for number in (4, 5, 6, 7, 0, 1, 2, 3):
        step_x, step_y = NEIGHBOURS[number]
        rows = {0: pl.ds(0, 10), 1: pl.ds(6, 4), -1: pl.ds(0, 4)}[step_x]
        if step_y == 0:
            source, target = own2.at[rows], from_x2.at[number]
        elif step_x == 0:
            source = edge2 if step_y == 1 else own2.at[:, 0:8, :]
            target = from_y2.at[number - 2]
        else:
            source = edge2.at[rows] if step_y == 1 else own2.at[rows, 0:8, :]
            target = from_corner2.at[number - 4]
        round2.append(send(16 + number, source, target, step_x, step_y))
    send_edges(12, 14, 8)
    send_edges(14, 22, 7)

    q2[...] = jnp.zeros_like(q2)
    q3[:, 24:32, :] = jnp.zeros((15, 8, NZ), F32)
    for pair in range(10):
        q2[3 + 2 * pair, 7:23, :] = own2[pair]
        q2[4 + 2 * pair, 7:23, :] = pltpu.roll(own2[pair], 64, axis=1)

    for copy in round2:
        copy.wait_recv()

    def add_to2(row, start, value):
        end = start + value.shape[0]
        for place, plane in ((row, value), (row + 1, pltpu.roll(value, 64, axis=1))):
            if 0 <= place < 26:
                q2[place, start:end, :] = q2[place, start:end, :] + plane

    for pair in range(10):
        add_to2(3 + 2 * pair, 4, from_y2[0, pair])
        add_to2(3 + 2 * pair, 15, from_y2[1, pair])
    for side, first in ((0, -1), (1, 19)):
        for pair in range(4):
            add_to2(first + 2 * pair, 7, from_x2[side, pair])
            add_to2(first + 2 * pair, 4, from_corner2[2 * side, pair])
            add_to2(first + 2 * pair, 15, from_corner2[2 * side + 1, pair])

    for m in range(8):
        total = jnp.zeros((24, NZ), F32)
        for offset, weight in taps:
            total = total + weight * q2[2 * m + 4 + offset, 0:24, :]
        part2[24 * m : 24 * (m + 1), :] = total
    tile = jnp.zeros((8, NZ), F32)
    for n in range(4):
        total = jnp.zeros((8, NZ), F32)
        for offset, weight in taps:
            total = total + weight * part2[pl.ds(8 + 2 * n + offset, 8, stride=24), :]
        tile = tile + times_const(total, high_ref[C_M23 + n], low_ref[C_M23 + n])
    ring_x[1] = tile

    round3 = []
    for step in (4, 5, 3, 6, 2, 7, 1):
        place = (N_GX - step + 1) % N_GX
        round3.append(send(23 + step, ring_x.at[1], ring_x.at[place], step, 0))

    def stencil_small(source, row, start, count, k_ref):
        total = jnp.zeros((count, NZ), F32)
        for across in range(4):
            for along in range(4):
                value = None
                for sign_r in sorted({across, -across}):
                    for sign_s in sorted({along, -along}):
                        piece = source[row + sign_r, start + sign_s : start + sign_s + count, :]
                        value = piece if value is None else value + piece
                total = total + k_ref[4 * across + along : 4 * across + along + 1, :] * value
        return total

    def stencil2(x, carried):
        smooth2[x] = stencil_small(q2, x + 3, 7, 16, k2_ref)
        return carried

    lax.fori_loop(0, 20, stencil2, 0)

    for copy in round3:
        copy.wait_recv()

    column = const_times(
        high_ref[C_UR, 0:32, 0:64], low_ref[C_UR, 0:32, 0:64], ring_x[...].reshape(64, NZ)
    )
    ring_y[core] = times_const(column[0:16], high_ref[C_BD0], low_ref[C_BD0]) + times_const(
        column[16:32], high_ref[C_BD1], low_ref[C_BD1]
    )
    round5 = {}
    for step in FAR_FIRST:
        place = 2 * (HALF_GY - step) + core
        round5[step] = send(34 + step, ring_y.at[core], ring_y.at[place], 0, 2 * step)

    def hand_on(place):
        row = ring_y.at[2 * place + core]
        return send(50 + place, row, row, 0, 1 - 2 * core)

    handed = [hand_on(0)]
    round4 = []
    for number, step in enumerate((1, -1, 2, -2)):
        round4.append(send(31 + number, ring_x.at[0:3], halo.at[2 - step], 0, step))

    for copy in round1:
        copy.wait_recv()

    def add_y(x, carried):
        q1[x + 3, 3:11, :] = q1[x + 3, 3:11, :] + from_y[0, x]
        q1[x + 3, 24:32, :] = q1[x + 3, 24:32, :] + from_y[1, x]
        return carried

    lax.fori_loop(0, EX, add_y, 0)
    for side, start in ((0, 0), (1, 35)):
        for x in range(6):
            row = start + x
            q1[row, 8:32, :] = q1[row, 8:32, :] + from_x[side, x]
            q1[row, 3:11, :] = q1[row, 3:11, :] + from_corner[2 * side, x]
            q1[row, 24:32, :] = q1[row, 24:32, :] + from_corner[2 * side + 1, x]

    def sum_y(x, carried):
        for dy in range(1, 4):
            sums1[dy - 1, x] = q1[x, 8 + dy : 32 + dy, :] + q1[x, 8 - dy : 32 - dy, :]
        return carried

    lax.fori_loop(0, 41, sum_y, 0)

    def stencil1(x, carried):
        total = jnp.zeros((EY, NZ), F32)
        for dy in range(4):
            for dx in range(4):
                if dy == 0:
                    value = q1[x + 3 + dx, 8:32, :]
                    if dx:
                        value = value + q1[x + 3 - dx, 8:32, :]
                else:
                    value = sums1[dy - 1, x + 3 + dx]
                    if dx:
                        value = value + sums1[dy - 1, x + 3 - dx]
                total = total + k1_ref[4 * dx + dy : 4 * dx + dy + 1, :] * value
        smooth1[x] = total
        return carried

    lax.fori_loop(0, EX, stencil1, 0)

    for step in reversed(FAR_FIRST):
        round5[step].wait_recv()
        handed.append(hand_on(HALF_GY - step))

    halo[2] = ring_x[0:3]
    for copy in round4:
        copy.wait_recv()
    for y in range(-5, 10):
        place = y % 4
        source = halo[y // 4 + 2].reshape(24, NZ)
        if place:
            source = pltpu.roll(source, NZ - 32 * place, axis=1)
        q3[y + 5, 0:24, :] = source

    def stencil3(y, carried):
        field3[y] = stencil_small(q3, y + 3, 6, 16, k3_ref)
        return carried

    lax.fori_loop(0, 9, stencil3, 0)

    for copy in handed:
        copy.wait_recv()

    def add_slot(slot, totals):
        values = ring_y[slot]
        return tuple(
            total + table[row % 4, slot + (3 - row // 4) - core] * values
            for row, total in enumerate(totals)
        )

    coarse = lax.fori_loop(
        0, N_GY, add_slot, tuple(jnp.zeros((16, NZ), F32) for _ in range(9)), unroll=4
    )
    coarse = jnp.concatenate(coarse, axis=0)
    half0 = times_const(coarse, high_ref[C_NZ0], low_ref[C_NZ0])
    half1 = times_const(coarse, high_ref[C_NZ1], low_ref[C_NZ1])
    for row in range(9):
        both = jnp.concatenate(
            [half0[16 * row : 16 * (row + 1)], half1[16 * row : 16 * (row + 1)]], axis=0
        )
        field3[row] = field3[row] + const_times(
            high_ref[C_PU, 0:16, 0:32], low_ref[C_PU, 0:16, 0:32], both
        )

    fields = [prolonged_rows(lambda m: field3[m + 2], y) for y in range(-1, 11)]
    up3[...] = times_const(jnp.concatenate(fields, axis=0), high_ref[C_M23T], low_ref[C_M23T])

    def column3(m):
        return up3[pl.ds(m + 2, 12, stride=16), :]

    for x in range(-1, 19):
        smooth2[x + 1, 0:12, :] = smooth2[x + 1, 0:12, :] + prolonged_rows(column3, x)

    part = times_const(
        smooth2[...].reshape(20 * 16, NZ), high_ref[C_M12T], low_ref[C_M12T]
    ).reshape(20, 16, NZ)
    smooth2[...] = part

    def widen_y(x, carried):
        rows = [smooth2[x, n : n + 12, :] for n in range(4)]
        up2[x, pl.ds(0, 12, stride=2), :] = rows[1]
        up2[x, pl.ds(1, 12, stride=2), :] = 0.5625 * (rows[1] + rows[2]) - 0.0625 * (
            rows[0] + rows[3]
        )
        return carried

    lax.fori_loop(0, 20, widen_y, 0)

    def widen_x(m, carried):
        values = [up2[m + n] for n in range(4)]
        sums[2 * m] = smooth1[2 * m] + values[1]
        sums[2 * m + 1] = smooth1[2 * m + 1] + (
            0.5625 * (values[1] + values[2]) - 0.0625 * (values[0] + values[3])
        )
        return carried

    lax.fori_loop(0, 17, widen_x, 0)
    sums[34] = smooth1[34] + up2[18]

    flat = sums[...].reshape(EX * EY, NZ)
    value = times_const(flat, inverse_high_ref[...], inverse_low_ref[...])
    window[...] = value.reshape(EX, EY, NZ)
    grid_ref[...] = window[:CX, :CY, :]

    def sample(plane, carried):
        sample_plane(plane, tables, window, atom_ref)
        return carried

    lax.fori_loop(0, CX, sample, 0, unroll=4)

    for copy in started:
        copy.wait_send()


def finish_kernel(grid_in, atom_in, grid_out, atom_out, grid, atom, sems):
    pairs = ((grid_in, grid, grid_out), (atom_in, atom, atom_out))
    loads = [
        pltpu.make_async_copy(source, middle, sems.at[number])
        for number, (source, middle, target) in enumerate(pairs)
    ]
    stores = [
        pltpu.make_async_copy(middle, target, sems.at[2 + number])
        for number, (source, middle, target) in enumerate(pairs)
    ]
    for load in loads:
        load.start()
    for load, store in zip(loads, stores):
        load.wait()
        store.start()
    for store in stores:
        store.wait()


def in_vmem(count):
    return [pl.BlockSpec(memory_space=pltpu.VMEM)] * count


def local(charges, fractions, cells):
    charge = charges.reshape(1, ATOMS_DEV)
    fraction = fractions.reshape(3, 1, ATOMS_DEV)
    cell = cells.reshape(2, ATOMS_DEV)
    forward = [jnp.asarray(part) for part in split_pair(real_basis(NZ).T)]
    inverse = [jnp.asarray(part) for part in split_pair(real_basis(NZ))]
    high, low = split_constants()
    inputs = [
        charge,
        fraction,
        cell,
        *forward,
        *inverse,
        jnp.asarray(stencil_table(1, 128)),
        jnp.asarray(stencil_table(2, 64)),
        jnp.asarray(stencil_table(3, 32)),
        jnp.asarray(high),
        jnp.asarray(low),
        jnp.asarray(coarse_table()),
    ]
    potential, sampled = pl.pallas_call(
        levels_entry,
        out_shape=(
            jax.ShapeDtypeStruct((CX, CY, NZ), F32),
            jax.ShapeDtypeStruct((1, ATOMS_DEV), F32),
        ),
        in_specs=[pl.BlockSpec(memory_space=pltpu.HBM)] * N_IN,
        out_specs=in_vmem(2),
        scratch_shapes=[pltpu.VMEM(value.shape, value.dtype) for value in inputs]
        + [
            pltpu.SemaphoreType.DMA((N_IN,)),
            pltpu.VMEM((CX, 4, PLANE), F32),
            pltpu.VMEM((CX, EY, PLANE), F32),
            pltpu.VMEM((CX, NZ, PLANE), BF16),
            pltpu.VMEM((CX, NZ, PLANE), BF16),
            pltpu.VMEM((EX, EY, NZ), F32),
            pltpu.VMEM((EX, EY, NZ), F32),
            pltpu.VMEM((EX, EY, NZ), F32),
            pltpu.VMEM((EX, 8, NZ), F32),
            pltpu.VMEM((2, 6, EY, NZ), F32),
            pltpu.VMEM((2, EX, 8, NZ), F32),
            pltpu.VMEM((4, 6, 8, NZ), F32),
            pltpu.VMEM((2, 4, 16, NZ), F32),
            pltpu.VMEM((2, 10, 8, NZ), F32),
            pltpu.VMEM((4, 4, 8, NZ), F32),
            pltpu.VMEM((10, 16, NZ), F32),
            pltpu.VMEM((10, 8, NZ), F32),
            pltpu.VMEM((41, 40, NZ), F32),
            pltpu.VMEM((3, 41, EY, NZ), F32),
            pltpu.VMEM((EX, EY, NZ), F32),
            pltpu.VMEM((EX, 16, NZ), F32),
            pltpu.VMEM((26, 32, NZ), F32),
            pltpu.VMEM((20, 16, NZ), F32),
            pltpu.VMEM((8 * 24, NZ), F32),
            pltpu.VMEM((N_GX, 8, NZ), F32),
            pltpu.VMEM((5, 3, 8, NZ), F32),
            pltpu.VMEM((N_GY, 16, NZ), F32),
            pltpu.VMEM((15, 32, NZ), F32),
            pltpu.VMEM((9, 16, NZ), F32),
            pltpu.VMEM((12 * 16, NZ), F32),
            pltpu.VMEM((20, EY, NZ), F32),
            pltpu.SemaphoreType.DMA((N_SEMS,)),
            pltpu.SemaphoreType.DMA((N_SEMS,)),
        ],
        compiler_params=pltpu.CompilerParams(collective_id=0, has_side_effects=True),
        name="levels",
    )(*inputs)
    potential, sampled = pl.pallas_call(
        finish_kernel,
        out_shape=(
            jax.ShapeDtypeStruct((CX, CY, NZ), F32),
            jax.ShapeDtypeStruct((1, ATOMS_DEV), F32),
        ),
        in_specs=[pl.BlockSpec(memory_space=pl.ANY)] * 2,
        out_specs=[pl.BlockSpec(memory_space=pl.ANY)] * 2,
        scratch_shapes=[
            pltpu.VMEM((CX, CY, NZ), F32),
            pltpu.VMEM((1, ATOMS_DEV), F32),
            pltpu.SemaphoreType.DMA((4,)),
        ],
        name="finish",
    )(potential, sampled)
    return potential, sampled.reshape(1, 1, ATOMS_DEV)


def solution(mesh):
    placed = (P("gx", "gy", None), P("gx", "gy", None, None), P("gx", "gy", None, None))
    return jax.shard_map(
        local,
        mesh=mesh,
        in_specs=placed,
        out_specs=(P("gx", "gy", None), P("gx", "gy", None)),
        check_vma=False,
    )
```
